64 devices in a mesh: data: 4 (over x, y), dap: 16 (over z, core).
Axes of the slice: x: 2, y: 2, z: 8, core: 2. Of those that a mesh axis runs over, the one named last changes fastest.
The devices are a block of a 4x4x8 slice.
Arguments:
- msa_act: bfloat16 [512, 192, 256], P(('data', 'dap')), parts along dimension 0
- pair_act: bfloat16 [768, 192, 128], P(('data', 'dap')), parts along dimension 0
- msa_mask: int32 [512, 192], P('data'), parts along dimension 0
- res_mask: int32 [768], P('data'), parts along dimension 0
- w_row_bias: bfloat16 [2, 128, 8], replicated
- w_row_in: bfloat16 [2, 256, 4, 8, 32], replicated
- w_row_out: bfloat16 [2, 8, 32, 256], replicated
- w_col_in: bfloat16 [2, 256, 4, 8, 32], replicated
- w_col_out: bfloat16 [2, 8, 32, 256], replicated
- w_opm_in: bfloat16 [2, 256, 2, 32], replicated
- w_opm_out: bfloat16 [2, 32, 32, 128], replicated
- w_ts_bias: bfloat16 [2, 128, 4], replicated
- w_ts_in: bfloat16 [2, 128, 4, 4, 32], replicated
- w_ts_out: bfloat16 [2, 4, 32, 128], replicated
- w_te_bias: bfloat16 [2, 128, 4], replicated
- w_te_in: bfloat16 [2, 128, 4, 4, 32], replicated
- w_te_out: bfloat16 [2, 4, 32, 128], replicated
Outputs:
- output 1: bfloat16 [512, 192, 256], P(('data', 'dap')), parts along dimension 0
- output 2: bfloat16 [768, 192, 128], P(('data', 'dap')), parts along dimension 0
There are 4 independent parts. The reference program is written for one: setup_inputs(seed, part) draws one part's arguments, and reference() takes and returns one part's arrays. A program takes and returns all parts, laid end to end along the dimension named above; an argument that names none is the same for every part.
All inputs are finite; a program needn't handle non-finite values.
Results may differ from the reference program's by a relative error of at most 0.0162995.
Values are sent between devices in bfloat16 or wider.
A program may use at most 768 MiB of HBM per device.

```python
import jax
import jax.numpy as jnp
from jax import lax

NR = 192
NS = 128
C_M = 256
C_Z = 128
HEADS_MSA = 8
HEAD_MSA = 32
HEADS_TRI = 4
HEAD_TRI = 32
OPM_DIM = 32


def draw_normal(key, shape, scale):
    return (jax.random.normal(key, shape, jnp.float32) * scale).astype(jnp.bfloat16)


def setup_inputs(seed: int = 0, part: int = 0) -> dict:
    base_key = jax.random.key(seed)
    part_keys = jax.random.split(jax.random.fold_in(base_key, part), 4)
    w_keys = jax.random.split(jax.random.fold_in(base_key, 1000), 13)
    width_msa = HEADS_MSA * HEAD_MSA
    width_tri = HEADS_TRI * HEAD_TRI
    return {
        'msa_act': draw_normal(part_keys[0], (NS, NR, C_M), 1.0),
        'pair_act': draw_normal(part_keys[1], (NR, NR, C_Z), 1.0),
        'msa_mask': (jax.random.randint(part_keys[2], (NS, NR), 0, 4) > 0).astype(jnp.int32),
        'res_mask': (jax.random.randint(part_keys[3], (NR,), 0, 4) > 0).astype(jnp.int32),
        'w_row_bias': draw_normal(w_keys[0], (2, C_Z, HEADS_MSA), 1.5 * C_Z ** -0.5),
        'w_row_in': draw_normal(w_keys[1], (2, C_M, 4, HEADS_MSA, HEAD_MSA), 1.25 * C_M ** -0.5),
        'w_row_out': draw_normal(w_keys[2], (2, HEADS_MSA, HEAD_MSA, C_M), 0.5 * width_msa ** -0.5),
        'w_col_in': draw_normal(w_keys[3], (2, C_M, 4, HEADS_MSA, HEAD_MSA), 1.25 * C_M ** -0.5),
        'w_col_out': draw_normal(w_keys[4], (2, HEADS_MSA, HEAD_MSA, C_M), 0.5 * width_msa ** -0.5),
        'w_opm_in': draw_normal(w_keys[5], (2, C_M, 2, OPM_DIM), C_M ** -0.5),
        'w_opm_out': draw_normal(w_keys[6], (2, OPM_DIM, OPM_DIM, C_Z), 0.25 * NS ** 0.5 / OPM_DIM),
        'w_ts_bias': draw_normal(w_keys[7], (2, C_Z, HEADS_TRI), 1.5 * C_Z ** -0.5),
        'w_ts_in': draw_normal(w_keys[8], (2, C_Z, 4, HEADS_TRI, HEAD_TRI), 1.25 * C_Z ** -0.5),
        'w_ts_out': draw_normal(w_keys[9], (2, HEADS_TRI, HEAD_TRI, C_Z), 0.5 * width_tri ** -0.5),
        'w_te_bias': draw_normal(w_keys[10], (2, C_Z, HEADS_TRI), 1.5 * C_Z ** -0.5),
        'w_te_in': draw_normal(w_keys[11], (2, C_Z, 4, HEADS_TRI, HEAD_TRI), 1.25 * C_Z ** -0.5),
        'w_te_out': draw_normal(w_keys[12], (2, HEADS_TRI, HEAD_TRI, C_Z), 0.5 * width_tri ** -0.5),
    }


def layer_norm(values):
    flat = values.astype(jnp.float32)
    row_mean = jnp.mean(flat, axis=-1, keepdims=True)
    centered = flat - row_mean
    row_var = jnp.mean(centered * centered, axis=-1, keepdims=True)
    return (centered * lax.rsqrt(row_var + 1e-5)).astype(jnp.bfloat16)


def add_residual(current, update):
    return (current.astype(jnp.float32) + update).astype(jnp.bfloat16)


def pair_bias(pair_ln, w_bias):
    num_res = pair_ln.shape[0]
    flat = jnp.dot(pair_ln.reshape(num_res * num_res, -1), w_bias, preferred_element_type=jnp.float32)
    return jnp.transpose(flat.astype(jnp.bfloat16).reshape(num_res, num_res, -1), (2, 0, 1))


def attend_one(x_ln, w_in, w_out, bias_hqk, key_mask):
    length = x_ln.shape[0]
    heads = w_in.shape[2]
    head_dim = w_in.shape[3]
    projected = jnp.dot(x_ln, w_in.reshape(w_in.shape[0], -1), preferred_element_type=jnp.float32)
    projected = projected.astype(jnp.bfloat16).astype(jnp.float32).reshape(length, 4, heads, head_dim)
    logits = jnp.einsum('qhd,khd->hqk', projected[:, 0], projected[:, 1]) * head_dim ** -0.5
    if bias_hqk is not None:
        logits = logits + bias_hqk.astype(jnp.float32)
    logits = jnp.where(key_mask[None, None, :] > 0, logits, -1e9)
    attn_probs = jax.nn.softmax(logits, axis=-1).astype(jnp.bfloat16).astype(jnp.float32)
    attended = jnp.einsum('hqk,khd->qhd', attn_probs, projected[:, 2])
    gated = (attended * jax.nn.sigmoid(projected[:, 3])).astype(jnp.bfloat16)
    return jnp.dot(gated.reshape(length, heads * head_dim), w_out.reshape(heads * head_dim, -1), preferred_element_type=jnp.float32)


def row_attention(msa_act, bias_hqk, msa_mask, w_in, w_out):
    def one_seq(inputs):
        seq_act, seq_mask = inputs
        return add_residual(seq_act, attend_one(layer_norm(seq_act), w_in, w_out, bias_hqk, seq_mask))
    return lax.map(one_seq, (msa_act, msa_mask))


def column_attention(msa_act, msa_mask, w_in, w_out):
    def one_col(inputs):
        col_act, col_mask = inputs
        return add_residual(col_act, attend_one(layer_norm(col_act), w_in, w_out, None, col_mask))
    result = lax.map(one_col, (jnp.swapaxes(msa_act, 0, 1), msa_mask.T))
    return jnp.swapaxes(result, 0, 1)


def outer_mean(msa_act, pair_act, msa_mask, w_in, w_out):
    num_seq, num_res, width = msa_act.shape
    mask_f32 = msa_mask.astype(jnp.float32)
    projected = jnp.dot(layer_norm(msa_act).reshape(num_seq * num_res, width), w_in.reshape(width, -1), preferred_element_type=jnp.float32)
    projected = projected.reshape(num_seq, num_res, 2, -1) * mask_f32[:, :, None, None]
    projected = projected.astype(jnp.bfloat16).astype(jnp.float32)
    left = jnp.swapaxes(projected[:, :, 0], 0, 1)
    right = projected[:, :, 1]
    pair_norm = jnp.dot(mask_f32.T, mask_f32)
    w_flat = w_out.reshape(-1, w_out.shape[-1])
    def one_row(inputs):
        left_row, norm_row = inputs
        outer = jnp.einsum('sp,sjq->jpq', left_row, right).astype(jnp.bfloat16)
        update = jnp.dot(outer.reshape(num_res, -1), w_flat, preferred_element_type=jnp.float32)
        return update / (1e-3 + norm_row[:, None])
    return add_residual(pair_act, lax.map(one_row, (left, pair_norm)))


def triangle_start(pair_act, res_mask, w_bias, w_in, w_out):
    pair_ln = layer_norm(pair_act)
    bias_hqk = pair_bias(pair_ln, w_bias)
    def one_row(row_ln):
        return attend_one(row_ln, w_in, w_out, bias_hqk, res_mask)
    return add_residual(pair_act, lax.map(one_row, pair_ln))


def triangle_end(pair_act, res_mask, w_bias, w_in, w_out):
    flipped = triangle_start(jnp.swapaxes(pair_act, 0, 1), res_mask, w_bias, w_in, w_out)
    return jnp.swapaxes(flipped, 0, 1)


def reference(msa_act, pair_act, msa_mask, res_mask, w_row_bias, w_row_in, w_row_out, w_col_in, w_col_out, w_opm_in, w_opm_out, w_ts_bias, w_ts_in, w_ts_out, w_te_bias, w_te_in, w_te_out):
    bias_first = pair_bias(layer_norm(pair_act), w_row_bias[0])
    msa_act = row_attention(msa_act, bias_first, msa_mask, w_row_in[0], w_row_out[0])
    msa_act = column_attention(msa_act, msa_mask, w_col_in[0], w_col_out[0])
    pair_act = outer_mean(msa_act, pair_act, msa_mask, w_opm_in[0], w_opm_out[0])
    pair_act = triangle_start(pair_act, res_mask, w_ts_bias[0], w_ts_in[0], w_ts_out[0])
    pair_act = triangle_end(pair_act, res_mask, w_te_bias[0], w_te_in[0], w_te_out[0])
    bias_second = pair_bias(layer_norm(pair_act), w_row_bias[1])
    msa_act = column_attention(msa_act, msa_mask, w_col_in[1], w_col_out[1])
    pair_act = outer_mean(msa_act, pair_act, msa_mask, w_opm_in[1], w_opm_out[1])
    msa_act = row_attention(msa_act, bias_second, msa_mask, w_row_in[1], w_row_out[1])
    pair_act = triangle_end(pair_act, res_mask, w_te_bias[1], w_te_in[1], w_te_out[1])
    pair_act = triangle_start(pair_act, res_mask, w_ts_bias[1], w_ts_in[1], w_ts_out[1])
    return msa_act, pair_act
```

```python
import functools

import jax
import jax.numpy as jnp
from jax import lax
from jax.experimental import pallas as pl
from jax.experimental.pallas import tpu as pltpu
from jax.sharding import PartitionSpec as P

F32 = jnp.float32
BF16 = jnp.bfloat16
LOG2E = 1.4426950408889634
NEG = -1e9 * LOG2E
HEAD = 32
INTERPRET = False


def dot(lhs, rhs, lc, rc):
    return lax.dot_general(lhs, rhs, (((lc,), (rc,)), ((), ())), preferred_element_type=F32)


def layer_norm(x):
    mean = jnp.mean(x, axis=-1, keepdims=True)
    cen = x - mean
    var = jnp.mean(cen * cen, axis=-1, keepdims=True)
    return (cen * lax.rsqrt(var + 1e-5)).astype(BF16)


def attention(x, wt, wk, wo, bias, mask2d, kcol):
    length = x.shape[0]
    width = wk.shape[1]
    xl = layer_norm(x)
    t = dot(wt, xl, 1, 1).astype(BF16)
    k = dot(xl, wk, 1, 0)
    if kcol is not None:
        k = k * kcol
    k = k.astype(BF16)
    outs = []
    for h in range(width // HEAD):
        grp, r = h // 4, h % 4
        parts = [t[HEAD * h:HEAD * h + HEAD]]
        if r > 0:
            parts.insert(0, jnp.zeros((HEAD * r, length), BF16))
        if r < 3:
            parts.append(jnp.zeros((HEAD * (3 - r), length), BF16))
        qh = jnp.concatenate(parts, axis=0)
        s = dot(k[:, 128 * grp:128 * grp + 128], qh, 1, 0) * (HEAD ** -0.5 * LOG2E)
        if bias is not None:
            s = s + bias[h]
        if mask2d is not None:
            s = jnp.where(mask2d > 0, s, NEG)
        top = jnp.max(s, axis=0, keepdims=True)
        e = jnp.exp2(s - top)
        den = jnp.sum(e, axis=0, keepdims=True)
        o = dot(t[width + HEAD * h:width + HEAD * h + HEAD], e.astype(BF16), 1, 0)
        gate = jax.nn.sigmoid(t[2 * width + HEAD * h:2 * width + HEAD * h + HEAD].astype(F32))
        outs.append((o * (1.0 / den) * gate).astype(BF16))
    return dot(jnp.concatenate(outs, axis=0), wo, 0, 0)


def residual(x, update):
    return (x + update).astype(BF16)


def spread(row, length):
    return jnp.broadcast_to(row, (length, length)).T


def stage(stg, pair, first, second, ndev):
    rows = first.shape[0] // ndev
    off = pl.multiple_of(2 * rows * pair, 8)
    for d in range(ndev):
        both = jnp.concatenate([first[rows * d:rows * d + rows], second[rows * d:rows * d + rows]], axis=0)
        stg[d, pl.ds(off, 2 * rows), :] = both.astype(BF16)


def fill(work, ref):
    for t in range(work.shape[0]):
        work[t] = ref[..., 128 * t:128 * t + 128].astype(F32).reshape(work.shape[1:])


def take(work, start, count, stride):
    return jnp.concatenate([work.at[t][pl.ds(start, count, stride=stride), :] for t in range(work.shape[0])], axis=1)


def bias_pieces(load, count, wb, piece):
    def body(b, _):
        zl = layer_norm(load(b))
        piece[b] = dot(wb[...], zl, 1, 1).astype(BF16)
        return 0
    lax.fori_loop(0, count, body, 0)


def spread_bias(gath, gf, bias, transpose, mask_row):
    length, heads = gath.shape[0], gath.shape[1]
    gf[...] = gath[...].astype(F32)
    keep = None if mask_row is None else spread(mask_row, length)
    for h in range(heads):
        value = gf[:, h, :]
        if transpose:
            value = value.T
        value = value * LOG2E
        if keep is not None:
            value = jnp.where(keep > 0, value, NEG)
        bias[h] = value


def run(body, outs, scratch, *args):
    return pl.pallas_call(
        body,
        out_shape=[jax.ShapeDtypeStruct(s, d) for s, d in outs],
        in_specs=[pl.BlockSpec(memory_space=pltpu.VMEM)] * len(args),
        out_specs=[pl.BlockSpec(memory_space=pltpu.VMEM)] * len(outs),
        scratch_shapes=[pltpu.VMEM(s, d) for s, d in scratch],
        interpret=INTERPRET,
        compiler_params=pltpu.CompilerParams(vmem_limit_bytes=56 * 2**20),
    )(*args)


def solution(mesh):
    nd = mesh.shape['dap']

    def local_step(m, z, msa_mask, res_mask, w_row_bias, w_row_in, w_row_out, w_col_in, w_col_out, w_opm_in, w_opm_out, w_ts_bias, w_ts_in, w_ts_out, w_te_bias, w_te_in, w_te_out):
        me = lax.axis_index('dap')
        sl, nr, cm = m.shape
        rl, _, cz = z.shape
        ns = sl * nd
        hm, ht = w_row_bias.shape[2], w_ts_bias.shape[2]
        wm, wz = hm * HEAD, ht * HEAD
        od = w_opm_in.shape[3]

        maskf = msa_mask.astype(F32)
        mask_seq = lax.dynamic_slice_in_dim(maskf, me * sl, sl, 0)
        mask_col = lax.dynamic_slice_in_dim(maskf, me * rl, rl, 1).T
        mask_b = msa_mask.astype(BF16)
        mask_r = res_mask.astype(F32)[None, :]

        def split(w, width):
            c = w.shape[1]
            w = w.reshape(2, c, 4, width)
            wt = jnp.stack([w[:, :, 0], w[:, :, 2], w[:, :, 3]], axis=1)
            return wt.transpose(0, 1, 3, 2).reshape(2, 3 * width, c), w[:, :, 1]

        row_t, row_k = split(w_row_in, wm)
        col_t, col_k = split(w_col_in, wm)
        ts_t, ts_k = split(w_ts_in, wz)
        te_t, te_k = split(w_te_in, wz)
        row_o = w_row_out.reshape(2, wm, cm)
        col_o = w_col_out.reshape(2, wm, cm)
        ts_o = w_ts_out.reshape(2, wz, cz)
        te_o = w_te_out.reshape(2, wz, cz)
        row_b = w_row_bias.transpose(0, 2, 1)
        ts_b = w_ts_bias.transpose(0, 2, 1)
        te_b = w_te_bias.transpose(0, 2, 1)
        opm_i = w_opm_in.reshape(2, cm, 2 * od).transpose(0, 2, 1)
        opm_o = jnp.stack([w_opm_out[0].transpose(2, 1, 0), w_opm_out[1].transpose(2, 0, 1)]).reshape(2, cz, od * od)

        gather = lambda v: lax.all_gather(v, 'dap', axis=0, tiled=True)
        swap = lambda v: lax.all_to_all(v, 'dap', 0, 0, tiled=True)

        def bias_kernel(z_ref, wb, piece):
            bias_pieces(lambda b: z_ref[b].astype(F32), rl, wb, piece)

        def bias_call(zz, wb):
            return run(bias_kernel, [((rl, wb.shape[0], nr), BF16)], [], zz, wb)[0]

        def row_kernel(transpose, staged, m_ref, g_ref, mask_ref, wt, wk, wo, out_ref, gf, bias, work):
            spread_bias(g_ref, gf, bias, transpose, None)
            if not staged:
                fill(work, m_ref)

            def one(s):
                x = m_ref[s].astype(F32) if staged else take(work, s, nr, sl)
                keep = spread(mask_ref[pl.ds(s, 1), :], nr)
                return residual(x, attention(x, wt[...], wk[...], wo[...], bias, keep, None))

            def body(t, _):
                pair = [one(2 * t), one(2 * t + 1)]
                if staged:
                    stage(out_ref, t, pair[0].astype(F32), pair[1].astype(F32), nd)
                else:
                    out_ref[2 * t], out_ref[2 * t + 1] = pair
                return 0
            lax.fori_loop(0, sl // 2, body, 0)

        def row_call(mm, g, b, transpose, staged):
            rows = sl * rl
            out = (nd, rows, cm) if staged else (sl, nr, cm)
            work = (cm // 128, nd * rows, 128)
            return run(functools.partial(row_kernel, transpose, staged), [(out, BF16)],
                       [((nr, hm, nr), F32), ((hm, nr, nr), F32), (work, F32)],
                       mm, g, mask_seq, row_t[b], row_k[b], row_o[b])[0]

        def col_kernel(b, r_ref, mask_ref, wt, wk, wo, wi, new_ref, loc_ref, gat_ref, *scratch):
            work, = scratch
            if b == 0:
                fill(work, r_ref)

            def one(i):
                x = take(work, i, ns, rl) if b == 0 else r_ref[i].astype(F32)
                row = mask_ref[pl.ds(i, 1), :]
                new = residual(x, attention(x, wt[...], wk[...], wo[...], None, spread(row, ns), None))
                newf = new.astype(F32)
                if b == 0:
                    new_ref[i] = new
                ac = (dot(wi[...], layer_norm(newf), 1, 1) * row).astype(BF16)
                a, c = ac[:od], ac[od:]
                loc_ref[i] = a if b == 0 else c
                gat_ref[i] = c if b == 0 else a
                return newf

            def body(t, _):
                first, second = one(2 * t), one(2 * t + 1)
                if b == 1:
                    stage(new_ref, t, first, second, nd)
                return 0
            lax.fori_loop(0, rl // 2, body, 0)

        def col_call(r, b):
            rows = sl * rl
            out = (rl, ns, cm) if b == 0 else (nd, rows, cm)
            work = (cm // 128, nd * rows, 128)
            return run(functools.partial(col_kernel, b), [(out, BF16), ((rl, od, ns), BF16), ((rl, od, ns), BF16)],
                       [(work, F32)], r, mask_col, col_t[b], col_k[b], col_o[b], opm_i[b])

        def opm_kernel(z_ref, loc_ref, gat_ref, mc_ref, mask_ref, w_ref, wb, out_ref, piece, gf, xs):
            gf[...] = gat_ref[...].astype(F32).reshape(gf.shape)
            loc = loc_ref[...].reshape(rl * od, ns)
            norm = dot(mc_ref[...].astype(BF16), mask_ref[...], 1, 0)

            def grow(g, _):
                col = gf[pl.ds(g, nr, stride=od), :].astype(BF16)
                x = dot(loc, col, 1, 1).astype(BF16)
                off = pl.multiple_of(g * od, od)
                for i in range(rl):
                    xs[i, pl.ds(off, od), :] = x[od * i:od * i + od]
                return 0
            lax.fori_loop(0, od, grow, 0)
            for i in range(rl):
                upd = dot(w_ref[...], xs[i], 1, 0) / (1e-3 + norm[i:i + 1])
                new = residual(z_ref[i].astype(F32), upd.T)
                out_ref[i] = new
                piece[i] = dot(wb[...], layer_norm(new.astype(F32)), 1, 1).astype(BF16)

        def opm_call(zz, loc, gat, b, wb):
            return run(opm_kernel, [((rl, nr, cz), BF16), ((rl, ht, nr), BF16)],
                       [((nr * od, ns), F32), ((rl, od * od, nr), BF16)],
                       zz, loc, gat, mask_col, mask_b, opm_o[b], wb)

        def tri_kernel(staged, z_ref, g_ref, mask_ref, wt, wk, wo, out_ref, gf, bias, work, kc):
            spread_bias(g_ref, gf, bias, True, mask_ref[...])
            kc[...] = jnp.broadcast_to(mask_ref[...], (wz, nr)).T

            def one(b):
                x = z_ref[b].astype(F32)
                return residual(x, attention(x, wt[...], wk[...], wo[...], bias, None, kc[...]))

            def body(t, _):
                pair = [one(2 * t), one(2 * t + 1)]
                if staged:
                    stage(out_ref, t, pair[0].astype(F32), pair[1].astype(F32), nd)
                else:
                    out_ref[2 * t], out_ref[2 * t + 1] = pair
                return 0
            lax.fori_loop(0, rl // 2, body, 0)

        def tri_call(zz, g, wt, wk, wo, staged):
            out = (nd, rl * rl, cz) if staged else (rl, nr, cz)
            return run(functools.partial(tri_kernel, staged), [(out, BF16)],
                       [((nr, ht, nr), F32), ((ht, nr, nr), F32), ((nd, rl * rl, cz), F32), ((nr, wz), F32)],
                       zz, g, mask_r, wt, wk, wo)[0]

        def turn_kernel(r_ref, wb, out_ref, piece, work):
            work[...] = r_ref[...].astype(F32).reshape(work.shape)

            def body(b, _):
                x = work[pl.ds(b, nr, stride=rl), :]
                out_ref[b] = x.astype(BF16)
                piece[b] = dot(wb[...], layer_norm(x), 1, 1).astype(BF16)
                return 0
            lax.fori_loop(0, rl, body, 0)

        def turn_call(r, wb):
            return run(turn_kernel, [((rl, nr, cz), BF16), ((rl, ht, nr), BF16)], [((nr * rl, cz), F32)], r, wb)

        g = gather(bias_call(z, row_b[0]))
        r = swap(row_call(m, g, 0, True, True))
        m, loc, gat = col_call(r, 0)
        r2, loc2, gat2 = col_call(m, 1)
        z, piece = opm_call(z, loc, gather(gat), 0, ts_b[0])
        rz = swap(tri_call(z, gather(piece), ts_t[0], ts_k[0], ts_o[0], True))
        z, piece = turn_call(rz, te_b[0])
        z = tri_call(z, gather(piece), te_t[0], te_k[0], te_o[0], False)
        g = gather(bias_call(z, row_b[1]))
        z, piece = opm_call(z, loc2, gather(gat2), 1, te_b[1])
        m = row_call(swap(r2), g, 1, False, False)
        rz = swap(tri_call(z, gather(piece), te_t[1], te_k[1], te_o[1], True))
        z, piece = turn_call(rz, ts_b[1])
        z = tri_call(z, gather(piece), ts_t[1], ts_k[1], ts_o[1], False)
        return m, z

    in_specs = (P(('data', 'dap')), P(('data', 'dap')), P('data'), P('data')) + (P(),) * 13
    out_specs = (P(('data', 'dap')), P(('data', 'dap')))
    return jax.shard_map(local_step, mesh=mesh, in_specs=in_specs, out_specs=out_specs, check_vma=False)
```

```python
import functools

import jax
import jax.numpy as jnp
from jax import lax
from jax.experimental import pallas as pl
from jax.experimental.pallas import tpu as pltpu
from jax.sharding import PartitionSpec as P

F32 = jnp.float32
BF16 = jnp.bfloat16
LOG2E = 1.4426950408889634
NEG = -1e9 * LOG2E
HEAD = 32
INTERPRET = False


def dot(lhs, rhs, lc, rc):
    return lax.dot_general(lhs, rhs, (((lc,), (rc,)), ((), ())), preferred_element_type=F32)


def layer_norm(x):
    mean = jnp.mean(x, axis=-1, keepdims=True)
    cen = x - mean
    var = jnp.mean(cen * cen, axis=-1, keepdims=True)
    return (cen * lax.rsqrt(var + 1e-5)).astype(BF16)


def project(xs, wt, wk, t_ref, k_ref, first, kcol):
    xl = [layer_norm(x) for x in xs]
    ts = [dot(wt[...], v, 1, 1) for v in xl]
    ks = [dot(v, wk[...], 1, 0) for v in xl]
    for n, v in enumerate(ts):
        t_ref[first + n] = v.astype(BF16)
    for n, v in enumerate(ks):
        if kcol is not None:
            v = v * kcol
        k_ref[first + n] = v.astype(BF16)


def diagonal(t, base, length):
    cols = []
    for r in range(4):
        parts = [t[base + HEAD * r:base + HEAD * r + HEAD]]
        if r > 0:
            parts.insert(0, jnp.zeros((HEAD * r, length), BF16))
        if r < 3:
            parts.append(jnp.zeros((HEAD * (3 - r), length), BF16))
        cols.append(jnp.concatenate(parts, axis=0))
    return jnp.concatenate(cols, axis=1)


def core(t_ref, k_ref, o_ref, rows, groups, bias, keeps):
    length = k_ref.shape[1]
    width = 128 * groups
    units = [(n, b, g) for n, b in enumerate(rows) for g in range(groups)]
    scores = []
    for n, b, g in units:
        t = t_ref[b, 128 * g:128 * g + 128, :]
        scores.append(dot(k_ref[b, :, 128 * g:128 * g + 128], diagonal(t, 0, length), 1, 0))
    probs = []
    dens = []
    for (n, b, g), s in zip(units, scores):
        s = s * (HEAD ** -0.5 * LOG2E)
        if bias is not None:
            s = s + bias[g]
        if keeps is not None:
            s = jnp.where(keeps[n] > 0, s, NEG)
        e = jnp.exp2(s - jnp.max(s, axis=0, keepdims=True))
        dens.append(jnp.sum(e, axis=0, keepdims=True))
        probs.append(e.astype(BF16))
    outs = [dot(t_ref[b, width + 128 * g:width + 128 * g + 128, :], p, 1, 0) for (n, b, g), p in zip(units, probs)]
    for (n, b, g), o, den in zip(units, outs, dens):
        inv = 1.0 / den
        gate = jax.nn.sigmoid(t_ref[b, 2 * width + 128 * g:2 * width + 128 * g + 128, :].astype(F32))
        parts = []
        for r in range(4):
            lanes = slice(length * r, length * r + length)
            parts.append(o[HEAD * r:HEAD * r + HEAD, lanes] * inv[:, lanes])
        o_ref[b, 128 * g:128 * g + 128, :] = (jnp.concatenate(parts, axis=0) * gate).astype(BF16)


def residual(x, update):
    return (x + update).astype(BF16)


def spread(row, lanes):
    return jnp.broadcast_to(row, (lanes, row.shape[1])).T


def widen(block, lanes):
    return jnp.concatenate([block] * (lanes // 128), axis=1)


def stage(stg, pair, first, second, ndev):
    rows = first.shape[0] // ndev
    off = pl.multiple_of(2 * rows * pair, 8)
    for d in range(ndev):
        both = jnp.concatenate([first[rows * d:rows * d + rows], second[rows * d:rows * d + rows]], axis=0)
        stg[d, pl.ds(off, 2 * rows), :] = both.astype(BF16)


def fill(work, ref):
    for t in range(work.shape[0]):
        work[t] = ref[..., 128 * t:128 * t + 128].astype(F32).reshape(work.shape[1:])


def take(work, start, count, stride):
    return jnp.concatenate([work.at[t][pl.ds(start, count, stride=stride), :] for t in range(work.shape[0])], axis=1)


def bias_pieces(load, count, wb, piece):
    def body(t, _):
        zl = [layer_norm(load(4 * t + n)) for n in range(4)]
        ps = [dot(wb[...], v, 1, 1) for v in zl]
        for n, v in enumerate(ps):
            piece[4 * t + n] = v.astype(BF16)
        return 0
    lax.fori_loop(0, count // 4, body, 0)


def spread_bias(gath, gf, bias, transpose, mask_row):
    length, heads = gath.shape[0], gath.shape[1]
    gf[...] = gath[...].astype(F32)
    keep = None if mask_row is None else widen(spread(mask_row, 128), 4 * length)
    for g in range(heads // 4):
        parts = []
        for r in range(4):
            value = gf[:, 4 * g + r, :]
            parts.append(value.T if transpose else value)
        value = jnp.concatenate(parts, axis=1) * LOG2E
        if keep is not None:
            value = jnp.where(keep > 0, value, NEG)
        bias[g] = value


def run(body, outs, scratch, *args):
    return pl.pallas_call(
        body,
        out_shape=[jax.ShapeDtypeStruct(s, d) for s, d in outs],
        in_specs=[pl.BlockSpec(memory_space=pltpu.VMEM)] * len(args),
        out_specs=[pl.BlockSpec(memory_space=pltpu.VMEM)] * len(outs),
        scratch_shapes=[pltpu.VMEM(s, d) for s, d in scratch],
        interpret=INTERPRET,
        compiler_params=pltpu.CompilerParams(vmem_limit_bytes=56 * 2**20),
    )(*args)


def solution(mesh):
    nd = mesh.shape['dap']

    def local_step(m, z, msa_mask, res_mask, w_row_bias, w_row_in, w_row_out, w_col_in, w_col_out, w_opm_in, w_opm_out, w_ts_bias, w_ts_in, w_ts_out, w_te_bias, w_te_in, w_te_out):
        me = lax.axis_index('dap')
        sl, nr, cm = m.shape
        rl, _, cz = z.shape
        ns = sl * nd
        hm, ht = w_row_bias.shape[2], w_ts_bias.shape[2]
        wm, wz = hm * HEAD, ht * HEAD
        od = w_opm_in.shape[3]

        maskf = msa_mask.astype(F32)
        mask_seq = lax.dynamic_slice_in_dim(maskf, me * sl, sl, 0)
        mask_col = lax.dynamic_slice_in_dim(maskf, me * rl, rl, 1).T
        mask_b = msa_mask.astype(BF16)
        mask_r = res_mask.astype(F32)[None, :]

        def split(w, width):
            c = w.shape[1]
            w = w.reshape(2, c, 4, width)
            wt = jnp.stack([w[:, :, 0], w[:, :, 2], w[:, :, 3]], axis=1)
            return wt.transpose(0, 1, 3, 2).reshape(2, 3 * width, c), w[:, :, 1]

        row_t, row_k = split(w_row_in, wm)
        col_t, col_k = split(w_col_in, wm)
        ts_t, ts_k = split(w_ts_in, wz)
        te_t, te_k = split(w_te_in, wz)
        row_o = w_row_out.reshape(2, wm, cm)
        col_o = w_col_out.reshape(2, wm, cm)
        ts_o = w_ts_out.reshape(2, wz, cz)
        te_o = w_te_out.reshape(2, wz, cz)
        row_b = w_row_bias.transpose(0, 2, 1)
        ts_b = w_ts_bias.transpose(0, 2, 1)
        te_b = w_te_bias.transpose(0, 2, 1)
        opm_i = w_opm_in.reshape(2, cm, 2 * od).transpose(0, 2, 1)
        opm_o = jnp.stack([w_opm_out[0].transpose(2, 1, 0), w_opm_out[1].transpose(2, 0, 1)]).reshape(2, cz, od * od)

        gather = lambda v: lax.all_gather(v, 'dap', axis=0, tiled=True)
        swap = lambda v: lax.all_to_all(v, 'dap', 0, 0, tiled=True)

        def bias_kernel(z_ref, wb, piece):
            bias_pieces(lambda b: z_ref[b].astype(F32), rl, wb, piece)

        def bias_call(zz, wb):
            return run(bias_kernel, [((rl, wb.shape[0], nr), BF16)], [], zz, wb)[0]

        def row_kernel(transpose, staged, m_ref, g_ref, mask_ref, wt, wk, wo, out_ref, gf, bias, work, t_ref, k_ref, o_ref):
            if not staged:
                fill(work, m_ref)

            def load(s):
                return m_ref[s].astype(F32) if staged else take(work, s, nr, sl)

            def first(t, _):
                project([load(2 * t), load(2 * t + 1)], wt, wk, t_ref, k_ref, 2 * t, None)
                return 0
            lax.fori_loop(0, sl // 2, first, 0)
            spread_bias(g_ref, gf, bias, transpose, None)

            def second(s, _):
                keep = widen(spread(mask_ref[pl.ds(s, 1), :], 128), 4 * nr)
                core(t_ref, k_ref, o_ref, [s], hm // 4, bias, [keep])
                return 0
            lax.fori_loop(0, sl, second, 0)

            def third(t, _):
                ups = [dot(o_ref[2 * t + n], wo[...], 0, 0) for n in range(2)]
                pair = [residual(load(2 * t + n), ups[n]) for n in range(2)]
                if staged:
                    stage(out_ref, t, pair[0].astype(F32), pair[1].astype(F32), nd)
                else:
                    out_ref[2 * t], out_ref[2 * t + 1] = pair
                return 0
            lax.fori_loop(0, sl // 2, third, 0)

        def row_call(mm, g, b, transpose, staged):
            rows = sl * rl
            out = (nd, rows, cm) if staged else (sl, nr, cm)
            work = (cm // 128, nd * rows, 128)
            return run(functools.partial(row_kernel, transpose, staged), [(out, BF16)],
                       [((nr, hm, nr), F32), ((hm // 4, nr, 4 * nr), F32), (work, F32),
                        ((sl, 3 * wm, nr), BF16), ((sl, nr, wm), BF16), ((sl, wm, nr), BF16)],
                       mm, g, mask_seq, row_t[b], row_k[b], row_o[b])[0]

        def col_kernel(b, r_ref, mask_ref, wt, wk, wo, wi, new_ref, loc_ref, gat_ref, work, t_ref, k_ref, o_ref):
            if b == 0:
                fill(work, r_ref)

            def load(i):
                return take(work, i, ns, rl) if b == 0 else r_ref[i].astype(F32)

            def first(t, _):
                project([load(4 * t + n) for n in range(4)], wt, wk, t_ref, k_ref, 4 * t, None)
                return 0
            lax.fori_loop(0, rl // 4, first, 0)

            def second(t, _):
                rows = [2 * t, 2 * t + 1]
                keeps = [widen(spread(mask_ref[pl.ds(i, 1), :], 128), 4 * ns) for i in rows]
                core(t_ref, k_ref, o_ref, rows, hm // 4, None, keeps)
                return 0
            lax.fori_loop(0, rl // 2, second, 0)

            def third(t, _):
                rows = [4 * t + n for n in range(4)]
                ups = [dot(o_ref[i], wo[...], 0, 0) for i in rows]
                new = [residual(load(i), u) for i, u in zip(rows, ups)]
                newf = [v.astype(F32) for v in new]
                if b == 0:
                    for i, v in zip(rows, new):
                        new_ref[i] = v
                else:
                    stage(new_ref, 2 * t, newf[0], newf[1], nd)
                    stage(new_ref, 2 * t + 1, newf[2], newf[3], nd)
                ln = [layer_norm(v) for v in newf]
                acs = [dot(wi[...], v, 1, 1) for v in ln]
                for i, v in zip(rows, acs):
                    ac = (v * mask_ref[pl.ds(i, 1), :]).astype(BF16)
                    a, c = ac[:od], ac[od:]
                    loc_ref[i] = a if b == 0 else c
                    gat_ref[i] = c if b == 0 else a
                return 0
            lax.fori_loop(0, rl // 4, third, 0)

        def col_call(r, b):
            rows = sl * rl
            out = (rl, ns, cm) if b == 0 else (nd, rows, cm)
            work = (cm // 128, nd * rows, 128)
            return run(functools.partial(col_kernel, b), [(out, BF16), ((rl, od, ns), BF16), ((rl, od, ns), BF16)],
                       [(work, F32), ((rl, 3 * wm, ns), BF16), ((rl, ns, wm), BF16), ((rl, wm, ns), BF16)], r, mask_col, col_t[b], col_k[b], col_o[b], opm_i[b])

        def opm_kernel(z_ref, loc_ref, gat_ref, mc_ref, mask_ref, w_ref, wb, out_ref, piece, gf, xs, nrm):
            gf[...] = gat_ref[...].astype(F32).reshape(gf.shape)
            nrm[...] = dot(mc_ref[...].astype(BF16), mask_ref[...], 1, 0)

            def grow(t, _):
                loc = loc_ref[...].reshape(rl * od, ns)
                for n in range(4):
                    g = 4 * t + n
                    col = gf[pl.ds(g, nr, stride=od), :].astype(BF16)
                    x = dot(loc, col, 1, 1).astype(BF16)
                    off = pl.multiple_of(g * od, od)
                    for i in range(rl):
                        xs[i, pl.ds(off, od), :] = x[od * i:od * i + od]
                return 0
            lax.fori_loop(0, od // 4, grow, 0)

            def fold(t, _):
                rows = [4 * t + n for n in range(4)]
                ups = [dot(w_ref[...], xs[i], 1, 0) for i in rows]
                ups = [u / (1e-3 + nrm[pl.ds(i, 1), :]) for i, u in zip(rows, ups)]
                ups = [u.T for u in ups]
                new = [residual(z_ref[i].astype(F32), u) for i, u in zip(rows, ups)]
                for i, v in zip(rows, new):
                    out_ref[i] = v
                ln = [layer_norm(v.astype(F32)) for v in new]
                ps = [dot(wb[...], v, 1, 1) for v in ln]
                for i, v in zip(rows, ps):
                    piece[i] = v.astype(BF16)
                return 0
            lax.fori_loop(0, rl // 4, fold, 0)

        def opm_call(zz, loc, gat, b, wb):
            return run(opm_kernel, [((rl, nr, cz), BF16), ((rl, ht, nr), BF16)],
                       [((nr * od, ns), F32), ((rl, od * od, nr), BF16), ((rl, nr), F32)],
                       zz, loc, gat, mask_col, mask_b, opm_o[b], wb)

        def tri_kernel(staged, z_ref, g_ref, mask_ref, wt, wk, wo, out_ref, gf, bias, kc, t_ref, k_ref, o_ref):
            kc[...] = spread(mask_ref[...], wz)

            def first(t, _):
                project([z_ref[4 * t + n].astype(F32) for n in range(4)], wt, wk, t_ref, k_ref, 4 * t, kc[...])
                return 0
            lax.fori_loop(0, rl // 4, first, 0)
            spread_bias(g_ref, gf, bias, True, mask_ref[...])

            def second(t, _):
                core(t_ref, k_ref, o_ref, [2 * t, 2 * t + 1], ht // 4, bias, None)
                return 0
            lax.fori_loop(0, rl // 2, second, 0)

            def third(t, _):
                rows = [4 * t + n for n in range(4)]
                ups = [dot(o_ref[i], wo[...], 0, 0) for i in rows]
                new = [residual(z_ref[i].astype(F32), u) for i, u in zip(rows, ups)]
                if staged:
                    for n in range(2):
                        stage(out_ref, 2 * t + n, new[2 * n].astype(F32), new[2 * n + 1].astype(F32), nd)
                else:
                    for i, v in zip(rows, new):
                        out_ref[i] = v
                return 0
            lax.fori_loop(0, rl // 4, third, 0)

        def tri_call(zz, g, wt, wk, wo, staged):
            out = (nd, rl * rl, cz) if staged else (rl, nr, cz)
            return run(functools.partial(tri_kernel, staged), [(out, BF16)],
                       [((nr, ht, nr), F32), ((ht // 4, nr, 4 * nr), F32), ((nr, wz), F32),
                        ((rl, 3 * wz, nr), BF16), ((rl, nr, wz), BF16), ((rl, wz, nr), BF16)],
                       zz, g, mask_r, wt, wk, wo)[0]

        def turn_kernel(r_ref, wb, out_ref, piece, work):
            work[...] = r_ref[...].astype(F32).reshape(work.shape)

            for b in range(rl):
                out_ref[b] = work[pl.ds(b, nr, stride=rl), :].astype(BF16)
            bias_pieces(lambda b: out_ref[b].astype(F32), rl, wb, piece)

        def turn_call(r, wb):
            return run(turn_kernel, [((rl, nr, cz), BF16), ((rl, ht, nr), BF16)], [((nr * rl, cz), F32)], r, wb)

        g = gather(bias_call(z, row_b[0]))
        r = swap(row_call(m, g, 0, True, True))
        m, loc, gat = col_call(r, 0)
        r2, loc2, gat2 = col_call(m, 1)
        z, piece = opm_call(z, loc, gather(gat), 0, ts_b[0])
        rz = swap(tri_call(z, gather(piece), ts_t[0], ts_k[0], ts_o[0], True))
        z, piece = turn_call(rz, te_b[0])
        z = tri_call(z, gather(piece), te_t[0], te_k[0], te_o[0], False)
        g = gather(bias_call(z, row_b[1]))
        z, piece = opm_call(z, loc2, gather(gat2), 1, te_b[1])
        m = row_call(swap(r2), g, 1, False, False)
        rz = swap(tri_call(z, gather(piece), te_t[1], te_k[1], te_o[1], True))
        z, piece = turn_call(rz, ts_b[1])
        z = tri_call(z, gather(piece), ts_t[1], ts_k[1], ts_o[1], False)
        return m, z

    in_specs = (P(('data', 'dap')), P(('data', 'dap')), P('data'), P('data')) + (P(),) * 13
    out_specs = (P(('data', 'dap')), P(('data', 'dap')))
    return jax.shard_map(local_step, mesh=mesh, in_specs=in_specs, out_specs=out_specs, check_vma=False)
```

```python
import functools

import jax
import jax.numpy as jnp
from jax import lax
from jax.experimental import pallas as pl
from jax.experimental.pallas import tpu as pltpu
from jax.sharding import PartitionSpec as P

F32 = jnp.float32
BF16 = jnp.bfloat16
LOG2E = 1.4426950408889634
NEG = -1e9 * LOG2E
HEAD = 32
MESH = pl.DeviceIdType.MESH


def dot(lhs, rhs, lc, rc):
    return lax.dot_general(lhs, rhs, (((lc,), (rc,)), ((), ())), preferred_element_type=F32)


def layer_norm(x):
    mean = jnp.mean(x, axis=-1, keepdims=True)
    cen = x - mean
    var = jnp.mean(cen * cen, axis=-1, keepdims=True)
    return (cen * lax.rsqrt(var + 1e-5)).astype(BF16)


def project(xs, wt, wk, t_ref, k_ref, first, kcol):
    xl = [layer_norm(x) for x in xs]
    ts = [dot(wt[...], v, 1, 1) for v in xl]
    ks = [dot(v, wk[...], 1, 0) for v in xl]
    for n, v in enumerate(ts):
        t_ref[first + n] = v.astype(BF16)
    for n, v in enumerate(ks):
        if kcol is not None:
            v = v * kcol
        k_ref[first + n] = v.astype(BF16)


def diagonal(t, base, length):
    cols = []
    for r in range(4):
        parts = [t[base + HEAD * r:base + HEAD * r + HEAD]]
        if r > 0:
            parts.insert(0, jnp.zeros((HEAD * r, length), BF16))
        if r < 3:
            parts.append(jnp.zeros((HEAD * (3 - r), length), BF16))
        cols.append(jnp.concatenate(parts, axis=0))
    return jnp.concatenate(cols, axis=1)


def core(t_ref, k_ref, o_ref, rows, groups, bias, keeps):
    length = k_ref.shape[1]
    width = 128 * groups
    units = [(n, b, g) for n, b in enumerate(rows) for g in range(groups)]
    scores = []
    for n, b, g in units:
        t = t_ref[b, 128 * g:128 * g + 128, :]
        scores.append(dot(k_ref[b, :, 128 * g:128 * g + 128], diagonal(t, 0, length), 1, 0))
    probs = []
    dens = []
    for (n, b, g), s in zip(units, scores):
        s = s * (HEAD ** -0.5 * LOG2E)
        if bias is not None:
            s = s + bias[g]
        if keeps is not None:
            s = jnp.where(keeps[n] > 0, s, NEG)
        e = jnp.exp2(s - jnp.max(s, axis=0, keepdims=True))
        dens.append(jnp.sum(e, axis=0, keepdims=True))
        probs.append(e.astype(BF16))
    outs = [dot(t_ref[b, width + 128 * g:width + 128 * g + 128, :], p, 1, 0) for (n, b, g), p in zip(units, probs)]
    for (n, b, g), o, den in zip(units, outs, dens):
        inv = 1.0 / den
        gate = jax.nn.sigmoid(t_ref[b, 2 * width + 128 * g:2 * width + 128 * g + 128, :].astype(F32))
        parts = []
        for r in range(4):
            lanes = slice(length * r, length * r + length)
            parts.append(o[HEAD * r:HEAD * r + HEAD, lanes] * inv[:, lanes])
        o_ref[b, 128 * g:128 * g + 128, :] = (jnp.concatenate(parts, axis=0) * gate).astype(BF16)


def residual(x, update):
    return (x + update).astype(BF16)


def spread(row, lanes):
    return jnp.broadcast_to(row, (lanes, row.shape[1])).T


def widen(block, lanes):
    return jnp.concatenate([block] * (lanes // 128), axis=1)


def stage(stg, pair, first, second, ndev):
    rows = first.shape[0] // ndev
    off = pl.multiple_of(2 * rows * pair, 8)
    for d in range(ndev):
        both = jnp.concatenate([first[rows * d:rows * d + rows], second[rows * d:rows * d + rows]], axis=0)
        stg[d, pl.ds(off, 2 * rows), :] = both.astype(BF16)


def fill(work, ref):
    for t in range(work.shape[0]):
        work[t] = ref[..., 128 * t:128 * t + 128].astype(F32).reshape(work.shape[1:])


def take(work, start, count, stride):
    return jnp.concatenate([work.at[t][pl.ds(start, count, stride=stride), :] for t in range(work.shape[0])], axis=1)


def spread_bias(gath, gf, bias, transpose, mask_row):
    length, heads = gath.shape[0], gath.shape[1]
    gf[...] = gath[...].astype(F32)
    keep = None if mask_row is None else widen(spread(mask_row, 128), 4 * length)
    for g in range(heads // 4):
        parts = []
        for r in range(4):
            value = gf[:, 4 * g + r, :]
            parts.append(value.T if transpose else value)
        value = jnp.concatenate(parts, axis=1) * LOG2E
        if keep is not None:
            value = jnp.where(keep > 0, value, NEG)
        bias[g] = value


def bias_pieces(load, count, wb, store):
    def body(t, _):
        zl = [layer_norm(load(4 * t + n)) for n in range(4)]
        ps = [dot(wb, v, 1, 1) for v in zl]
        for n, v in enumerate(ps):
            store(4 * t + n, v.astype(BF16))
        return 0
    lax.fori_loop(0, count // 4, body, 0)


class Comm:
    def __init__(self, nd, sems):
        self.nd = nd
        self.me = lax.axis_index('dap')
        self.partner = self.me + 1 - 2 * lax.rem(self.me, 2)
        self.ssem, self.rsem, self.fsem, self.gsem = sems

    def copy(self, src, dst, send, recv, dev):
        return pltpu.make_async_remote_copy(src_ref=src, dst_ref=dst, send_sem=send, recv_sem=recv,
                                            device_id={'dap': dev}, device_id_type=MESH)

    def barrier_signal(self):
        bar = pltpu.get_barrier_semaphore()

        def body(k, _):
            pl.semaphore_signal(bar, inc=1, device_id={'dap': lax.rem(self.me + k, self.nd)}, device_id_type=MESH)
            return 0
        lax.fori_loop(1, self.nd, body, 0)

    def barrier_wait(self):
        pl.semaphore_wait(pltpu.get_barrier_semaphore(), self.nd - 1)

    def await_bytes(self, ref, sem):
        pltpu.make_async_copy(ref, ref, sem).wait()

    def gather_start(self, buf, i):
        n = buf.shape[0] // self.nd
        own = buf.at[pl.ds(self.me * n, n)]

        def body(k, _):
            self.copy(own, own, self.ssem.at[i], self.gsem.at[i, k], lax.rem(self.me + 2 * k, self.nd)).start()
            return 0
        lax.fori_loop(1, self.nd // 2, body, 0)
        self.copy(own, own, self.ssem.at[i], self.gsem.at[i, 0], self.partner).start()

    def gather_finish(self, buf, i):
        n = buf.shape[0] // self.nd
        half = self.nd // 2

        def body(k, _):
            slot = buf.at[pl.ds(lax.rem(self.me + self.nd - 2 * k, self.nd) * n, n)]
            self.await_bytes(slot, self.gsem.at[i, k])
            self.copy(slot, slot, self.fsem.at[i], self.rsem.at[i], self.partner).start()
            return 0
        lax.fori_loop(1, half, body, 0)
        self.await_bytes(buf.at[pl.ds(0, n)], self.gsem.at[i, 0])
        rest = buf.at[pl.ds(0, (half - 1) * n)]
        self.await_bytes(rest, self.rsem.at[i])
        self.await_bytes(rest, self.fsem.at[i])
        self.await_bytes(buf.at[pl.ds(0, half * n)], self.ssem.at[i])

    def swap_start(self, send, recv, i, off, rows):
        part = pl.ds(off, rows)

        def body(k, _):
            d = lax.rem(self.me + k, self.nd)
            self.copy(send.at[d, part], recv.at[self.me, part], self.ssem.at[i], self.rsem.at[i], d).start()
            return 0
        lax.fori_loop(1, self.nd, body, 0)
        pltpu.make_async_copy(send.at[self.me, part], recv.at[self.me, part], self.rsem.at[i]).start()

    def swap_finish(self, send, recv, i):
        self.await_bytes(recv, self.rsem.at[i])
        self.await_bytes(send.at[pl.ds(0, self.nd - 1)], self.ssem.at[i])


def kernel(names, outs, nd, refs):
    r = dict(zip(names, refs))
    class N:
        pass
    v = N()
    v.__dict__.update(r)
    sl, nr, cm = v.m.shape
    rl, _, cz = v.z.shape
    ns = sl * nd
    wm, wz = v.row_k.shape[2], v.ts_k.shape[2]
    gm, gz = wm // 128, wz // 128
    od = v.opm_i.shape[1] // 2
    comm = Comm(nd, (v.ssem, v.rsem, v.fsem, v.gsem))
    me = comm.me
    rows_m = sl * rl

    def store_piece(buf):
        def store(i, val):
            buf[me * rl + i] = val
        return store

    def loop(n, body):
        def step(t, _):
            body(t)
            return 0
        lax.fori_loop(0, n, step, 0)

    def row_project(load, b):
        loop(sl // 2, lambda t: project([load(2 * t), load(2 * t + 1)], v.row_t[b], v.row_k[b], v.rt, v.rk, 2 * t, None))

    def row_attend(load, b, finish):
        def body(t):
            for n in range(2):
                keep = widen(spread(v.mask_seq[pl.ds(2 * t + n, 1), :], 128), 4 * nr)
                core(v.rt, v.rk, v.ro, [2 * t + n], gm, v.rbias, [keep])
            ups = [dot(v.ro[2 * t + n], v.row_o[b], 0, 0) for n in range(2)]
            finish(t, [residual(load(2 * t + n), ups[n]) for n in range(2)])
        loop(sl // 2, body)

    def col_project(load, b):
        loop(rl // 4, lambda t: project([load(4 * t + n) for n in range(4)], v.col_t[b], v.col_k[b], v.ct, v.ck, 4 * t, None))

    def col_attend(load, b, finish, loc, gat):
        def body(t):
            rows = [2 * t, 2 * t + 1]
            keeps = [widen(spread(v.mask_col[pl.ds(i, 1), :], 128), 4 * ns) for i in rows]
            core(v.ct, v.ck, v.co, rows, gm, None, keeps)
        loop(rl // 2, body)

        def out(t):
            rows = [4 * t + n for n in range(4)]
            ups = [dot(v.co[i], v.col_o[b], 0, 0) for i in rows]
            new = [residual(load(i), u) for i, u in zip(rows, ups)]
            newf = [x.astype(F32) for x in new]
            finish(t, new, newf)
            ln = [layer_norm(x) for x in newf]
            acs = [dot(v.opm_i[b], x, 1, 1) for x in ln]
            for i, x in zip(rows, acs):
                ac = (x * v.mask_col[pl.ds(i, 1), :]).astype(BF16)
                a, c = ac[:od], ac[od:]
                loc[i] = a if b == 0 else c
                gat[me * rl + i] = c if b == 0 else a
        loop(rl // 4, out)

    def opm(loc, gat, b, load, wb, piece):
        v.gcol[...] = gat[...].astype(F32).reshape(v.gcol.shape)
        v.nrm[...] = dot(v.mask_col[...].astype(BF16), v.mask_b[...], 1, 0)

        def grow(t):
            left = loc[...].reshape(rl * od, ns)
            for n in range(4):
                g = 4 * t + n
                col = v.gcol[pl.ds(g, nr, stride=od), :].astype(BF16)
                x = dot(left, col, 1, 1).astype(BF16)
                off = pl.multiple_of(g * od, od)
                for i in range(rl):
                    v.xs[i, pl.ds(off, od), :] = x[od * i:od * i + od]
        loop(od // 4, grow)

        def fold(t):
            rows = [4 * t + n for n in range(4)]
            ups = [dot(v.opm_o[b], v.xs[i], 1, 0) for i in rows]
            ups = [u / (1e-3 + v.nrm[pl.ds(i, 1), :]) for i, u in zip(rows, ups)]
            ups = [u.T for u in ups]
            new = [residual(load(i), u) for i, u in zip(rows, ups)]
            for i, x in zip(rows, new):
                v.zc[i] = x
            ln = [layer_norm(x.astype(F32)) for x in new]
            ps = [dot(wb, x, 1, 1) for x in ln]
            for i, x in zip(rows, ps):
                piece[me * rl + i] = x.astype(BF16)
        loop(rl // 4, fold)

    def zload(i):
        return v.zc[i].astype(F32)

    def tri_project(wt, wk):
        loop(rl // 4, lambda t: project([zload(4 * t + n) for n in range(4)], wt, wk, v.tt, v.tk, 4 * t, v.kc[...]))

    def tri_attend(wo, finish):
        def body(t):
            core(v.tt, v.tk, v.to, [2 * t, 2 * t + 1], gz, v.tbias, None)
            rows = [2 * t, 2 * t + 1]
            ups = [dot(v.to[i], wo, 0, 0) for i in rows]
            finish(t, [residual(zload(i), u) for i, u in zip(rows, ups)])
        loop(rl // 2, body)

    def send_pair(send, recv, i, rows):
        def finish(t, pair):
            stage(send, t, pair[0].astype(F32), pair[1].astype(F32), nd)
            comm.swap_start(send, recv, i, pl.multiple_of(2 * rows * t, 8), 2 * rows)
        return finish

    def keep_pair(out):
        def finish(t, pair):
            out[2 * t], out[2 * t + 1] = pair
        return finish

    def turn(recv):
        fill(v.zwork, recv)
        for b in range(rl):
            v.zc[b] = take(v.zwork, b, nr, rl).astype(BF16)

    comm.barrier_signal()
    bias_pieces(lambda i: v.z[i].astype(F32), rl, v.row_b[0], store_piece(v.g0))
    v.kc[...] = spread(v.mask_r[...], wz)
    comm.barrier_wait()
    comm.gather_start(v.g0, 0)
    mload = lambda s: v.m[s].astype(F32)
    row_project(mload, 0)
    comm.gather_finish(v.g0, 0)
    spread_bias(v.g0, v.gf, v.rbias, True, None)
    row_attend(mload, 0, send_pair(v.s0, v.r0, 8, rl))
    comm.swap_finish(v.s0, v.r0, 8)

    fill(v.mwork, v.r0)
    cload = lambda i: take(v.mwork, i, ns, rl)
    col_project(cload, 0)

    def keep_four(t, new, newf):
        for n, x in enumerate(new):
            v.mc[4 * t + n] = x
    col_attend(cload, 0, keep_four, v.loc0, v.g1)
    comm.gather_start(v.g1, 1)

    c2load = lambda i: v.mc[i].astype(F32)
    col_project(c2load, 1)

    def send_four(t, new, newf):
        for n in range(2):
            stage(v.s1, 2 * t + n, newf[2 * n], newf[2 * n + 1], nd)
    col_attend(c2load, 1, send_four, v.loc1, v.g2)
    comm.gather_finish(v.g1, 1)
    opm(v.loc0, v.g1, 0, lambda i: v.z[i].astype(F32), v.ts_b[0], v.g3)
    comm.gather_start(v.g3, 3)
    tri_project(v.ts_t[0], v.ts_k[0])
    comm.gather_finish(v.g3, 3)
    spread_bias(v.g3, v.gf2, v.tbias, True, v.mask_r[...])
    tri_attend(v.ts_o[0], send_pair(v.s2, v.r2, 9, rl))
    comm.gather_start(v.g2, 2)
    comm.swap_finish(v.s2, v.r2, 9)
    turn(v.r2)
    bias_pieces(zload, rl, v.te_b[0], store_piece(v.g4))
    comm.gather_start(v.g4, 4)
    comm.swap_start(v.s1, v.r1, 10, 0, rows_m)
    tri_project(v.te_t[0], v.te_k[0])
    comm.gather_finish(v.g4, 4)
    spread_bias(v.g4, v.gf2, v.tbias, True, v.mask_r[...])
    tri_attend(v.te_o[0], keep_pair(v.zc))

    bias_pieces(zload, rl, v.row_b[1], store_piece(v.g5))
    comm.gather_start(v.g5, 5)
    comm.gather_finish(v.g2, 2)
    opm(v.loc1, v.g2, 1, zload, v.te_b[1], v.g6)
    comm.gather_start(v.g6, 6)
    comm.swap_finish(v.s1, v.r1, 10)
    fill(v.mwork, v.r1)
    rload = lambda s: take(v.mwork, s, nr, sl)
    row_project(rload, 1)
    tri_project(v.te_t[1], v.te_k[1])
    comm.gather_finish(v.g5, 5)
    comm.gather_finish(v.g6, 6)
    spread_bias(v.g6, v.gf2, v.tbias, True, v.mask_r[...])
    tri_attend(v.te_o[1], send_pair(v.s3, v.r3, 11, rl))
    spread_bias(v.g5, v.gf, v.rbias, False, None)
    row_attend(rload, 1, keep_pair(v.m_out))
    comm.swap_finish(v.s3, v.r3, 11)
    turn(v.r3)
    bias_pieces(zload, rl, v.ts_b[1], store_piece(v.g7))
    comm.gather_start(v.g7, 7)
    tri_project(v.ts_t[1], v.ts_k[1])
    comm.gather_finish(v.g7, 7)
    spread_bias(v.g7, v.gf2, v.tbias, True, v.mask_r[...])
    tri_attend(v.ts_o[1], keep_pair(v.z_out))


def solution(mesh):
    nd = mesh.shape['dap']

    def local_step(m, z, msa_mask, res_mask, w_row_bias, w_row_in, w_row_out, w_col_in, w_col_out, w_opm_in, w_opm_out, w_ts_bias, w_ts_in, w_ts_out, w_te_bias, w_te_in, w_te_out):
        me = lax.axis_index('dap')
        sl, nr, cm = m.shape
        rl, _, cz = z.shape
        ns = sl * nd
        hm, ht = w_row_bias.shape[2], w_ts_bias.shape[2]
        wm, wz = hm * HEAD, ht * HEAD
        od = w_opm_in.shape[3]

        maskf = msa_mask.astype(F32)
        mask_seq = lax.dynamic_slice_in_dim(maskf, me * sl, sl, 0)
        mask_col = lax.dynamic_slice_in_dim(maskf, me * rl, rl, 1).T
        mask_b = msa_mask.astype(BF16)
        mask_r = res_mask.astype(F32)[None, :]

        def split(w, width):
            c = w.shape[1]
            w = w.reshape(2, c, 4, width)
            wt = jnp.stack([w[:, :, 0], w[:, :, 2], w[:, :, 3]], axis=1)
            return wt.transpose(0, 1, 3, 2).reshape(2, 3 * width, c), w[:, :, 1]

        row_t, row_k = split(w_row_in, wm)
        col_t, col_k = split(w_col_in, wm)
        ts_t, ts_k = split(w_ts_in, wz)
        te_t, te_k = split(w_te_in, wz)
        row_o = w_row_out.reshape(2, wm, cm)
        col_o = w_col_out.reshape(2, wm, cm)
        ts_o = w_ts_out.reshape(2, wz, cz)
        te_o = w_te_out.reshape(2, wz, cz)
        row_b = w_row_bias.transpose(0, 2, 1)
        ts_b = w_ts_bias.transpose(0, 2, 1)
        te_b = w_te_bias.transpose(0, 2, 1)
        opm_i = w_opm_in.reshape(2, cm, 2 * od).transpose(0, 2, 1)
        opm_o = jnp.stack([w_opm_out[0].transpose(2, 1, 0), w_opm_out[1].transpose(2, 0, 1)]).reshape(2, cz, od * od)

        ins = dict(m=m, z=z, mask_seq=mask_seq, mask_col=mask_col, mask_b=mask_b, mask_r=mask_r,
                   row_t=row_t, row_k=row_k, row_o=row_o, row_b=row_b, col_t=col_t, col_k=col_k, col_o=col_o,
                   ts_t=ts_t, ts_k=ts_k, ts_o=ts_o, ts_b=ts_b, te_t=te_t, te_k=te_k, te_o=te_o, te_b=te_b,
                   opm_i=opm_i, opm_o=opm_o)
        outs = dict(m_out=m, z_out=z)
        gm, gz = wm // 128, wz // 128
        xm, xz = (nd, sl * rl, cm), (nd, rl * rl, cz)
        grow, gtri, gopm = (nd * rl, hm, nr), (nd * rl, ht, nr), (nd * rl, od, ns)
        scratch = dict(
            s0=(xm, BF16), r0=(xm, BF16), s1=(xm, BF16), r1=(xm, BF16),
            s2=(xz, BF16), r2=(xz, BF16), s3=(xz, BF16), r3=(xz, BF16),
            g0=(grow, BF16), g5=(grow, BF16), g1=(gopm, BF16), g2=(gopm, BF16),
            g3=(gtri, BF16), g4=(gtri, BF16), g6=(gtri, BF16), g7=(gtri, BF16),
            gf=(grow, F32), gf2=(gtri, F32), rbias=((gm, nr, 4 * nr), F32), tbias=((gz, nr, 4 * nr), F32),
            mwork=((cm // 128, nd * sl * rl, 128), F32), zwork=((cz // 128, nr * rl, 128), F32),
            gcol=((nr * od, ns), F32), xs=((rl, od * od, nr), BF16), nrm=((rl, nr), F32), kc=((nr, wz), F32),
            rt=((sl, 3 * wm, nr), BF16), rk=((sl, nr, wm), BF16), ro=((sl, wm, nr), BF16),
            ct=((rl, 3 * wm, ns), BF16), ck=((rl, ns, wm), BF16), co=((rl, wm, ns), BF16),
            tt=((rl, 3 * wz, nr), BF16), tk=((rl, nr, wz), BF16), to=((rl, wz, nr), BF16),
            mc=((rl, ns, cm), BF16), zc=((rl, nr, cz), BF16), loc0=((rl, od, ns), BF16), loc1=((rl, od, ns), BF16))
        sems = dict(ssem=(12,), rsem=(12,), fsem=(8,), gsem=(8, nd // 2))
        names = list(ins) + list(outs) + list(scratch) + list(sems)
        return pl.pallas_call(
            lambda *refs: kernel(names, outs, nd, refs),
            out_shape=[jax.ShapeDtypeStruct(o.shape, o.dtype) for o in outs.values()],
            in_specs=[pl.BlockSpec(memory_space=pltpu.VMEM)] * len(ins),
            out_specs=[pl.BlockSpec(memory_space=pltpu.VMEM)] * len(outs),
            scratch_shapes=[pltpu.VMEM(*x) for x in scratch.values()] + [pltpu.SemaphoreType.DMA(x) for x in sems.values()],
            compiler_params=pltpu.CompilerParams(collective_id=0, has_side_effects=True, vmem_limit_bytes=67043328),
        )(*ins.values())

    in_specs = (P(('data', 'dap')), P(('data', 'dap')), P('data'), P('data')) + (P(),) * 13
    out_specs = (P(('data', 'dap')), P(('data', 'dap')))
    return jax.shard_map(local_step, mesh=mesh, in_specs=in_specs, out_specs=out_specs, check_vma=False)
```

```python
import functools

import jax
import jax.numpy as jnp
from jax import lax
from jax.experimental import pallas as pl
from jax.experimental.pallas import tpu as pltpu
from jax.sharding import PartitionSpec as P

F32 = jnp.float32
BF16 = jnp.bfloat16
LOG2E = 1.4426950408889634
NEG = -1e9 * LOG2E
HEAD = 32
MESH = pl.DeviceIdType.MESH


def dot(lhs, rhs, lc, rc):
    return lax.dot_general(lhs, rhs, (((lc,), (rc,)), ((), ())), preferred_element_type=F32)


def layer_norm(x):
    mean = jnp.mean(x, axis=-1, keepdims=True)
    cen = x - mean
    var = jnp.mean(cen * cen, axis=-1, keepdims=True)
    return (cen * lax.rsqrt(var + 1e-5)).astype(BF16)


def project(xs, wt, wk, t_ref, k_ref, first, kcol):
    xl = [layer_norm(x) for x in xs]
    ts = [dot(wt[...], v, 1, 1) for v in xl]
    ks = [dot(v, wk[...], 1, 0) for v in xl]
    for n, v in enumerate(ts):
        t_ref[first + n] = v.astype(BF16)
    for n, v in enumerate(ks):
        if kcol is not None:
            v = v * kcol
        k_ref[first + n] = v.astype(BF16)


def diagonal(t, base, length):
    cols = []
    for r in range(4):
        parts = [t[base + HEAD * r:base + HEAD * r + HEAD]]
        if r > 0:
            parts.insert(0, jnp.zeros((HEAD * r, length), BF16))
        if r < 3:
            parts.append(jnp.zeros((HEAD * (3 - r), length), BF16))
        cols.append(jnp.concatenate(parts, axis=0))
    return jnp.concatenate(cols, axis=1)


def core(t_ref, k_ref, o_ref, rows, groups, bias, keeps):
    length = k_ref.shape[1]
    width = 128 * groups
    units = [(n, b, g) for n, b in enumerate(rows) for g in range(groups)]
    scores = []
    for n, b, g in units:
        t = t_ref[b, 128 * g:128 * g + 128, :]
        scores.append(dot(k_ref[b, :, 128 * g:128 * g + 128], diagonal(t, 0, length), 1, 0))
    probs = []
    dens = []
    for (n, b, g), s in zip(units, scores):
        s = s * (HEAD ** -0.5 * LOG2E)
        if bias is not None:
            s = s + bias[g]
        if keeps is not None:
            s = jnp.where(keeps[n] > 0, s, NEG)
        e = jnp.exp2(s - jnp.max(s, axis=0, keepdims=True))
        dens.append(jnp.sum(e, axis=0, keepdims=True))
        probs.append(e.astype(BF16))
    outs = [dot(t_ref[b, width + 128 * g:width + 128 * g + 128, :], p, 1, 0) for (n, b, g), p in zip(units, probs)]
    for (n, b, g), o, den in zip(units, outs, dens):
        inv = 1.0 / den
        gate = jax.nn.sigmoid(t_ref[b, 2 * width + 128 * g:2 * width + 128 * g + 128, :].astype(F32))
        parts = []
        for r in range(4):
            lanes = slice(length * r, length * r + length)
            parts.append(o[HEAD * r:HEAD * r + HEAD, lanes] * inv[:, lanes])
        o_ref[b, 128 * g:128 * g + 128, :] = (jnp.concatenate(parts, axis=0) * gate).astype(BF16)


def residual(x, update):
    return (x + update).astype(BF16)


def spread(row, lanes):
    return jnp.broadcast_to(row, (lanes, row.shape[1])).T


def widen(block, lanes):
    return jnp.concatenate([block] * (lanes // 128), axis=1)


def stage(stg, pair, first, second, ndev):
    rows = first.shape[0] // ndev
    off = pl.multiple_of(2 * rows * pair, 8)
    for d in range(ndev):
        both = jnp.concatenate([first[rows * d:rows * d + rows], second[rows * d:rows * d + rows]], axis=0)
        stg[d, pl.ds(off, 2 * rows), :] = both.astype(BF16)


def fill(work, ref):
    for t in range(work.shape[0]):
        work[t] = ref[..., 128 * t:128 * t + 128].astype(F32).reshape(work.shape[1:])


def take(work, start, count, stride):
    return jnp.concatenate([work.at[t][pl.ds(start, count, stride=stride), :] for t in range(work.shape[0])], axis=1)


def spread_bias(gath, gf, bias, transpose, mask_row):
    length, heads = gath.shape[0], gath.shape[1]
    gf[...] = gath[...].astype(F32)
    keep = None if mask_row is None else widen(spread(mask_row, 128), 4 * length)
    for g in range(heads // 4):
        parts = []
        for r in range(4):
            value = gf[:, 4 * g + r, :]
            parts.append(value.T if transpose else value)
        value = jnp.concatenate(parts, axis=1) * LOG2E
        if keep is not None:
            value = jnp.where(keep > 0, value, NEG)
        bias[g] = value


def bias_pieces(load, count, wb, store):
    def body(t, _):
        zl = [layer_norm(load(4 * t + n)) for n in range(4)]
        ps = [dot(wb, v, 1, 1) for v in zl]
        for n, v in enumerate(ps):
            store(4 * t + n, v.astype(BF16))
        return 0
    lax.fori_loop(0, count // 4, body, 0)


class Comm:
    def __init__(self, nd, sems):
        self.nd = nd
        self.me = lax.axis_index('dap')
        self.partner = self.me + 1 - 2 * lax.rem(self.me, 2)
        self.ssem, self.rsem, self.fsem, self.gsem = sems

    def copy(self, src, dst, send, recv, dev):
        return pltpu.make_async_remote_copy(src_ref=src, dst_ref=dst, send_sem=send, recv_sem=recv,
                                            device_id={'dap': dev}, device_id_type=MESH)

    def near(self, k, unit):
        off = ((k + 1) // 2) * (2 * lax.rem(k, 2) - 1)
        return lax.rem(self.me + self.nd + unit * off, self.nd)

    def barrier_signal(self):
        bar = pltpu.get_barrier_semaphore()

        def body(k, _):
            pl.semaphore_signal(bar, inc=1, device_id={'dap': lax.rem(self.me + k, self.nd)}, device_id_type=MESH)
            return 0
        lax.fori_loop(1, self.nd, body, 0)

    def barrier_wait(self):
        pl.semaphore_wait(pltpu.get_barrier_semaphore(), self.nd - 1)

    def await_bytes(self, ref, sem):
        pltpu.make_async_copy(ref, ref, sem).wait()

    def gather_start(self, buf, i):
        n = buf.shape[0] // self.nd
        own = buf.at[pl.ds(self.me * n, n)]

        def body(k, _):
            self.copy(own, own, self.ssem.at[i], self.gsem.at[i, k], self.near(k, 2)).start()
            return 0
        lax.fori_loop(1, self.nd // 2, body, 0)
        self.copy(own, own, self.ssem.at[i], self.gsem.at[i, 0], self.partner).start()

    def gather_finish(self, buf, i):
        n = buf.shape[0] // self.nd
        half = self.nd // 2

        def body(k, _):
            slot = buf.at[pl.ds(self.near(k, -2) * n, n)]
            self.await_bytes(slot, self.gsem.at[i, k])
            self.copy(slot, slot, self.fsem.at[i], self.rsem.at[i], self.partner).start()
            return 0
        lax.fori_loop(1, half, body, 0)
        self.await_bytes(buf.at[pl.ds(0, n)], self.gsem.at[i, 0])
        rest = buf.at[pl.ds(0, (half - 1) * n)]
        self.await_bytes(rest, self.rsem.at[i])
        self.await_bytes(rest, self.fsem.at[i])
        self.await_bytes(buf.at[pl.ds(0, half * n)], self.ssem.at[i])

    def slot(self, buf, off, part=None):
        n = buf.shape[0] // self.nd
        base = lax.rem(self.me + self.nd + 2 * off, self.nd) * n
        if part is None:
            return buf.at[pl.ds(base, n)]
        return buf.at[pl.ds(base + part * (n // 2), n // 2)]

    def relay(self, ref, i, recv, dev):
        self.copy(ref, ref, self.ssem.at[i], recv, dev).start()

    def relay_start(self, buf, i):
        own = self.slot(buf, 0)
        right, left = lax.rem(self.me + 2, self.nd), lax.rem(self.me + self.nd - 2, self.nd)
        self.relay(own, i, self.gsem.at[i, 0], right)
        self.relay(own, i, self.gsem.at[i, 4], left)
        self.relay(own, i, self.rsem.at[i], self.partner)

    def relay_step(self, buf, i, p):
        right, left = lax.rem(self.me + 2, self.nd), lax.rem(self.me + self.nd - 2, self.nd)
        for sign, base, dev, part in ((-1, 0, right, 0), (1, 4, left, 1)):
            ref = self.slot(buf, sign * p)
            self.await_bytes(ref, self.gsem.at[i, base + p - 1])
            on = self.slot(buf, sign * p, part) if p == self.nd // 4 - 1 else ref
            self.relay(on, i, self.gsem.at[i, base + p], dev)
            self.relay(ref, i, self.rsem.at[i], self.partner)

    def relay_finish(self, buf, i):
        n = buf.shape[0] // self.nd
        half = self.nd // 2
        far = self.slot(buf, self.nd // 4)
        for part in range(2):
            self.await_bytes(self.slot(buf, self.nd // 4, part), self.gsem.at[i, 4 * part + self.nd // 4 - 1])
        self.relay(far, i, self.rsem.at[i], self.partner)
        self.await_bytes(buf.at[pl.ds(0, half * n)], self.rsem.at[i])
        self.await_bytes(buf.at[pl.ds(0, (2 * half - 1) * n)], self.ssem.at[i])

    def swap_start(self, send, recv, i, off, rows):
        part = pl.ds(off, rows)

        def body(k, _):
            d = self.near(k, 1)
            self.copy(send.at[d, part], recv.at[self.me, part], self.ssem.at[i], self.rsem.at[i], d).start()
            return 0
        lax.fori_loop(1, self.nd, body, 0)
        pltpu.make_async_copy(send.at[self.me, part], recv.at[self.me, part], self.rsem.at[i]).start()

    def swap_finish(self, send, recv, i):
        self.await_bytes(recv, self.rsem.at[i])
        self.await_bytes(send.at[pl.ds(0, self.nd - 1)], self.ssem.at[i])


def kernel(names, outs, nd, refs):
    r = dict(zip(names, refs))
    class N:
        pass
    v = N()
    v.__dict__.update(r)
    sl, nr, cm = v.m.shape
    rl, _, cz = v.z.shape
    ns = sl * nd
    wm, wz = v.row_k.shape[2], v.ts_k.shape[2]
    gm, gz = wm // 128, wz // 128
    od = v.opm_i.shape[1] // 2
    comm = Comm(nd, (v.ssem, v.rsem, v.fsem, v.gsem))
    me = comm.me
    rows_m = sl * rl

    def store_piece(buf):
        def store(i, val):
            buf[me * rl + i] = val
        return store

    def loop(n, body):
        def step(t, _):
            body(t)
            return 0
        lax.fori_loop(0, n, step, 0)

    def row_project(load, b):
        loop(sl // 2, lambda t: project([load(2 * t), load(2 * t + 1)], v.row_t[b], v.row_k[b], v.rt, v.rk, 2 * t, None))

    def row_attend(load, b, finish):
        def body(t):
            for n in range(2):
                keep = widen(spread(v.mask_seq[pl.ds(2 * t + n, 1), :], 128), 4 * nr)
                core(v.rt, v.rk, v.ro, [2 * t + n], gm, v.rbias, [keep])
            ups = [dot(v.ro[2 * t + n], v.row_o[b], 0, 0) for n in range(2)]
            finish(t, [residual(load(2 * t + n), ups[n]) for n in range(2)])
        loop(sl // 2, body)

    def col_project(load, b):
        loop(rl // 4, lambda t: project([load(4 * t + n) for n in range(4)], v.col_t[b], v.col_k[b], v.ct, v.ck, 4 * t, None))

    def col_attend(first, count):
        def body(u):
            t = first + u
            rows = [2 * t, 2 * t + 1]
            keeps = [widen(spread(v.mask_col[pl.ds(i, 1), :], 128), 4 * ns) for i in rows]
            core(v.ct, v.ck, v.co, rows, gm, None, keeps)
        loop(count, body)

    def col_out(load, b, finish, loc, gat):
        def out(t):
            rows = [4 * t + n for n in range(4)]
            ups = [dot(v.co[i], v.col_o[b], 0, 0) for i in rows]
            new = [residual(load(i), u) for i, u in zip(rows, ups)]
            newf = [x.astype(F32) for x in new]
            finish(t, new, newf)
            ln = [layer_norm(x) for x in newf]
            acs = [dot(v.opm_i[b], x, 1, 1) for x in ln]
            for i, x in zip(rows, acs):
                ac = (x * v.mask_col[pl.ds(i, 1), :]).astype(BF16)
                a, c = ac[:od], ac[od:]
                loc[i] = a if b == 0 else c
                gat[me * rl + i] = c if b == 0 else a
        loop(rl // 4, out)

    def opm(loc, gat, b, load, wb, piece, between):
        v.gcol[...] = gat[...].astype(F32).reshape(v.gcol.shape)
        v.nrm[...] = dot(v.mask_col[...].astype(BF16), v.mask_b[...], 1, 0)

        def grow(t):
            left = loc[...].reshape(rl * od, ns)
            for n in range(4):
                g = 4 * t + n
                col = v.gcol[pl.ds(g, nr, stride=od), :].astype(BF16)
                x = dot(left, col, 1, 1).astype(BF16)
                off = pl.multiple_of(g * od, od)
                for i in range(rl):
                    v.xs[i, pl.ds(off, od), :] = x[od * i:od * i + od]
        loop(od // 4, grow)
        between()

        def fold(t):
            rows = [4 * t + n for n in range(4)]
            ups = [dot(v.opm_o[b], v.xs[i], 1, 0) for i in rows]
            ups = [u / (1e-3 + v.nrm[pl.ds(i, 1), :]) for i, u in zip(rows, ups)]
            ups = [u.T for u in ups]
            new = [residual(load(i), u) for i, u in zip(rows, ups)]
            for i, x in zip(rows, new):
                v.zc[i] = x
            ln = [layer_norm(x.astype(F32)) for x in new]
            ps = [dot(wb, x, 1, 1) for x in ln]
            for i, x in zip(rows, ps):
                piece[me * rl + i] = x.astype(BF16)
        loop(rl // 4, fold)

    def zload(i):
        return v.zc[i].astype(F32)

    def tri_project(wt, wk):
        loop(rl // 4, lambda t: project([zload(4 * t + n) for n in range(4)], wt, wk, v.tt, v.tk, 4 * t, v.kc[...]))

    def tri_attend(wo, finish):
        def body(t):
            core(v.tt, v.tk, v.to, [2 * t, 2 * t + 1], gz, v.tbias, None)
            rows = [2 * t, 2 * t + 1]
            ups = [dot(v.to[i], wo, 0, 0) for i in rows]
            finish(t, [residual(zload(i), u) for i, u in zip(rows, ups)])
        loop(rl // 2, body)

    def pair_pieces(t, pair, wb, piece):
        ps = [dot(wb, layer_norm(x.astype(F32)), 1, 1) for x in pair]
        for n, x in enumerate(ps):
            piece[me * rl + 2 * t + n] = x.astype(BF16)

    def send_pair(send, recv, i, rows, wb=None, piece=None):
        def finish(t, pair):
            stage(send, t, pair[0].astype(F32), pair[1].astype(F32), nd)
            comm.swap_start(send, recv, i, pl.multiple_of(2 * rows * t, 8), 2 * rows)
            if piece is not None:
                pair_pieces(t, pair, wb, piece)
        return finish

    def keep_pair(out, wb=None, piece=None):
        def finish(t, pair):
            out[2 * t], out[2 * t + 1] = pair
            if piece is not None:
                pair_pieces(t, pair, wb, piece)
        return finish

    def turn(recv):
        fill(v.zwork, recv)
        for b in range(rl):
            v.zc[b] = take(v.zwork, b, nr, rl).astype(BF16)

    comm.barrier_signal()
    bias_pieces(lambda i: v.z[i].astype(F32), rl, v.row_b[0], store_piece(v.g0))
    v.kc[...] = spread(v.mask_r[...], wz)
    comm.barrier_wait()
    comm.gather_start(v.g0, 0)
    mload = lambda s: v.m[s].astype(F32)
    row_project(mload, 0)
    comm.gather_finish(v.g0, 0)
    spread_bias(v.g0, v.gf, v.rbias, True, None)
    row_attend(mload, 0, send_pair(v.s0, v.r0, 8, rl))
    comm.swap_finish(v.s0, v.r0, 8)

    fill(v.mwork, v.r0)
    cload = lambda i: take(v.mwork, i, ns, rl)
    col_project(cload, 0)

    def keep_four(t, new, newf):
        for n, x in enumerate(new):
            v.mc[4 * t + n] = x
    col_attend(0, rl // 2)
    col_out(cload, 0, keep_four, v.loc0, v.g1)
    comm.relay_start(v.g1, 1)

    c2load = lambda i: v.mc[i].astype(F32)

    def send_four(t, new, newf):
        for n in range(2):
            stage(v.s1, 2 * t + n, newf[2 * n], newf[2 * n + 1], nd)
    col_project(c2load, 1)
    comm.relay_step(v.g1, 1, 1)
    col_attend(0, rl // 4)
    comm.relay_step(v.g1, 1, 2)
    col_attend(rl // 4, rl // 4)
    comm.relay_step(v.g1, 1, 3)
    col_out(c2load, 1, send_four, v.loc1, v.g2)
    comm.relay_finish(v.g1, 1)
    comm.relay_start(v.g2, 2)
    opm(v.loc0, v.g1, 0, lambda i: v.z[i].astype(F32), v.ts_b[0], v.g3, lambda: comm.relay_step(v.g2, 2, 1))
    comm.gather_start(v.g3, 3)
    comm.relay_step(v.g2, 2, 2)
    tri_project(v.ts_t[0], v.ts_k[0])
    comm.gather_finish(v.g3, 3)
    comm.relay_step(v.g2, 2, 3)
    spread_bias(v.g3, v.gf2, v.tbias, True, v.mask_r[...])
    tri_attend(v.ts_o[0], send_pair(v.s2, v.r2, 9, rl, v.te_b[0], v.g4))
    comm.gather_start(v.g4, 4)
    comm.swap_finish(v.s2, v.r2, 9)
    turn(v.r2)
    tri_project(v.te_t[0], v.te_k[0])
    comm.gather_finish(v.g4, 4)
    comm.swap_start(v.s1, v.r1, 10, 0, rows_m)
    spread_bias(v.g4, v.gf2, v.tbias, False, v.mask_r[...])
    tri_attend(v.te_o[0], keep_pair(v.zc, v.row_b[1], v.g5))

    comm.relay_finish(v.g2, 2)
    comm.relay_start(v.g5, 5)
    opm(v.loc1, v.g2, 1, zload, v.te_b[1], v.g6, lambda: comm.relay_step(v.g5, 5, 1))
    comm.gather_start(v.g6, 6)
    comm.relay_step(v.g5, 5, 2)
    comm.swap_finish(v.s1, v.r1, 10)
    fill(v.mwork, v.r1)
    rload = lambda s: take(v.mwork, s, nr, sl)
    row_project(rload, 1)
    comm.relay_step(v.g5, 5, 3)
    tri_project(v.te_t[1], v.te_k[1])
    comm.gather_finish(v.g6, 6)
    spread_bias(v.g6, v.gf2, v.tbias, True, v.mask_r[...])
    tri_attend(v.te_o[1], send_pair(v.s3, v.r3, 11, rl, v.ts_b[1], v.g7))
    comm.gather_start(v.g7, 7)
    comm.relay_finish(v.g5, 5)
    spread_bias(v.g5, v.gf, v.rbias, False, None)
    row_attend(rload, 1, keep_pair(v.m_out))
    comm.swap_finish(v.s3, v.r3, 11)
    turn(v.r3)
    tri_project(v.ts_t[1], v.ts_k[1])
    comm.gather_finish(v.g7, 7)
    spread_bias(v.g7, v.gf2, v.tbias, False, v.mask_r[...])
    tri_attend(v.ts_o[1], keep_pair(v.z_out))


def solution(mesh):
    nd = mesh.shape['dap']

    def local_step(m, z, msa_mask, res_mask, w_row_bias, w_row_in, w_row_out, w_col_in, w_col_out, w_opm_in, w_opm_out, w_ts_bias, w_ts_in, w_ts_out, w_te_bias, w_te_in, w_te_out):
        me = lax.axis_index('dap')
        sl, nr, cm = m.shape
        rl, _, cz = z.shape
        ns = sl * nd
        hm, ht = w_row_bias.shape[2], w_ts_bias.shape[2]
        wm, wz = hm * HEAD, ht * HEAD
        od = w_opm_in.shape[3]

        maskf = msa_mask.astype(F32)
        mask_seq = lax.dynamic_slice_in_dim(maskf, me * sl, sl, 0)
        mask_col = lax.dynamic_slice_in_dim(maskf, me * rl, rl, 1).T
        mask_b = msa_mask.astype(BF16)
        mask_r = res_mask.astype(F32)[None, :]

        def split(w, width):
            c = w.shape[1]
            w = w.reshape(2, c, 4, width)
            wt = jnp.stack([w[:, :, 0], w[:, :, 2], w[:, :, 3]], axis=1)
            return wt.transpose(0, 1, 3, 2).reshape(2, 3 * width, c), w[:, :, 1]

        row_t, row_k = split(w_row_in, wm)
        col_t, col_k = split(w_col_in, wm)
        ts_t, ts_k = split(w_ts_in, wz)
        te_t, te_k = split(w_te_in, wz)
        row_o = w_row_out.reshape(2, wm, cm)
        col_o = w_col_out.reshape(2, wm, cm)
        ts_o = w_ts_out.reshape(2, wz, cz)
        te_o = w_te_out.reshape(2, wz, cz)
        row_b = w_row_bias.transpose(0, 2, 1)
        ts_b = w_ts_bias.transpose(0, 2, 1)
        te_b = w_te_bias.transpose(0, 2, 1)
        opm_i = w_opm_in.reshape(2, cm, 2 * od).transpose(0, 2, 1)
        opm_o = jnp.stack([w_opm_out[0].transpose(2, 1, 0), w_opm_out[1].transpose(2, 0, 1)]).reshape(2, cz, od * od)

        ins = dict(m=m, z=z, mask_seq=mask_seq, mask_col=mask_col, mask_b=mask_b, mask_r=mask_r,
                   row_t=row_t, row_k=row_k, row_o=row_o, row_b=row_b, col_t=col_t, col_k=col_k, col_o=col_o,
                   ts_t=ts_t, ts_k=ts_k, ts_o=ts_o, ts_b=ts_b, te_t=te_t, te_k=te_k, te_o=te_o, te_b=te_b,
                   opm_i=opm_i, opm_o=opm_o)
        outs = dict(m_out=m, z_out=z)
        gm, gz = wm // 128, wz // 128
        xm, xz = (nd, sl * rl, cm), (nd, rl * rl, cz)
        grow, gtri, gopm = (nd * rl, hm, nr), (nd * rl, ht, nr), (nd * rl, od, ns)
        scratch = dict(
            s0=(xm, BF16), r0=(xm, BF16), s1=(xm, BF16), r1=(xm, BF16),
            s2=(xz, BF16), r2=(xz, BF16), s3=(xz, BF16), r3=(xz, BF16),
            g0=(grow, BF16), g5=(grow, BF16), g1=(gopm, BF16), g2=(gopm, BF16),
            g3=(gtri, BF16), g4=(gtri, BF16), g6=(gtri, BF16), g7=(gtri, BF16),
            gf=(grow, F32), gf2=(gtri, F32), rbias=((gm, nr, 4 * nr), F32), tbias=((gz, nr, 4 * nr), F32),
            mwork=((cm // 128, nd * sl * rl, 128), F32), zwork=((cz // 128, nr * rl, 128), F32),
            gcol=((nr * od, ns), F32), xs=((rl, od * od, nr), BF16), nrm=((rl, nr), F32), kc=((nr, wz), F32),
            rt=((sl, 3 * wm, nr), BF16), rk=((sl, nr, wm), BF16), ro=((sl, wm, nr), BF16),
            ct=((rl, 3 * wm, ns), BF16), ck=((rl, ns, wm), BF16), co=((rl, wm, ns), BF16),
            tt=((rl, 3 * wz, nr), BF16), tk=((rl, nr, wz), BF16), to=((rl, wz, nr), BF16),
            mc=((rl, ns, cm), BF16), zc=((rl, nr, cz), BF16), loc0=((rl, od, ns), BF16), loc1=((rl, od, ns), BF16))
        sems = dict(ssem=(12,), rsem=(12,), fsem=(8,), gsem=(8, nd // 2))
        names = list(ins) + list(outs) + list(scratch) + list(sems)
        return pl.pallas_call(
            lambda *refs: kernel(names, outs, nd, refs),
            out_shape=[jax.ShapeDtypeStruct(o.shape, o.dtype) for o in outs.values()],
            in_specs=[pl.BlockSpec(memory_space=pltpu.VMEM)] * len(ins),
            out_specs=[pl.BlockSpec(memory_space=pltpu.VMEM)] * len(outs),
            scratch_shapes=[pltpu.VMEM(*x) for x in scratch.values()] + [pltpu.SemaphoreType.DMA(x) for x in sems.values()],
            compiler_params=pltpu.CompilerParams(collective_id=0, has_side_effects=True, vmem_limit_bytes=67043328),
        )(*ins.values())

    in_specs = (P(('data', 'dap')), P(('data', 'dap')), P('data'), P('data')) + (P(),) * 13
    out_specs = (P(('data', 'dap')), P(('data', 'dap')))
    return jax.shard_map(local_step, mesh=mesh, in_specs=in_specs, out_specs=out_specs, check_vma=False)
```

```python
import functools

import jax
import jax.numpy as jnp
from jax import lax
from jax.experimental import pallas as pl
from jax.experimental.pallas import tpu as pltpu
from jax.sharding import PartitionSpec as P

F32 = jnp.float32
BF16 = jnp.bfloat16
LOG2E = 1.4426950408889634
NEG = -1e9 * LOG2E
HEAD = 32
MESH = pl.DeviceIdType.MESH


def dot(lhs, rhs, lc, rc):
    return lax.dot_general(lhs, rhs, (((lc,), (rc,)), ((), ())), preferred_element_type=F32)


def layer_norm(x):
    mean = jnp.mean(x, axis=-1, keepdims=True)
    cen = x - mean
    var = jnp.mean(cen * cen, axis=-1, keepdims=True)
    return (cen * lax.rsqrt(var + 1e-5)).astype(BF16)


def project(xs, w, t_ref, k_ref, first, kcol):
    width = w.shape[0] // 4
    xl = [layer_norm(x) for x in xs]
    for n, v in enumerate([dot(w[:width], v, 1, 1) for v in xl]):
        t_ref[first + n, 0:width] = v.astype(BF16)
    for n, v in enumerate([dot(w[2 * width:], v, 1, 1) for v in xl]):
        t_ref[first + n, width:3 * width] = v.astype(BF16)
    for n, v in enumerate([dot(v, w[width:2 * width], 1, 1) for v in xl]):
        if kcol is not None:
            v = v * kcol
        k_ref[first + n] = v.astype(BF16)


def diagonal(t, base, length):
    cols = []
    for r in range(4):
        parts = [t[base + HEAD * r:base + HEAD * r + HEAD]]
        if r > 0:
            parts.insert(0, jnp.zeros((HEAD * r, length), BF16))
        if r < 3:
            parts.append(jnp.zeros((HEAD * (3 - r), length), BF16))
        cols.append(jnp.concatenate(parts, axis=0))
    return jnp.concatenate(cols, axis=1)


def core(t_ref, k_ref, o_ref, rows, groups, bias, keeps):
    length = k_ref.shape[1]
    width = 128 * groups
    units = [(n, b, g) for n, b in enumerate(rows) for g in range(groups)]
    scores = []
    for n, b, g in units:
        t = t_ref[b, 128 * g:128 * g + 128, :]
        scores.append(dot(k_ref[b, :, 128 * g:128 * g + 128], diagonal(t, 0, length), 1, 0))
    yield
    probs = []
    dens = []
    for (n, b, g), s in zip(units, scores):
        s = s * (HEAD ** -0.5 * LOG2E)
        if bias is not None:
            s = s + bias[g]
        if keeps is not None:
            s = jnp.where(keeps[n] > 0, s, NEG)
        e = jnp.exp2(s - jnp.max(s, axis=0, keepdims=True))
        dens.append(jnp.sum(e, axis=0, keepdims=True))
        probs.append(e.astype(BF16))
    yield
    outs = [dot(t_ref[b, width + 128 * g:width + 128 * g + 128, :], p, 1, 0) for (n, b, g), p in zip(units, probs)]
    yield
    for (n, b, g), o, den in zip(units, outs, dens):
        inv = 1.0 / den
        gate = jax.nn.sigmoid(t_ref[b, 2 * width + 128 * g:2 * width + 128 * g + 128, :].astype(F32))
        parts = []
        for r in range(4):
            lanes = slice(length * r, length * r + length)
            parts.append(o[HEAD * r:HEAD * r + HEAD, lanes] * inv[:, lanes])
        o_ref[b, 128 * g:128 * g + 128, :] = (jnp.concatenate(parts, axis=0) * gate).astype(BF16)


def interleave(*gens):
    live = list(gens)
    while live:
        for gen in list(live):
            try:
                next(gen)
            except StopIteration:
                live.remove(gen)


def residual(x, update):
    return (x + update).astype(BF16)


def spread(row, lanes):
    return jnp.broadcast_to(row, (lanes, row.shape[1])).T


def widen(block, lanes):
    return jnp.concatenate([block] * (lanes // 128), axis=1)


def stage(stg, pair, first, second, ndev):
    rows = first.shape[0] // ndev
    off = pl.multiple_of(2 * rows * pair, 8)
    for d in range(ndev):
        both = jnp.concatenate([first[rows * d:rows * d + rows], second[rows * d:rows * d + rows]], axis=0)
        stg[d, pl.ds(off, 2 * rows), :] = both.astype(BF16)


def fill(work, ref):
    for t in range(work.shape[0]):
        work[t] = ref[..., 128 * t:128 * t + 128].astype(F32).reshape(work.shape[1:])


def take(work, start, count, stride):
    return jnp.concatenate([work.at[t][pl.ds(start, count, stride=stride), :] for t in range(work.shape[0])], axis=1)


def spread_bias(gath, gf, bias, transpose, mask_row):
    length, heads = gath.shape[0], gath.shape[1]
    gf[...] = gath[...].astype(F32)
    keep = None if mask_row is None else widen(spread(mask_row, 128), 4 * length)
    for g in range(heads // 4):
        parts = []
        for r in range(4):
            value = gf[:, 4 * g + r, :]
            parts.append(value.T if transpose else value)
        value = jnp.concatenate(parts, axis=1) * LOG2E
        if keep is not None:
            value = jnp.where(keep > 0, value, NEG)
        bias[g] = value


def bias_pieces(load, count, wb, store):
    def body(t, _):
        zl = [layer_norm(load(4 * t + n)) for n in range(4)]
        ps = [dot(wb, v, 1, 1) for v in zl]
        for n, v in enumerate(ps):
            store(4 * t + n, v.astype(BF16))
        return 0
    lax.fori_loop(0, count // 4, body, 0)


class Comm:
    def __init__(self, nd, sems):
        self.nd = nd
        self.me = lax.axis_index('dap')
        self.partner = self.me + 1 - 2 * lax.rem(self.me, 2)
        self.ssem, self.rsem, self.fsem, self.gsem = sems

    def copy(self, src, dst, send, recv, dev):
        return pltpu.make_async_remote_copy(src_ref=src, dst_ref=dst, send_sem=send, recv_sem=recv,
                                            device_id={'dap': dev}, device_id_type=MESH)

    def near(self, k, unit):
        off = ((k + 1) // 2) * (2 * lax.rem(k, 2) - 1)
        return lax.rem(self.me + self.nd + unit * off, self.nd)

    def barrier_signal(self):
        bar = pltpu.get_barrier_semaphore()

        def body(k, _):
            pl.semaphore_signal(bar, inc=1, device_id={'dap': lax.rem(self.me + k, self.nd)}, device_id_type=MESH)
            return 0
        lax.fori_loop(1, self.nd, body, 0)

    def barrier_wait(self):
        pl.semaphore_wait(pltpu.get_barrier_semaphore(), self.nd - 1)

    def await_bytes(self, ref, sem):
        pltpu.make_async_copy(ref, ref, sem).wait()

    def gather_start(self, buf, i):
        n = buf.shape[0] // self.nd
        own = buf.at[pl.ds(self.me * n, n)]

        def body(k, _):
            self.copy(own, own, self.ssem.at[i], self.gsem.at[i, k], self.near(k, 2)).start()
            return 0
        lax.fori_loop(1, self.nd // 2, body, 0)
        self.copy(own, own, self.ssem.at[i], self.gsem.at[i, 0], self.partner).start()

    def gather_finish(self, buf, i):
        n = buf.shape[0] // self.nd
        half = self.nd // 2

        def body(k, _):
            slot = buf.at[pl.ds(self.near(k, -2) * n, n)]
            self.await_bytes(slot, self.gsem.at[i, k])
            self.copy(slot, slot, self.fsem.at[i], self.rsem.at[i], self.partner).start()
            return 0
        lax.fori_loop(1, half, body, 0)
        self.await_bytes(buf.at[pl.ds(0, n)], self.gsem.at[i, 0])
        rest = buf.at[pl.ds(0, (half - 1) * n)]
        self.await_bytes(rest, self.rsem.at[i])
        self.await_bytes(rest, self.fsem.at[i])
        self.await_bytes(buf.at[pl.ds(0, half * n)], self.ssem.at[i])

    def slot(self, buf, off, part=None):
        n = buf.shape[0] // self.nd
        base = lax.rem(self.me + self.nd + 2 * off, self.nd) * n
        if part is None:
            return buf.at[pl.ds(base, n)]
        return buf.at[pl.ds(base + part * (n // 2), n // 2)]

    def relay(self, ref, i, recv, dev):
        self.copy(ref, ref, self.ssem.at[i], recv, dev).start()

    def relay_start(self, buf, i):
        own = self.slot(buf, 0)
        right, left = lax.rem(self.me + 2, self.nd), lax.rem(self.me + self.nd - 2, self.nd)
        self.relay(own, i, self.gsem.at[i, 0], right)
        self.relay(own, i, self.gsem.at[i, 4], left)
        self.relay(own, i, self.rsem.at[i], self.partner)

    def relay_step(self, buf, i, p):
        right, left = lax.rem(self.me + 2, self.nd), lax.rem(self.me + self.nd - 2, self.nd)
        for sign, base, dev, part in ((-1, 0, right, 0), (1, 4, left, 1)):
            ref = self.slot(buf, sign * p)
            self.await_bytes(ref, self.gsem.at[i, base + p - 1])
            on = self.slot(buf, sign * p, part) if p == self.nd // 4 - 1 else ref
            self.relay(on, i, self.gsem.at[i, base + p], dev)
            self.relay(ref, i, self.rsem.at[i], self.partner)

    def relay_finish(self, buf, i):
        n = buf.shape[0] // self.nd
        half = self.nd // 2
        far = self.slot(buf, self.nd // 4)
        for part in range(2):
            self.await_bytes(self.slot(buf, self.nd // 4, part), self.gsem.at[i, 4 * part + self.nd // 4 - 1])
        self.relay(far, i, self.rsem.at[i], self.partner)
        self.await_bytes(buf.at[pl.ds(0, half * n)], self.rsem.at[i])
        self.await_bytes(buf.at[pl.ds(0, (2 * half - 1) * n)], self.ssem.at[i])

    def swap_start(self, send, recv, i, off, rows):
        part = pl.ds(off, rows)

        for k in range(1, self.nd):
            off = (k + 1) // 2 if k % 2 else -(k // 2)
            d = lax.rem(self.me + self.nd + off, self.nd)
            self.copy(send.at[d, part], recv.at[self.me, part], self.ssem.at[i], self.rsem.at[i], d).start()
        pltpu.make_async_copy(send.at[self.me, part], recv.at[self.me, part], self.rsem.at[i]).start()

    def swap_finish(self, send, recv, i):
        self.await_bytes(recv, self.rsem.at[i])
        self.await_bytes(send.at[pl.ds(0, self.nd - 1)], self.ssem.at[i])


def kernel(names, outs, nd, refs):
    r = dict(zip(names, refs))
    class N:
        pass
    v = N()
    v.__dict__.update(r)
    sl, nr, cm = v.m.shape
    rl, _, cz = v.z.shape
    ns = sl * nd
    wm, wz = v.row_w.shape[1] // 4, v.ts_w.shape[1] // 4
    gm, gz = wm // 128, wz // 128
    od = v.opm_i.shape[1] // 2
    comm = Comm(nd, (v.ssem, v.rsem, v.fsem, v.gsem))
    me = comm.me
    rows_m = sl * rl

    def store_piece(buf):
        def store(i, val):
            buf[me * rl + i] = val
        return store

    def loop(n, body):
        def step(t, _):
            body(t)
            return 0
        lax.fori_loop(0, n, step, 0)

    def row_project(load, b):
        loop(sl // 2, lambda t: project([load(2 * t), load(2 * t + 1)], v.row_w.at[b], v.rt, v.rk, 2 * t, None))

    def row_attend(load, b, finish):
        def attend(s):
            keep = widen(spread(v.mask_seq[pl.ds(s, 1), :], 128), 4 * nr)
            return core(v.rt, v.rk, v.ro, [s], gm, v.rbias, [keep])

        def back(t):
            ups = [dot(v.ro[2 * t + n], v.row_o[b], 0, 0) for n in range(2)]
            yield
            yield from finish(t, [residual(load(2 * t + n), ups[n]) for n in range(2)])

        def body(u):
            interleave(back(u), attend(2 * u + 2))
            interleave(attend(2 * u + 3))
        interleave(attend(0))
        interleave(attend(1))
        loop(sl // 2 - 1, body)
        interleave(back(sl // 2 - 1))

    def col_project(load, b):
        loop(rl // 4, lambda t: project([load(4 * t + n) for n in range(4)], v.col_w.at[b], v.ct, v.ck, 4 * t, None))

    def col_attend(first, count):
        def body(u):
            t = first + u
            rows = [2 * t, 2 * t + 1]
            keeps = [widen(spread(v.mask_col[pl.ds(i, 1), :], 128), 4 * ns) for i in rows]
            interleave(core(v.ct, v.ck, v.co, rows, gm, None, keeps))
        loop(count, body)

    def col_out(load, b, finish, loc, gat):
        def out(t):
            rows = [4 * t + n for n in range(4)]
            ups = [dot(v.co[i], v.col_o[b], 0, 0) for i in rows]
            new = [residual(load(i), u) for i, u in zip(rows, ups)]
            newf = [x.astype(F32) for x in new]
            finish(t, new, newf)
            ln = [layer_norm(x) for x in newf]
            acs = [dot(v.opm_i[b], x, 1, 1) for x in ln]
            for i, x in zip(rows, acs):
                ac = (x * v.mask_col[pl.ds(i, 1), :]).astype(BF16)
                a, c = ac[:od], ac[od:]
                loc[i] = a if b == 0 else c
                gat[me * rl + i] = c if b == 0 else a
        loop(rl // 4, out)

    def opm(loc, gat, b, load, wb, piece, between):
        v.gcol[...] = gat[...].astype(F32).reshape(v.gcol.shape)
        v.nrm[...] = dot(v.mask_col[...].astype(BF16), v.msa_mask[...].astype(F32).astype(BF16), 1, 0)

        def grow(t):
            left = loc[...].reshape(rl * od, ns)
            for n in range(4):
                g = 4 * t + n
                col = v.gcol[pl.ds(g, nr, stride=od), :].astype(BF16)
                x = dot(left, col, 1, 1).astype(BF16)
                off = pl.multiple_of(g * od, od)
                for i in range(rl):
                    v.xs[i, pl.ds(off, od), :] = x[od * i:od * i + od]
        loop(od // 4, grow)
        between()

        def fold(t):
            rows = [4 * t + n for n in range(4)]
            ups = [dot(v.opm_w[b], v.xs[i], 1, 0) for i in rows]
            ups = [u / (1e-3 + v.nrm[pl.ds(i, 1), :]) for i, u in zip(rows, ups)]
            ups = [u.T for u in ups]
            new = [residual(load(i), u) for i, u in zip(rows, ups)]
            for i, x in zip(rows, new):
                v.zc[i] = x
            ln = [layer_norm(x.astype(F32)) for x in new]
            ps = [dot(wb, x, 1, 1) for x in ln]
            for i, x in zip(rows, ps):
                piece[me * rl + i] = x.astype(BF16)
        loop(rl // 4, fold)

    def zload(i):
        return v.zc[i].astype(F32)

    def tri_project(w):
        loop(rl // 4, lambda t: project([zload(4 * t + n) for n in range(4)], w, v.tt, v.tk, 4 * t, v.kc[...]))

    def tri_attend(wo, finish):
        def attend(t):
            return core(v.tt, v.tk, v.to, [4 * t + n for n in range(4)], gz, v.tbias, None)

        def back(t):
            rows = [4 * t + n for n in range(4)]
            ups = [dot(v.to[i], wo, 0, 0) for i in rows]
            yield
            yield from finish(t, [residual(zload(i), u) for i, u in zip(rows, ups)])

        interleave(attend(0))
        loop(rl // 4 - 1, lambda u: interleave(back(u), attend(u + 1)))
        interleave(back(rl // 4 - 1))

    def pieces(t, new, wb, piece):
        ln = [layer_norm(x.astype(F32)) for x in new]
        yield
        ps = [dot(wb, x, 1, 1) for x in ln]
        for n, x in enumerate(ps):
            piece[me * rl + len(new) * t + n] = x.astype(BF16)

    def send(out, recv, i, rows, wb=None, piece=None):
        def finish(t, new):
            half = len(new) // 2
            for n in range(half):
                stage(out, half * t + n, new[2 * n].astype(F32), new[2 * n + 1].astype(F32), nd)
            count = len(new) * rows
            comm.swap_start(out, recv, i, pl.multiple_of(count * t, 8), count)
            if piece is not None:
                yield from pieces(t, new, wb, piece)
            else:
                yield
        return finish

    def keep(out, wb=None, piece=None):
        def finish(t, new):
            for n, x in enumerate(new):
                out[len(new) * t + n] = x
            if piece is not None:
                yield from pieces(t, new, wb, piece)
            else:
                yield
        return finish

    def turn(recv):
        fill(v.zwork, recv)
        for b in range(rl):
            v.zc[b] = take(v.zwork, b, nr, rl).astype(BF16)

    def mask_r():
        return v.res_mask[...].astype(F32)

    def prepare():
        v.mask_t[...] = v.msa_mask[...].astype(F32).T
        v.mask_seq[...] = v.msa_mask[pl.ds(pl.multiple_of(me * sl, sl), sl), :].astype(F32)
        for i in range(rl):
            v.mask_col[pl.ds(i, 1), :] = v.mask_t[pl.ds(me * rl + i, 1), :]
        v.kc[...] = spread(mask_r(), wz)
        size = od * od
        v.gcol[0:size] = v.opm_o[0].astype(F32)
        for q in range(od):
            v.gcol[size + od * q:size + od * q + od] = v.gcol[pl.ds(q, od, stride=od), :]
        for j in range(size // 128):
            v.opm_w[0, :, 128 * j:128 * j + 128] = v.gcol[size + 128 * j:size + 128 * j + 128].T.astype(BF16)
            v.opm_w[1, :, 128 * j:128 * j + 128] = v.opm_o[1, 128 * j:128 * j + 128, :].astype(F32).T.astype(BF16)

    comm.barrier_signal()
    bias_pieces(lambda i: v.z[i].astype(F32), rl, v.row_b[0], store_piece(v.g0))
    comm.barrier_wait()
    comm.gather_start(v.g0, 0)
    mload = lambda s: v.m[s].astype(F32)
    row_project(mload, 0)
    prepare()
    comm.gather_finish(v.g0, 0)
    spread_bias(v.g0, v.gf, v.rbias, True, None)
    row_attend(mload, 0, send(v.s0, v.r0, 8, rl))
    comm.swap_finish(v.s0, v.r0, 8)

    fill(v.mwork, v.r0)
    cload = lambda i: take(v.mwork, i, ns, rl)
    col_project(cload, 0)

    def keep_four(t, new, newf):
        for n, x in enumerate(new):
            v.mc[4 * t + n] = x
    col_attend(0, rl // 2)
    col_out(cload, 0, keep_four, v.loc0, v.g1)
    comm.relay_start(v.g1, 1)

    c2load = lambda i: v.mc[i].astype(F32)

    def send_four(t, new, newf):
        for n in range(2):
            stage(v.s1, 2 * t + n, newf[2 * n], newf[2 * n + 1], nd)
    col_project(c2load, 1)
    comm.relay_step(v.g1, 1, 1)
    col_attend(0, rl // 4)
    comm.relay_step(v.g1, 1, 2)
    col_attend(rl // 4, rl // 4)
    comm.relay_step(v.g1, 1, 3)
    col_out(c2load, 1, send_four, v.loc1, v.g2)
    comm.relay_finish(v.g1, 1)
    comm.relay_start(v.g2, 2)
    opm(v.loc0, v.g1, 0, lambda i: v.z[i].astype(F32), v.ts_b[0], v.g3, lambda: comm.relay_step(v.g2, 2, 1))
    comm.gather_start(v.g3, 3)
    comm.relay_step(v.g2, 2, 2)
    tri_project(v.ts_w.at[0])
    comm.gather_finish(v.g3, 3)
    comm.relay_step(v.g2, 2, 3)
    spread_bias(v.g3, v.gf2, v.tbias, True, mask_r())
    tri_attend(v.ts_o[0], send(v.s2, v.r2, 9, rl, v.te_b[0], v.g4))
    comm.gather_start(v.g4, 4)
    comm.swap_finish(v.s2, v.r2, 9)
    turn(v.r2)
    tri_project(v.te_w.at[0])
    comm.gather_finish(v.g4, 4)
    comm.swap_start(v.s1, v.r1, 10, 0, rows_m)
    spread_bias(v.g4, v.gf2, v.tbias, False, mask_r())
    tri_attend(v.te_o[0], keep(v.zc, v.row_b[1], v.g5))

    comm.relay_finish(v.g2, 2)
    comm.relay_start(v.g5, 5)
    opm(v.loc1, v.g2, 1, zload, v.te_b[1], v.g6, lambda: comm.relay_step(v.g5, 5, 1))
    comm.gather_start(v.g6, 6)
    comm.relay_step(v.g5, 5, 2)
    comm.swap_finish(v.s1, v.r1, 10)
    fill(v.mwork, v.r1)
    rload = lambda s: take(v.mwork, s, nr, sl)
    row_project(rload, 1)
    comm.relay_step(v.g5, 5, 3)
    tri_project(v.te_w.at[1])
    comm.gather_finish(v.g6, 6)
    spread_bias(v.g6, v.gf2, v.tbias, True, mask_r())
    tri_attend(v.te_o[1], send(v.s3, v.r3, 11, rl, v.ts_b[1], v.g7))
    comm.gather_start(v.g7, 7)
    comm.relay_finish(v.g5, 5)
    spread_bias(v.g5, v.gf, v.rbias, False, None)
    row_attend(rload, 1, keep(v.m_out))
    comm.swap_finish(v.s3, v.r3, 11)
    turn(v.r3)
    tri_project(v.ts_w.at[1])
    comm.gather_finish(v.g7, 7)
    spread_bias(v.g7, v.gf2, v.tbias, False, mask_r())
    tri_attend(v.ts_o[1], keep(v.z_out))


def solution(mesh):
    nd = mesh.shape['dap']

    def local_step(m, z, msa_mask, res_mask, w_row_bias, w_row_in, w_row_out, w_col_in, w_col_out, w_opm_in, w_opm_out, w_ts_bias, w_ts_in, w_ts_out, w_te_bias, w_te_in, w_te_out):
        sl, nr, cm = m.shape
        rl, _, cz = z.shape
        ns = sl * nd
        hm, ht = w_row_bias.shape[2], w_ts_bias.shape[2]
        wm, wz = hm * HEAD, ht * HEAD
        od = w_opm_in.shape[3]

        def rows_of(w):
            return jnp.moveaxis(w, 1, -1).reshape(2, -1, w.shape[1])

        ins = dict(m=m, z=z, msa_mask=msa_mask, res_mask=res_mask[None, :],
                   row_w=rows_of(w_row_in), row_o=w_row_out.reshape(2, wm, cm), row_b=rows_of(w_row_bias),
                   col_w=rows_of(w_col_in), col_o=w_col_out.reshape(2, wm, cm),
                   ts_w=rows_of(w_ts_in), ts_o=w_ts_out.reshape(2, wz, cz), ts_b=rows_of(w_ts_bias),
                   te_w=rows_of(w_te_in), te_o=w_te_out.reshape(2, wz, cz), te_b=rows_of(w_te_bias),
                   opm_i=rows_of(w_opm_in), opm_o=w_opm_out.reshape(2, od * od, cz))
        outs = dict(m_out=m, z_out=z)
        gm, gz = wm // 128, wz // 128
        xm, xz = (nd, sl * rl, cm), (nd, rl * rl, cz)
        grow, gtri, gopm = (nd * rl, hm, nr), (nd * rl, ht, nr), (nd * rl, od, ns)
        scratch = dict(
            s0=(xm, BF16), r0=(xm, BF16), s1=(xm, BF16), r1=(xm, BF16),
            s2=(xz, BF16), r2=(xz, BF16), s3=(xz, BF16), r3=(xz, BF16),
            g0=(grow, BF16), g5=(grow, BF16), g1=(gopm, BF16), g2=(gopm, BF16),
            g3=(gtri, BF16), g4=(gtri, BF16), g6=(gtri, BF16), g7=(gtri, BF16),
            gf=(grow, F32), gf2=(gtri, F32), rbias=((gm, nr, 4 * nr), F32), tbias=((gz, nr, 4 * nr), F32),
            mwork=((cm // 128, nd * sl * rl, 128), F32), zwork=((cz // 128, nr * rl, 128), F32),
            gcol=((nr * od, ns), F32), xs=((rl, od * od, nr), BF16), nrm=((rl, nr), F32), kc=((nr, wz), F32),
            rt=((sl, 3 * wm, nr), BF16), rk=((sl, nr, wm), BF16), ro=((sl, wm, nr), BF16),
            ct=((rl, 3 * wm, ns), BF16), ck=((rl, ns, wm), BF16), co=((rl, wm, ns), BF16),
            tt=((rl, 3 * wz, nr), BF16), tk=((rl, nr, wz), BF16), to=((rl, wz, nr), BF16),
            mask_t=((nr, ns), F32), mask_seq=((sl, nr), F32), mask_col=((rl, ns), F32), opm_w=((2, cz, od * od), BF16),
            mc=((rl, ns, cm), BF16), zc=((rl, nr, cz), BF16), loc0=((rl, od, ns), BF16), loc1=((rl, od, ns), BF16))
        sems = dict(ssem=(12,), rsem=(12,), fsem=(8,), gsem=(8, nd // 2))
        names = list(ins) + list(outs) + list(scratch) + list(sems)
        return pl.pallas_call(
            lambda *refs: kernel(names, outs, nd, refs),
            out_shape=[jax.ShapeDtypeStruct(o.shape, o.dtype) for o in outs.values()],
            in_specs=[pl.BlockSpec(memory_space=pltpu.VMEM)] * len(ins),
            out_specs=[pl.BlockSpec(memory_space=pltpu.VMEM)] * len(outs),
            scratch_shapes=[pltpu.VMEM(*x) for x in scratch.values()] + [pltpu.SemaphoreType.DMA(x) for x in sems.values()],
            compiler_params=pltpu.CompilerParams(collective_id=0, has_side_effects=True, vmem_limit_bytes=67043328),
        )(*ins.values())

    in_specs = (P(('data', 'dap')), P(('data', 'dap')), P('data'), P('data')) + (P(),) * 13
    out_specs = (P(('data', 'dap')), P(('data', 'dap')))
    return jax.shard_map(local_step, mesh=mesh, in_specs=in_specs, out_specs=out_specs, check_vma=False)
```

```python
import functools

import jax
import jax.numpy as jnp
from jax import lax
from jax.experimental import pallas as pl
from jax.experimental.pallas import tpu as pltpu
from jax.sharding import PartitionSpec as P

F32 = jnp.float32
BF16 = jnp.bfloat16
LOG2E = 1.4426950408889634
NEG = -1e9 * LOG2E
HEAD = 32
MESH = pl.DeviceIdType.MESH


def dot(lhs, rhs, lc, rc):
    return lax.dot_general(lhs, rhs, (((lc,), (rc,)), ((), ())), preferred_element_type=F32)


def layer_norm(x):
    mean = jnp.mean(x, axis=-1, keepdims=True)
    cen = x - mean
    var = jnp.mean(cen * cen, axis=-1, keepdims=True)
    return (cen * lax.rsqrt(var + 1e-5)).astype(BF16)


def project(xs, w, t_ref, k_ref, first, kcol):
    width = w.shape[0] // 4
    xl = [layer_norm(x) for x in xs]
    for n, v in enumerate([dot(w[:width], v, 1, 1) for v in xl]):
        t_ref[first + n, 0:width] = v.astype(BF16)
    for n, v in enumerate([dot(w[2 * width:], v, 1, 1) for v in xl]):
        t_ref[first + n, width:3 * width] = v.astype(BF16)
    for n, v in enumerate([dot(v, w[width:2 * width], 1, 1) for v in xl]):
        if kcol is not None:
            v = v * kcol
        k_ref[first + n] = v.astype(BF16)


def diagonal(t, base, length):
    cols = []
    for r in range(4):
        parts = [t[base + HEAD * r:base + HEAD * r + HEAD]]
        if r > 0:
            parts.insert(0, jnp.zeros((HEAD * r, length), BF16))
        if r < 3:
            parts.append(jnp.zeros((HEAD * (3 - r), length), BF16))
        cols.append(jnp.concatenate(parts, axis=0))
    return jnp.concatenate(cols, axis=1)


def core(t_ref, k_ref, o_ref, rows, groups, bias, keeps):
    length = k_ref.shape[1]
    width = 128 * groups
    units = [(n, b, g) for n, b in enumerate(rows) for g in range(groups)]
    scores = []
    for n, b, g in units:
        t = t_ref[b, 128 * g:128 * g + 128, :]
        scores.append(dot(k_ref[b, :, 128 * g:128 * g + 128], diagonal(t, 0, length), 1, 0))
    yield
    probs = []
    dens = []
    for (n, b, g), s in zip(units, scores):
        s = s * (HEAD ** -0.5 * LOG2E)
        if bias is not None:
            s = s + bias[g]
        if keeps is not None:
            s = jnp.where(keeps[n] > 0, s, NEG)
        e = jnp.exp2(s - jnp.max(s, axis=0, keepdims=True))
        dens.append(jnp.sum(e, axis=0, keepdims=True))
        probs.append(e.astype(BF16))
    yield
    outs = [dot(t_ref[b, width + 128 * g:width + 128 * g + 128, :], p, 1, 0) for (n, b, g), p in zip(units, probs)]
    yield
    for (n, b, g), o, den in zip(units, outs, dens):
        inv = 1.0 / den
        gate = jax.nn.sigmoid(t_ref[b, 2 * width + 128 * g:2 * width + 128 * g + 128, :].astype(F32))
        parts = []
        for r in range(4):
            lanes = slice(length * r, length * r + length)
            parts.append(o[HEAD * r:HEAD * r + HEAD, lanes] * inv[:, lanes])
        o_ref[b, 128 * g:128 * g + 128, :] = (jnp.concatenate(parts, axis=0) * gate).astype(BF16)


def interleave(*gens):
    live = list(gens)
    while live:
        for gen in list(live):
            try:
                next(gen)
            except StopIteration:
                live.remove(gen)


def residual(x, update):
    return (x + update).astype(BF16)


def spread(row, lanes):
    return jnp.broadcast_to(row, (lanes, row.shape[1])).T


def widen(block, lanes):
    return jnp.concatenate([block] * (lanes // 128), axis=1)


def stage(stg, pair, first, second, ndev):
    rows = first.shape[0] // ndev
    off = pl.multiple_of(2 * rows * pair, 8)
    for d in range(ndev):
        both = jnp.concatenate([first[rows * d:rows * d + rows], second[rows * d:rows * d + rows]], axis=0)
        stg[d, pl.ds(off, 2 * rows), :] = both.astype(BF16)


def fill(work, ref):
    for t in range(work.shape[0]):
        work[t] = ref[..., 128 * t:128 * t + 128].astype(F32).reshape(work.shape[1:])


def take(work, start, count, stride):
    return jnp.concatenate([work.at[t][pl.ds(start, count, stride=stride), :] for t in range(work.shape[0])], axis=1)


def spread_bias(gath, gf, bias, transpose, mask_row):
    length, heads = gath.shape[0], gath.shape[1]
    gf[...] = gath[...].astype(F32)
    keep = None if mask_row is None else widen(spread(mask_row, 128), 4 * length)
    for g in range(heads // 4):
        parts = []
        for r in range(4):
            value = gf[:, 4 * g + r, :]
            parts.append(value.T if transpose else value)
        value = jnp.concatenate(parts, axis=1) * LOG2E
        if keep is not None:
            value = jnp.where(keep > 0, value, NEG)
        bias[g] = value


def bias_pieces(load, count, wb, store):
    def body(t, _):
        zl = [layer_norm(load(4 * t + n)) for n in range(4)]
        ps = [dot(wb, v, 1, 1) for v in zl]
        for n, v in enumerate(ps):
            store(4 * t + n, v.astype(BF16))
        return 0
    lax.fori_loop(0, count // 4, body, 0)


class Comm:
    def __init__(self, nd, sems):
        self.nd = nd
        self.me = lax.axis_index('dap')
        self.partner = self.me + 1 - 2 * lax.rem(self.me, 2)
        self.ssem, self.rsem, self.fsem, self.gsem, self.xsem = sems

    def copy(self, src, dst, send, recv, dev):
        return pltpu.make_async_remote_copy(src_ref=src, dst_ref=dst, send_sem=send, recv_sem=recv,
                                            device_id={'dap': dev}, device_id_type=MESH)

    def near(self, k, unit):
        off = ((k + 1) // 2) * (2 * lax.rem(k, 2) - 1)
        return lax.rem(self.me + self.nd + unit * off, self.nd)

    def barrier_signal(self):
        bar = pltpu.get_barrier_semaphore()

        def body(k, _):
            pl.semaphore_signal(bar, inc=1, device_id={'dap': lax.rem(self.me + k, self.nd)}, device_id_type=MESH)
            return 0
        lax.fori_loop(1, self.nd, body, 0)

    def barrier_wait(self):
        pl.semaphore_wait(pltpu.get_barrier_semaphore(), self.nd - 1)

    def await_bytes(self, ref, sem):
        pltpu.make_async_copy(ref, ref, sem).wait()

    def at(self, chips, same=True):
        base = self.me if same else self.partner
        return lax.rem(base + self.nd + 2 * chips, self.nd)

    def slot(self, buf, chips, start=0, count=None):
        n = buf.shape[0] // self.nd
        return buf.at[pl.ds(self.at(chips) * n + start, n if count is None else count)]

    def gather_start(self, buf, i):
        own = self.slot(buf, 0)

        def body(k, _):
            self.copy(own, own, self.ssem.at[i], self.gsem.at[i, k, 0], self.near(k, 2)).start()
            return 0
        lax.fori_loop(1, self.nd // 2 - 1, body, 0)
        self.copy(own, own, self.ssem.at[i], self.gsem.at[i, 0, 0], self.partner).start()

    def gather_finish(self, buf, i):
        n = buf.shape[0] // self.nd
        half = self.nd // 2
        far = self.nd // 4

        def across(ref):
            self.copy(ref, ref, self.fsem.at[i], self.rsem.at[i], self.partner).start()

        def body(k, _):
            slot = buf.at[pl.ds(self.near(k, -2) * n, n)]
            self.await_bytes(slot, self.gsem.at[i, k, 0])
            across(slot)
            return 0
        lax.fori_loop(1, half - 3, body, 0)
        for part, sign in ((0, 1), (1, -1)):
            self.await_bytes(self.slot(buf, sign * (1 - far)), self.gsem.at[i, half - 3 + part, 0])
            on = self.slot(buf, sign * (1 - far), part * (n // 2), n // 2)
            self.copy(on, on, self.fsem.at[i], self.gsem.at[i, half - 1 + part, 0], self.at(sign)).start()
            across(self.slot(buf, sign * (1 - far)))
        for part in range(2):
            self.await_bytes(self.slot(buf, far, part * (n // 2), n // 2), self.gsem.at[i, half - 1 + part, 0])
        across(self.slot(buf, far))
        self.await_bytes(buf.at[pl.ds(0, n)], self.gsem.at[i, 0, 0])
        rest = buf.at[pl.ds(0, (half - 1) * n)]
        self.await_bytes(rest, self.rsem.at[i])
        self.await_bytes(buf.at[pl.ds(0, half * n)], self.fsem.at[i])
        self.await_bytes(rest, self.ssem.at[i])

    def relay(self, ref, i, recv, dev):
        self.copy(ref, ref, self.ssem.at[i], recv, dev).start()

    def relay_start(self, buf, i, c=0, nc=1):
        m = buf.shape[0] // self.nd // nc
        own = self.slot(buf, 0, c * m, m)
        self.relay(own, i, self.gsem.at[i, 0, c], self.at(1))
        self.relay(own, i, self.gsem.at[i, 4, c], self.at(-1))
        self.relay(own, i, self.rsem.at[i], self.partner)

    def relay_step(self, buf, i, p, c=0, nc=1):
        m = buf.shape[0] // self.nd // nc
        for part, sign in ((0, 1), (1, -1)):
            ref = self.slot(buf, -sign * p, c * m, m)
            self.await_bytes(ref, self.gsem.at[i, 4 * part + p - 1, c])
            on = self.slot(buf, -sign * p, c * m + part * (m // 2), m // 2) if p == self.nd // 4 - 1 else ref
            self.relay(on, i, self.gsem.at[i, 4 * part + p, c], self.at(sign))
            self.relay(ref, i, self.rsem.at[i], self.partner)

    def relay_finish(self, buf, i, nc=1):
        n = buf.shape[0] // self.nd
        m = n // nc
        half = self.nd // 2
        for c in range(nc):
            for part in range(2):
                ref = self.slot(buf, self.nd // 4, c * m + part * (m // 2), m // 2)
                self.await_bytes(ref, self.gsem.at[i, 4 * part + self.nd // 4 - 1, c])
        self.relay(self.slot(buf, self.nd // 4), i, self.rsem.at[i], self.partner)
        self.await_bytes(buf.at[pl.ds(0, half * n)], self.rsem.at[i])
        self.await_bytes(buf.at[pl.ds(0, (2 * half - 1) * n)], self.ssem.at[i])

    def swap_start(self, send, recv, via, i, t, rows):
        part = pl.ds(pl.multiple_of(rows * t, 8), rows)
        far = self.nd // 4
        for same, sign in ((True, 1), (False, -1)):
            x = 0 if same else 1
            self.copy(send.at[self.at(far, same), part], via.at[x, part], self.ssem.at[i],
                      self.xsem.at[i - 8, x, t], self.at(sign)).start()
        for k in range(1, far):
            for sign in (1, -1):
                for same in (True, False):
                    d = self.at(sign * k, same)
                    self.copy(send.at[d, part], recv.at[self.me, part], self.ssem.at[i], self.rsem.at[i], d).start()
        self.copy(send.at[self.partner, part], recv.at[self.me, part], self.ssem.at[i], self.rsem.at[i], self.partner).start()
        pltpu.make_async_copy(send.at[self.me, part], recv.at[self.me, part], self.rsem.at[i]).start()

    def swap_on(self, recv, via, i, t, rows):
        part = pl.ds(pl.multiple_of(rows * t, 8), rows)
        far = self.nd // 4
        for same, sign in ((True, 1), (False, -1)):
            x = 0 if same else 1
            self.await_bytes(via.at[x, part], self.xsem.at[i - 8, x, t])
            self.copy(via.at[x, part], recv.at[self.at(-sign), part], self.fsem.at[i], self.rsem.at[i],
                      self.at(sign * (far - 1), same)).start()

    def swap_finish(self, send, recv, via, i):
        self.await_bytes(recv, self.rsem.at[i])
        self.await_bytes(send.at[pl.ds(0, self.nd - 1)], self.ssem.at[i])
        self.await_bytes(via, self.fsem.at[i])


def kernel(names, outs, nd, refs):
    r = dict(zip(names, refs))
    class N:
        pass
    v = N()
    v.__dict__.update(r)
    sl, nr, cm = v.m.shape
    rl, _, cz = v.z.shape
    ns = sl * nd
    wm, wz = v.row_w.shape[1] // 4, v.ts_w.shape[1] // 4
    gm, gz = wm // 128, wz // 128
    od = v.opm_i.shape[1] // 2
    comm = Comm(nd, (v.ssem, v.rsem, v.fsem, v.gsem, v.xsem))
    me = comm.me
    rows_m = sl * rl

    def store_piece(buf):
        def store(i, val):
            buf[me * rl + i] = val
        return store

    def loop(n, body):
        def step(t, _):
            body(t)
            return 0
        lax.fori_loop(0, n, step, 0)

    def row_project(load, b):
        loop(sl // 2, lambda t: project([load(2 * t), load(2 * t + 1)], v.row_w.at[b], v.rt, v.rk, 2 * t, None))

    def row_attend(load, b, finish):
        def attend(s):
            keep = widen(spread(v.mask_seq[pl.ds(s, 1), :], 128), 4 * nr)
            return core(v.rt, v.rk, v.ro, [s], gm, v.rbias, [keep])

        def back(t):
            ups = [dot(v.ro[2 * t + n], v.row_o[b], 0, 0) for n in range(2)]
            yield
            yield from finish(t, [residual(load(2 * t + n), ups[n]) for n in range(2)])

        def body(u):
            interleave(back(u), attend(2 * u + 2))
            interleave(attend(2 * u + 3))
        interleave(attend(0))
        interleave(attend(1))
        loop(sl // 2 - 1, body)
        interleave(back(sl // 2 - 1))

    def col_project(load, b, after=lambda t: None):
        def body(t):
            project([load(4 * t + n) for n in range(4)], v.col_w.at[b], v.ct, v.ck, 4 * t, None)
            after(t)
        loop(rl // 4, body)

    def col_attend(first, count, after=lambda u: None):
        def body(u):
            t = first + u
            rows = [2 * t, 2 * t + 1]
            keeps = [widen(spread(v.mask_col[pl.ds(i, 1), :], 128), 4 * ns) for i in rows]
            interleave(core(v.ct, v.ck, v.co, rows, gm, None, keeps))
            after(u)
        loop(count, body)

    def col_out(load, b, finish, loc, gat, after=lambda t: None):
        def out(t):
            rows = [4 * t + n for n in range(4)]
            ups = [dot(v.co[i], v.col_o[b], 0, 0) for i in rows]
            new = [residual(load(i), u) for i, u in zip(rows, ups)]
            newf = [x.astype(F32) for x in new]
            finish(t, new, newf)
            ln = [layer_norm(x) for x in newf]
            acs = [dot(v.opm_i[b], x, 1, 1) for x in ln]
            for i, x in zip(rows, acs):
                ac = (x * v.mask_col[pl.ds(i, 1), :]).astype(BF16)
                a, c = ac[:od], ac[od:]
                loc[i] = a if b == 0 else c
                gat[me * rl + i] = c if b == 0 else a
            after(t)
        loop(rl // 4, out)

    def opm(loc, gat, b, load, wb, piece, between):
        v.gcol[...] = gat[...].astype(F32).reshape(v.gcol.shape)
        v.nrm[...] = dot(v.mask_col[...].astype(BF16), v.msa_mask[...].astype(F32).astype(BF16), 1, 0)

        def grow(t):
            left = loc[...].reshape(rl * od, ns)
            for n in range(4):
                g = 4 * t + n
                col = v.gcol[pl.ds(g, nr, stride=od), :].astype(BF16)
                x = dot(left, col, 1, 1).astype(BF16)
                off = pl.multiple_of(g * od, od)
                for i in range(rl):
                    v.xs[i, pl.ds(off, od), :] = x[od * i:od * i + od]
        loop(od // 4, grow)
        between()

        def fold(t):
            rows = [4 * t + n for n in range(4)]
            ups = [dot(v.opm_w[b], v.xs[i], 1, 0) for i in rows]
            ups = [u / (1e-3 + v.nrm[pl.ds(i, 1), :]) for i, u in zip(rows, ups)]
            ups = [u.T for u in ups]
            new = [residual(load(i), u) for i, u in zip(rows, ups)]
            for i, x in zip(rows, new):
                v.zc[i] = x
            ln = [layer_norm(x.astype(F32)) for x in new]
            ps = [dot(wb, x, 1, 1) for x in ln]
            for i, x in zip(rows, ps):
                piece[me * rl + i] = x.astype(BF16)
        loop(rl // 4, fold)

    def zload(i):
        return v.zc[i].astype(F32)

    def tri_project(w):
        loop(rl // 4, lambda t: project([zload(4 * t + n) for n in range(4)], w, v.tt, v.tk, 4 * t, v.kc[...]))

    def tri_attend(wo, finish):
        def attend(t):
            return core(v.tt, v.tk, v.to, [4 * t + n for n in range(4)], gz, v.tbias, None)

        def back(t):
            rows = [4 * t + n for n in range(4)]
            ups = [dot(v.to[i], wo, 0, 0) for i in rows]
            yield
            yield from finish(t, [residual(zload(i), u) for i, u in zip(rows, ups)])

        interleave(attend(0))
        loop(rl // 4 - 1, lambda u: interleave(back(u), attend(u + 1)))
        interleave(back(rl // 4 - 1))

    def pieces(t, new, wb, piece):
        ln = [layer_norm(x.astype(F32)) for x in new]
        yield
        ps = [dot(wb, x, 1, 1) for x in ln]
        for n, x in enumerate(ps):
            piece[me * rl + len(new) * t + n] = x.astype(BF16)

    def send(out, recv, via, i, rows, wb=None, piece=None):
        def finish(t, new):
            half = len(new) // 2
            for n in range(half):
                stage(out, half * t + n, new[2 * n].astype(F32), new[2 * n + 1].astype(F32), nd)
            count = len(new) * rows
            comm.swap_start(out, recv, via, i, t, count)
            if isinstance(t, int):
                comm.swap_on(recv, via, i, t - 1, count)
            else:
                @pl.when(t > 0)
                def _():
                    comm.swap_on(recv, via, i, t - 1, count)
            if piece is not None:
                yield from pieces(t, new, wb, piece)
            else:
                yield
        return finish

    def keep(out, wb=None, piece=None):
        def finish(t, new):
            for n, x in enumerate(new):
                out[len(new) * t + n] = x
            if piece is not None:
                yield from pieces(t, new, wb, piece)
            else:
                yield
        return finish

    def turn(recv):
        fill(v.zwork, recv)
        for b in range(rl):
            v.zc[b] = take(v.zwork, b, nr, rl).astype(BF16)

    def mask_r():
        return v.res_mask[...].astype(F32)

    def prepare():
        v.mask_t[...] = v.msa_mask[...].astype(F32).T
        v.mask_seq[...] = v.msa_mask[pl.ds(pl.multiple_of(me * sl, sl), sl), :].astype(F32)
        for i in range(rl):
            v.mask_col[pl.ds(i, 1), :] = v.mask_t[pl.ds(me * rl + i, 1), :]
        v.kc[...] = spread(mask_r(), wz)
        size = od * od
        v.gcol[0:size] = v.opm_o[0].astype(F32)
        for q in range(od):
            v.gcol[size + od * q:size + od * q + od] = v.gcol[pl.ds(q, od, stride=od), :]
        for j in range(size // 128):
            v.opm_w[0, :, 128 * j:128 * j + 128] = v.gcol[size + 128 * j:size + 128 * j + 128].T.astype(BF16)
            v.opm_w[1, :, 128 * j:128 * j + 128] = v.opm_o[1, 128 * j:128 * j + 128, :].astype(F32).T.astype(BF16)

    comm.barrier_signal()
    bias_pieces(lambda i: v.z[i].astype(F32), rl, v.row_b[0], store_piece(v.g0))
    comm.barrier_wait()
    comm.gather_start(v.g0, 0)
    mload = lambda s: v.m[s].astype(F32)
    row_project(mload, 0)
    prepare()
    comm.gather_finish(v.g0, 0)
    spread_bias(v.g0, v.gf, v.rbias, True, None)
    row_attend(mload, 0, send(v.s0, v.r0, v.x0, 8, rl))
    comm.swap_on(v.r0, v.x0, 8, sl // 2 - 1, 2 * rl)
    comm.swap_finish(v.s0, v.r0, v.x0, 8)

    fill(v.mwork, v.r0)
    cload = lambda i: take(v.mwork, i, ns, rl)
    col_project(cload, 0)

    def keep_four(t, new, newf):
        for n, x in enumerate(new):
            v.mc[4 * t + n] = x
    col_attend(0, rl // 2)
    nc = rl // 4
    col_out(cload, 0, keep_four, v.loc0, v.g1, lambda t: comm.relay_start(v.g1, 1, t, nc))

    c2load = lambda i: v.mc[i].astype(F32)

    def send_four(t, new, newf):
        for n in range(2):
            stage(v.s1, 2 * t + n, newf[2 * n], newf[2 * n + 1], nd)
    col_project(c2load, 1, lambda t: comm.relay_step(v.g1, 1, 1, t, nc))
    col_attend(0, rl // 4, lambda t: comm.relay_step(v.g1, 1, 2, t, nc))
    col_attend(rl // 4, rl // 4, lambda t: comm.relay_step(v.g1, 1, 3, t, nc))
    col_out(c2load, 1, send_four, v.loc1, v.g2)
    comm.relay_finish(v.g1, 1, nc)
    comm.relay_start(v.g2, 2)
    opm(v.loc0, v.g1, 0, lambda i: v.z[i].astype(F32), v.ts_b[0], v.g3, lambda: comm.relay_step(v.g2, 2, 1))
    comm.gather_start(v.g3, 3)
    comm.relay_step(v.g2, 2, 2)
    tri_project(v.ts_w.at[0])
    comm.gather_finish(v.g3, 3)
    comm.relay_step(v.g2, 2, 3)
    spread_bias(v.g3, v.gf2, v.tbias, True, mask_r())
    tri_attend(v.ts_o[0], send(v.s2, v.r2, v.x2, 9, rl, v.te_b[0], v.g4))
    comm.gather_start(v.g4, 4)
    comm.swap_on(v.r2, v.x2, 9, rl // 4 - 1, 4 * rl)
    comm.swap_finish(v.s2, v.r2, v.x2, 9)
    turn(v.r2)
    tri_project(v.te_w.at[0])
    comm.gather_finish(v.g4, 4)
    comm.swap_start(v.s1, v.r1, v.x1, 10, 0, rows_m)
    spread_bias(v.g4, v.gf2, v.tbias, False, mask_r())
    tri_attend(v.te_o[0], keep(v.zc, v.row_b[1], v.g5))

    comm.swap_on(v.r1, v.x1, 10, 0, rows_m)

    comm.relay_finish(v.g2, 2)
    comm.relay_start(v.g5, 5)
    opm(v.loc1, v.g2, 1, zload, v.te_b[1], v.g6, lambda: comm.relay_step(v.g5, 5, 1))
    comm.gather_start(v.g6, 6)
    comm.relay_step(v.g5, 5, 2)
    comm.swap_finish(v.s1, v.r1, v.x1, 10)
    fill(v.mwork, v.r1)
    rload = lambda s: take(v.mwork, s, nr, sl)
    row_project(rload, 1)
    comm.relay_step(v.g5, 5, 3)
    tri_project(v.te_w.at[1])
    comm.gather_finish(v.g6, 6)
    spread_bias(v.g6, v.gf2, v.tbias, True, mask_r())
    tri_attend(v.te_o[1], send(v.s3, v.r3, v.x3, 11, rl, v.ts_b[1], v.g7))
    comm.gather_start(v.g7, 7)
    comm.swap_on(v.r3, v.x3, 11, rl // 4 - 1, 4 * rl)
    comm.relay_finish(v.g5, 5)
    spread_bias(v.g5, v.gf, v.rbias, False, None)
    row_attend(rload, 1, keep(v.m_out))
    comm.swap_finish(v.s3, v.r3, v.x3, 11)
    turn(v.r3)
    tri_project(v.ts_w.at[1])
    comm.gather_finish(v.g7, 7)
    spread_bias(v.g7, v.gf2, v.tbias, False, mask_r())
    tri_attend(v.ts_o[1], keep(v.z_out))


def solution(mesh):
    nd = mesh.shape['dap']

    def local_step(m, z, msa_mask, res_mask, w_row_bias, w_row_in, w_row_out, w_col_in, w_col_out, w_opm_in, w_opm_out, w_ts_bias, w_ts_in, w_ts_out, w_te_bias, w_te_in, w_te_out):
        sl, nr, cm = m.shape
        rl, _, cz = z.shape
        ns = sl * nd
        hm, ht = w_row_bias.shape[2], w_ts_bias.shape[2]
        wm, wz = hm * HEAD, ht * HEAD
        od = w_opm_in.shape[3]

        def rows_of(w):
            return jnp.moveaxis(w, 1, -1).reshape(2, -1, w.shape[1])

        ins = dict(m=m, z=z, msa_mask=msa_mask, res_mask=res_mask[None, :],
                   row_w=rows_of(w_row_in), row_o=w_row_out.reshape(2, wm, cm), row_b=rows_of(w_row_bias),
                   col_w=rows_of(w_col_in), col_o=w_col_out.reshape(2, wm, cm),
                   ts_w=rows_of(w_ts_in), ts_o=w_ts_out.reshape(2, wz, cz), ts_b=rows_of(w_ts_bias),
                   te_w=rows_of(w_te_in), te_o=w_te_out.reshape(2, wz, cz), te_b=rows_of(w_te_bias),
                   opm_i=rows_of(w_opm_in), opm_o=w_opm_out.reshape(2, od * od, cz))
        outs = dict(m_out=m, z_out=z)
        gm, gz = wm // 128, wz // 128
        xm, xz = (nd, sl * rl, cm), (nd, rl * rl, cz)
        grow, gtri, gopm = (nd * rl, hm, nr), (nd * rl, ht, nr), (nd * rl, od, ns)
        scratch = dict(
            x0=((2,) + xm[1:], BF16), x1=((2,) + xm[1:], BF16), x2=((2,) + xz[1:], BF16), x3=((2,) + xz[1:], BF16),
            s0=(xm, BF16), r0=(xm, BF16), s1=(xm, BF16), r1=(xm, BF16),
            s2=(xz, BF16), r2=(xz, BF16), s3=(xz, BF16), r3=(xz, BF16),
            g0=(grow, BF16), g5=(grow, BF16), g1=(gopm, BF16), g2=(gopm, BF16),
            g3=(gtri, BF16), g4=(gtri, BF16), g6=(gtri, BF16), g7=(gtri, BF16),
            gf=(grow, F32), gf2=(gtri, F32), rbias=((gm, nr, 4 * nr), F32), tbias=((gz, nr, 4 * nr), F32),
            mwork=((cm // 128, nd * sl * rl, 128), F32), zwork=((cz // 128, nr * rl, 128), F32),
            gcol=((nr * od, ns), F32), xs=((rl, od * od, nr), BF16), nrm=((rl, nr), F32), kc=((nr, wz), F32),
            rt=((sl, 3 * wm, nr), BF16), rk=((sl, nr, wm), BF16), ro=((sl, wm, nr), BF16),
            ct=((rl, 3 * wm, ns), BF16), ck=((rl, ns, wm), BF16), co=((rl, wm, ns), BF16),
            tt=((rl, 3 * wz, nr), BF16), tk=((rl, nr, wz), BF16), to=((rl, wz, nr), BF16),
            mask_t=((nr, ns), F32), mask_seq=((sl, nr), F32), mask_col=((rl, ns), F32), opm_w=((2, cz, od * od), BF16),
            mc=((rl, ns, cm), BF16), zc=((rl, nr, cz), BF16), loc0=((rl, od, ns), BF16), loc1=((rl, od, ns), BF16))
        sems = dict(ssem=(12,), rsem=(12,), fsem=(12,), gsem=(8, nd // 2 + 1, 3), xsem=(4, 2, 4))
        names = list(ins) + list(outs) + list(scratch) + list(sems)
        return pl.pallas_call(
            lambda *refs: kernel(names, outs, nd, refs),
            out_shape=[jax.ShapeDtypeStruct(o.shape, o.dtype) for o in outs.values()],
            in_specs=[pl.BlockSpec(memory_space=pltpu.VMEM)] * len(ins),
            out_specs=[pl.BlockSpec(memory_space=pltpu.VMEM)] * len(outs),
            scratch_shapes=[pltpu.VMEM(*x) for x in scratch.values()] + [pltpu.SemaphoreType.DMA(x) for x in sems.values()],
            compiler_params=pltpu.CompilerParams(collective_id=0, has_side_effects=True, vmem_limit_bytes=67043328),
        )(*ins.values())

    in_specs = (P(('data', 'dap')), P(('data', 'dap')), P('data'), P('data')) + (P(),) * 13
    out_specs = (P(('data', 'dap')), P(('data', 'dap')))
    return jax.shard_map(local_step, mesh=mesh, in_specs=in_specs, out_specs=out_specs, check_vma=False)
```

```python
import functools

import jax
import jax.numpy as jnp
from jax import lax
from jax.experimental import pallas as pl
from jax.experimental.pallas import tpu as pltpu
from jax.sharding import PartitionSpec as P

F32 = jnp.float32
BF16 = jnp.bfloat16
LOG2E = 1.4426950408889634
NEG = -1e9 * LOG2E
HEAD = 32
MESH = pl.DeviceIdType.MESH


def dot(lhs, rhs, lc, rc):
    return lax.dot_general(lhs, rhs, (((lc,), (rc,)), ((), ())), preferred_element_type=F32)


def layer_norm(x):
    mean = jnp.mean(x, axis=-1, keepdims=True)
    cen = x - mean
    var = jnp.mean(cen * cen, axis=-1, keepdims=True)
    return (cen * lax.rsqrt(var + 1e-5)).astype(BF16)


def project(xs, w, t_ref, k_ref, first, kcol):
    width = w.shape[0] // 4
    xl = [layer_norm(x) for x in xs]
    for n, v in enumerate([dot(w[:width], v, 1, 1) for v in xl]):
        t_ref[first + n, 0:width] = v.astype(BF16)
    for n, v in enumerate([dot(w[2 * width:], v, 1, 1) for v in xl]):
        t_ref[first + n, width:3 * width] = v.astype(BF16)
    for n, v in enumerate([dot(v, w[width:2 * width], 1, 1) for v in xl]):
        if kcol is not None:
            v = v * kcol
        k_ref[first + n] = v.astype(BF16)


def diagonal(t, base, length):
    cols = []
    for r in range(4):
        parts = [t[base + HEAD * r:base + HEAD * r + HEAD]]
        if r > 0:
            parts.insert(0, jnp.zeros((HEAD * r, length), BF16))
        if r < 3:
            parts.append(jnp.zeros((HEAD * (3 - r), length), BF16))
        cols.append(jnp.concatenate(parts, axis=0))
    return jnp.concatenate(cols, axis=1)


def core(t_ref, k_ref, o_ref, rows, groups, bias, keeps):
    length = k_ref.shape[1]
    width = 128 * groups
    units = [(n, b, g) for n, b in enumerate(rows) for g in range(groups)]
    scores = []
    for n, b, g in units:
        t = t_ref[b, 128 * g:128 * g + 128, :]
        scores.append(dot(k_ref[b, :, 128 * g:128 * g + 128], diagonal(t, 0, length), 1, 0))
    yield
    probs = []
    dens = []
    for (n, b, g), s in zip(units, scores):
        s = s * (HEAD ** -0.5 * LOG2E)
        if bias is not None:
            s = s + bias[g]
        if keeps is not None:
            s = jnp.where(keeps[n] > 0, s, NEG)
        e = jnp.exp2(s - jnp.max(s, axis=0, keepdims=True))
        dens.append(jnp.sum(e, axis=0, keepdims=True))
        probs.append(e.astype(BF16))
    yield
    outs = [dot(t_ref[b, width + 128 * g:width + 128 * g + 128, :], p, 1, 0) for (n, b, g), p in zip(units, probs)]
    yield
    for (n, b, g), o, den in zip(units, outs, dens):
        inv = 1.0 / den
        gate = jax.nn.sigmoid(t_ref[b, 2 * width + 128 * g:2 * width + 128 * g + 128, :].astype(F32))
        parts = []
        for r in range(4):
            lanes = slice(length * r, length * r + length)
            parts.append(o[HEAD * r:HEAD * r + HEAD, lanes] * inv[:, lanes])
        o_ref[b, 128 * g:128 * g + 128, :] = (jnp.concatenate(parts, axis=0) * gate).astype(BF16)


def interleave(*gens):
    live = list(gens)
    while live:
        for gen in list(live):
            try:
                next(gen)
            except StopIteration:
                live.remove(gen)


def residual(x, update):
    return (x + update).astype(BF16)


def spread(row, lanes):
    return jnp.broadcast_to(row, (lanes, row.shape[1])).T


def widen(block, lanes):
    return jnp.concatenate([block] * (lanes // 128), axis=1)


def stage(stg, pair, first, second, ndev):
    rows = first.shape[0] // ndev
    off = pl.multiple_of(2 * rows * pair, 8)
    for d in range(ndev):
        both = jnp.concatenate([first[rows * d:rows * d + rows], second[rows * d:rows * d + rows]], axis=0)
        stg[d, pl.ds(off, 2 * rows), :] = both.astype(BF16)


def fill(work, ref):
    for t in range(work.shape[0]):
        work[t] = ref[..., 128 * t:128 * t + 128].astype(F32).reshape(work.shape[1:])


def take(work, start, count, stride):
    return jnp.concatenate([work.at[t][pl.ds(start, count, stride=stride), :] for t in range(work.shape[0])], axis=1)


def spread_bias(gath, gf, bias, transpose, mask_row):
    length, heads = gath.shape[0], gath.shape[1]
    gf[...] = gath[...].astype(F32)
    keep = None if mask_row is None else widen(spread(mask_row, 128), 4 * length)
    for g in range(heads // 4):
        parts = []
        for r in range(4):
            value = gf[:, 4 * g + r, :]
            parts.append(value.T if transpose else value)
        value = jnp.concatenate(parts, axis=1) * LOG2E
        if keep is not None:
            value = jnp.where(keep > 0, value, NEG)
        bias[g] = value


def bias_pieces(load, count, wb, store):
    def body(t, _):
        zl = [layer_norm(load(4 * t + n)) for n in range(4)]
        ps = [dot(wb, v, 1, 1) for v in zl]
        for n, v in enumerate(ps):
            store(4 * t + n, v.astype(BF16))
        return 0
    lax.fori_loop(0, count // 4, body, 0)


class Comm:
    def __init__(self, nd, sems):
        self.nd = nd
        self.me = lax.axis_index('dap')
        self.partner = self.me + 1 - 2 * lax.rem(self.me, 2)
        self.ssem, self.rsem, self.fsem, self.gsem = sems

    def copy(self, src, dst, send, recv, dev):
        return pltpu.make_async_remote_copy(src_ref=src, dst_ref=dst, send_sem=send, recv_sem=recv,
                                            device_id={'dap': dev}, device_id_type=MESH)

    def near(self, k, unit):
        off = ((k + 1) // 2) * (2 * lax.rem(k, 2) - 1)
        return lax.rem(self.me + self.nd + unit * off, self.nd)

    def barrier_signal(self):
        bar = pltpu.get_barrier_semaphore()

        def body(k, _):
            pl.semaphore_signal(bar, inc=1, device_id={'dap': lax.rem(self.me + k, self.nd)}, device_id_type=MESH)
            return 0
        lax.fori_loop(1, self.nd, body, 0)

    def barrier_wait(self):
        pl.semaphore_wait(pltpu.get_barrier_semaphore(), self.nd - 1)

    def await_bytes(self, ref, sem):
        pltpu.make_async_copy(ref, ref, sem).wait()

    def at(self, chips, same=True):
        base = self.me if same else self.partner
        return lax.rem(base + self.nd + 2 * chips, self.nd)

    def slot(self, buf, chips, start=0, count=None):
        n = buf.shape[0] // self.nd
        return buf.at[pl.ds(self.at(chips) * n + start, n if count is None else count)]

    def gather_start(self, buf, i):
        own = self.slot(buf, 0)

        def body(k, _):
            self.copy(own, own, self.ssem.at[i], self.gsem.at[i, k, 0], self.near(k, 2)).start()
            return 0
        lax.fori_loop(1, self.nd // 2, body, 0)
        self.copy(own, own, self.ssem.at[i], self.gsem.at[i, 0, 0], self.partner).start()

    def gather_finish(self, buf, i):
        n = buf.shape[0] // self.nd
        half = self.nd // 2

        def body(k, _):
            slot = buf.at[pl.ds(self.near(k, -2) * n, n)]
            self.await_bytes(slot, self.gsem.at[i, k, 0])
            self.copy(slot, slot, self.fsem.at[i], self.rsem.at[i], self.partner).start()
            return 0
        lax.fori_loop(1, half, body, 0)
        self.await_bytes(buf.at[pl.ds(0, n)], self.gsem.at[i, 0, 0])
        rest = buf.at[pl.ds(0, (half - 1) * n)]
        self.await_bytes(rest, self.rsem.at[i])
        self.await_bytes(rest, self.fsem.at[i])
        self.await_bytes(buf.at[pl.ds(0, half * n)], self.ssem.at[i])

    def relay(self, ref, i, recv, dev):
        self.copy(ref, ref, self.ssem.at[i], recv, dev).start()

    def relay_start(self, buf, i, c=0, nc=1):
        m = buf.shape[0] // self.nd // nc
        own = self.slot(buf, 0, c * m, m)
        self.relay(own, i, self.gsem.at[i, 0, c], self.at(1))
        self.relay(own, i, self.gsem.at[i, 4, c], self.at(-1))
        self.relay(own, i, self.rsem.at[i], self.partner)

    def relay_step(self, buf, i, p, c=0, nc=1):
        m = buf.shape[0] // self.nd // nc
        for part, sign in ((0, 1), (1, -1)):
            ref = self.slot(buf, -sign * p, c * m, m)
            self.await_bytes(ref, self.gsem.at[i, 4 * part + p - 1, c])
            on = self.slot(buf, -sign * p, c * m + part * (m // 2), m // 2) if p == self.nd // 4 - 1 else ref
            self.relay(on, i, self.gsem.at[i, 4 * part + p, c], self.at(sign))
            self.relay(ref, i, self.rsem.at[i], self.partner)

    def relay_finish(self, buf, i, nc=1):
        n = buf.shape[0] // self.nd
        m = n // nc
        half = self.nd // 2
        for c in range(nc):
            for part in range(2):
                ref = self.slot(buf, self.nd // 4, c * m + part * (m // 2), m // 2)
                self.await_bytes(ref, self.gsem.at[i, 4 * part + self.nd // 4 - 1, c])
        self.relay(self.slot(buf, self.nd // 4), i, self.rsem.at[i], self.partner)
        self.await_bytes(buf.at[pl.ds(0, half * n)], self.rsem.at[i])
        self.await_bytes(buf.at[pl.ds(0, (2 * half - 1) * n)], self.ssem.at[i])

    def swap_start(self, send, recv, i, t, rows):
        part = pl.ds(pl.multiple_of(rows * t, 8), rows)
        for k in range(1, self.nd):
            off = (k + 1) // 2 if k % 2 else -(k // 2)
            d = lax.rem(self.me + self.nd + off, self.nd)
            self.copy(send.at[d, part], recv.at[self.me, part], self.ssem.at[i], self.rsem.at[i], d).start()
        pltpu.make_async_copy(send.at[self.me, part], recv.at[self.me, part], self.rsem.at[i]).start()

    def swap_finish(self, send, recv, i):
        self.await_bytes(recv, self.rsem.at[i])
        self.await_bytes(send.at[pl.ds(0, self.nd - 1)], self.ssem.at[i])


def kernel(names, outs, nd, refs):
    r = dict(zip(names, refs))
    class N:
        pass
    v = N()
    v.__dict__.update(r)
    sl, nr, cm = v.m.shape
    rl, _, cz = v.z.shape
    ns = sl * nd
    wm, wz = v.row_w.shape[1] // 4, v.ts_w.shape[1] // 4
    gm, gz = wm // 128, wz // 128
    od = v.opm_i.shape[1] // 2
    comm = Comm(nd, (v.ssem, v.rsem, v.fsem, v.gsem))
    me = comm.me
    rows_m = sl * rl

    def store_piece(buf):
        def store(i, val):
            buf[me * rl + i] = val
        return store

    def loop(n, body):
        def step(t, _):
            body(t)
            return 0
        lax.fori_loop(0, n, step, 0)

    def row_project(load, b):
        loop(sl // 2, lambda t: project([load(2 * t), load(2 * t + 1)], v.row_w.at[b], v.rt, v.rk, 2 * t, None))

    def row_attend(load, b, finish):
        def attend(s):
            keep = widen(spread(v.mask_seq[pl.ds(s, 1), :], 128), 4 * nr)
            return core(v.rt, v.rk, v.ro, [s], gm, v.rbias, [keep])

        def back(t):
            ups = [dot(v.ro[2 * t + n], v.row_o[b], 0, 0) for n in range(2)]
            yield
            yield from finish(t, [residual(load(2 * t + n), ups[n]) for n in range(2)])

        def body(u):
            interleave(back(u), attend(2 * u + 2))
            interleave(attend(2 * u + 3))
        interleave(attend(0))
        interleave(attend(1))
        loop(sl // 2 - 1, body)
        interleave(back(sl // 2 - 1))

    def col_project(load, b, after=lambda t: None):
        def body(t):
            project([load(4 * t + n) for n in range(4)], v.col_w.at[b], v.ct, v.ck, 4 * t, None)
            after(t)
        loop(rl // 4, body)

    def col_attend(first, count, after=lambda u: None):
        def body(u):
            t = first + u
            rows = [2 * t, 2 * t + 1]
            keeps = [widen(spread(v.mask_col[pl.ds(i, 1), :], 128), 4 * ns) for i in rows]
            interleave(core(v.ct, v.ck, v.co, rows, gm, None, keeps))
            after(u)
        loop(count, body)

    def col_out(load, b, finish, loc, gat, after=lambda t: None):
        def out(t):
            rows = [4 * t + n for n in range(4)]
            ups = [dot(v.co[i], v.col_o[b], 0, 0) for i in rows]
            new = [residual(load(i), u) for i, u in zip(rows, ups)]
            newf = [x.astype(F32) for x in new]
            finish(t, new, newf)
            ln = [layer_norm(x) for x in newf]
            acs = [dot(v.opm_i[b], x, 1, 1) for x in ln]
            for i, x in zip(rows, acs):
                ac = (x * v.mask_col[pl.ds(i, 1), :]).astype(BF16)
                a, c = ac[:od], ac[od:]
                loc[i] = a if b == 0 else c
                gat[me * rl + i] = c if b == 0 else a
            after(t)
        loop(rl // 4, out)

    def opm(loc, gat, b, load, wb, piece, between):
        v.gcol[...] = gat[...].astype(F32).reshape(v.gcol.shape)
        v.nrm[...] = dot(v.mask_col[...].astype(BF16), v.msa_mask[...].astype(F32).astype(BF16), 1, 0)

        def grow(t):
            left = loc[...].reshape(rl * od, ns)
            for n in range(4):
                g = 4 * t + n
                col = v.gcol[pl.ds(g, nr, stride=od), :].astype(BF16)
                x = dot(left, col, 1, 1).astype(BF16)
                off = pl.multiple_of(g * od, od)
                for i in range(rl):
                    v.xs[i, pl.ds(off, od), :] = x[od * i:od * i + od]
        loop(od // 4, grow)
        between()

        def fold(t):
            rows = [4 * t + n for n in range(4)]
            ups = [dot(v.opm_w[b], v.xs[i], 1, 0) for i in rows]
            ups = [u / (1e-3 + v.nrm[pl.ds(i, 1), :]) for i, u in zip(rows, ups)]
            ups = [u.T for u in ups]
            new = [residual(load(i), u) for i, u in zip(rows, ups)]
            for i, x in zip(rows, new):
                v.zc[i] = x
            ln = [layer_norm(x.astype(F32)) for x in new]
            ps = [dot(wb, x, 1, 1) for x in ln]
            for i, x in zip(rows, ps):
                piece[me * rl + i] = x.astype(BF16)
        loop(rl // 4, fold)

    def zload(i):
        return v.zc[i].astype(F32)

    def tri_project(w):
        loop(rl // 4, lambda t: project([zload(4 * t + n) for n in range(4)], w, v.tt, v.tk, 4 * t, v.kc[...]))

    def tri_attend(wo, finish):
        def attend(t):
            return core(v.tt, v.tk, v.to, [4 * t + n for n in range(4)], gz, v.tbias, None)

        def back(t):
            rows = [4 * t + n for n in range(4)]
            ups = [dot(v.to[i], wo, 0, 0) for i in rows]
            yield
            yield from finish(t, [residual(zload(i), u) for i, u in zip(rows, ups)])

        interleave(attend(0))
        loop(rl // 4 - 1, lambda u: interleave(back(u), attend(u + 1)))
        interleave(back(rl // 4 - 1))

    def pieces(t, new, wb, piece):
        ln = [layer_norm(x.astype(F32)) for x in new]
        yield
        ps = [dot(wb, x, 1, 1) for x in ln]
        for n, x in enumerate(ps):
            piece[me * rl + len(new) * t + n] = x.astype(BF16)

    def send(out, recv, i, rows, wb=None, piece=None):
        def finish(t, new):
            half = len(new) // 2
            for n in range(half):
                stage(out, half * t + n, new[2 * n].astype(F32), new[2 * n + 1].astype(F32), nd)
            count = len(new) * rows
            comm.swap_start(out, recv, i, t, count)
            if piece is not None:
                yield from pieces(t, new, wb, piece)
            else:
                yield
        return finish

    def keep(out, wb=None, piece=None):
        def finish(t, new):
            for n, x in enumerate(new):
                out[len(new) * t + n] = x
            if piece is not None:
                yield from pieces(t, new, wb, piece)
            else:
                yield
        return finish

    def turn(recv):
        fill(v.zwork, recv)
        for b in range(rl):
            v.zc[b] = take(v.zwork, b, nr, rl).astype(BF16)

    def mask_r():
        return v.res_mask[...].astype(F32)

    def prepare():
        v.mask_t[...] = v.msa_mask[...].astype(F32).T
        v.mask_seq[...] = v.msa_mask[pl.ds(pl.multiple_of(me * sl, sl), sl), :].astype(F32)
        for i in range(rl):
            v.mask_col[pl.ds(i, 1), :] = v.mask_t[pl.ds(me * rl + i, 1), :]
        v.kc[...] = spread(mask_r(), wz)
        size = od * od
        v.gcol[0:size] = v.opm_o[0].astype(F32)
        for q in range(od):
            v.gcol[size + od * q:size + od * q + od] = v.gcol[pl.ds(q, od, stride=od), :]
        for j in range(size // 128):
            v.opm_w[0, :, 128 * j:128 * j + 128] = v.gcol[size + 128 * j:size + 128 * j + 128].T.astype(BF16)
            v.opm_w[1, :, 128 * j:128 * j + 128] = v.opm_o[1, 128 * j:128 * j + 128, :].astype(F32).T.astype(BF16)

    comm.barrier_signal()
    bias_pieces(lambda i: v.z[i].astype(F32), rl, v.row_b[0], store_piece(v.g0))
    comm.barrier_wait()
    comm.gather_start(v.g0, 0)
    mload = lambda s: v.m[s].astype(F32)
    row_project(mload, 0)
    prepare()
    comm.gather_finish(v.g0, 0)
    spread_bias(v.g0, v.gf, v.rbias, True, None)
    row_attend(mload, 0, send(v.s0, v.r0, 8, rl))
    comm.swap_finish(v.s0, v.r0, 8)

    fill(v.mwork, v.r0)
    cload = lambda i: take(v.mwork, i, ns, rl)
    col_project(cload, 0)

    def keep_four(t, new, newf):
        for n, x in enumerate(new):
            v.mc[4 * t + n] = x
    col_attend(0, rl // 2)
    nc = rl // 4
    col_out(cload, 0, keep_four, v.loc0, v.g1, lambda t: comm.relay_start(v.g1, 1, t, nc))

    c2load = lambda i: v.mc[i].astype(F32)

    def send_four(t, new, newf):
        for n in range(2):
            stage(v.s1, 2 * t + n, newf[2 * n], newf[2 * n + 1], nd)
    col_project(c2load, 1, lambda t: comm.relay_step(v.g1, 1, 1, t, nc))
    col_attend(0, rl // 4, lambda t: comm.relay_step(v.g1, 1, 2, t, nc))
    col_attend(rl // 4, rl // 4, lambda t: comm.relay_step(v.g1, 1, 3, t, nc))
    col_out(c2load, 1, send_four, v.loc1, v.g2)
    comm.relay_finish(v.g1, 1, nc)
    comm.relay_start(v.g2, 2)
    opm(v.loc0, v.g1, 0, lambda i: v.z[i].astype(F32), v.ts_b[0], v.g3, lambda: comm.relay_step(v.g2, 2, 1))
    comm.gather_start(v.g3, 3)
    comm.relay_step(v.g2, 2, 2)
    tri_project(v.ts_w.at[0])
    comm.gather_finish(v.g3, 3)
    comm.relay_step(v.g2, 2, 3)
    spread_bias(v.g3, v.gf2, v.tbias, True, mask_r())
    tri_attend(v.ts_o[0], send(v.s2, v.r2, 9, rl, v.te_b[0], v.g4))
    comm.gather_start(v.g4, 4)
    comm.swap_finish(v.s2, v.r2, 9)
    turn(v.r2)
    tri_project(v.te_w.at[0])
    comm.gather_finish(v.g4, 4)
    comm.swap_start(v.s1, v.r1, 10, 0, rows_m)
    spread_bias(v.g4, v.gf2, v.tbias, False, mask_r())
    tri_attend(v.te_o[0], keep(v.zc, v.row_b[1], v.g5))


    comm.relay_finish(v.g2, 2)
    comm.relay_start(v.g5, 5)
    opm(v.loc1, v.g2, 1, zload, v.te_b[1], v.g6, lambda: comm.relay_step(v.g5, 5, 1))
    comm.gather_start(v.g6, 6)
    comm.relay_step(v.g5, 5, 2)
    comm.swap_finish(v.s1, v.r1, 10)
    fill(v.mwork, v.r1)
    rload = lambda s: take(v.mwork, s, nr, sl)
    row_project(rload, 1)
    comm.relay_step(v.g5, 5, 3)
    tri_project(v.te_w.at[1])
    comm.gather_finish(v.g6, 6)
    spread_bias(v.g6, v.gf2, v.tbias, True, mask_r())
    tri_attend(v.te_o[1], send(v.s3, v.r3, 11, rl, v.ts_b[1], v.g7))
    comm.gather_start(v.g7, 7)
    comm.relay_finish(v.g5, 5)
    spread_bias(v.g5, v.gf, v.rbias, False, None)
    row_attend(rload, 1, keep(v.m_out))
    comm.swap_finish(v.s3, v.r3, 11)
    turn(v.r3)
    tri_project(v.ts_w.at[1])
    comm.gather_finish(v.g7, 7)
    spread_bias(v.g7, v.gf2, v.tbias, False, mask_r())
    tri_attend(v.ts_o[1], keep(v.z_out))


def solution(mesh):
    nd = mesh.shape['dap']

    def local_step(m, z, msa_mask, res_mask, w_row_bias, w_row_in, w_row_out, w_col_in, w_col_out, w_opm_in, w_opm_out, w_ts_bias, w_ts_in, w_ts_out, w_te_bias, w_te_in, w_te_out):
        sl, nr, cm = m.shape
        rl, _, cz = z.shape
        ns = sl * nd
        hm, ht = w_row_bias.shape[2], w_ts_bias.shape[2]
        wm, wz = hm * HEAD, ht * HEAD
        od = w_opm_in.shape[3]

        def rows_of(w):
            return jnp.moveaxis(w, 1, -1).reshape(2, -1, w.shape[1])

        ins = dict(m=m, z=z, msa_mask=msa_mask, res_mask=res_mask[None, :],
                   row_w=rows_of(w_row_in), row_o=w_row_out.reshape(2, wm, cm), row_b=rows_of(w_row_bias),
                   col_w=rows_of(w_col_in), col_o=w_col_out.reshape(2, wm, cm),
                   ts_w=rows_of(w_ts_in), ts_o=w_ts_out.reshape(2, wz, cz), ts_b=rows_of(w_ts_bias),
                   te_w=rows_of(w_te_in), te_o=w_te_out.reshape(2, wz, cz), te_b=rows_of(w_te_bias),
                   opm_i=rows_of(w_opm_in), opm_o=w_opm_out.reshape(2, od * od, cz))
        outs = dict(m_out=m, z_out=z)
        gm, gz = wm // 128, wz // 128
        xm, xz = (nd, sl * rl, cm), (nd, rl * rl, cz)
        grow, gtri, gopm = (nd * rl, hm, nr), (nd * rl, ht, nr), (nd * rl, od, ns)
        scratch = dict(
            s0=(xm, BF16), r0=(xm, BF16), s1=(xm, BF16), r1=(xm, BF16),
            s2=(xz, BF16), r2=(xz, BF16), s3=(xz, BF16), r3=(xz, BF16),
            g0=(grow, BF16), g5=(grow, BF16), g1=(gopm, BF16), g2=(gopm, BF16),
            g3=(gtri, BF16), g4=(gtri, BF16), g6=(gtri, BF16), g7=(gtri, BF16),
            gf=(grow, F32), gf2=(gtri, F32), rbias=((gm, nr, 4 * nr), F32), tbias=((gz, nr, 4 * nr), F32),
            mwork=((cm // 128, nd * sl * rl, 128), F32), zwork=((cz // 128, nr * rl, 128), F32),
            gcol=((nr * od, ns), F32), xs=((rl, od * od, nr), BF16), nrm=((rl, nr), F32), kc=((nr, wz), F32),
            rt=((sl, 3 * wm, nr), BF16), rk=((sl, nr, wm), BF16), ro=((sl, wm, nr), BF16),
            ct=((rl, 3 * wm, ns), BF16), ck=((rl, ns, wm), BF16), co=((rl, wm, ns), BF16),
            tt=((rl, 3 * wz, nr), BF16), tk=((rl, nr, wz), BF16), to=((rl, wz, nr), BF16),
            mask_t=((nr, ns), F32), mask_seq=((sl, nr), F32), mask_col=((rl, ns), F32), opm_w=((2, cz, od * od), BF16),
            mc=((rl, ns, cm), BF16), zc=((rl, nr, cz), BF16), loc0=((rl, od, ns), BF16), loc1=((rl, od, ns), BF16))
        sems = dict(ssem=(12,), rsem=(12,), fsem=(8,), gsem=(8, nd // 2, 3))
        names = list(ins) + list(outs) + list(scratch) + list(sems)
        return pl.pallas_call(
            lambda *refs: kernel(names, outs, nd, refs),
            out_shape=[jax.ShapeDtypeStruct(o.shape, o.dtype) for o in outs.values()],
            in_specs=[pl.BlockSpec(memory_space=pltpu.VMEM)] * len(ins),
            out_specs=[pl.BlockSpec(memory_space=pltpu.VMEM)] * len(outs),
            scratch_shapes=[pltpu.VMEM(*x) for x in scratch.values()] + [pltpu.SemaphoreType.DMA(x) for x in sems.values()],
            compiler_params=pltpu.CompilerParams(collective_id=0, has_side_effects=True, vmem_limit_bytes=67043328),
        )(*ins.values())

    in_specs = (P(('data', 'dap')), P(('data', 'dap')), P('data'), P('data')) + (P(),) * 13
    out_specs = (P(('data', 'dap')), P(('data', 'dap')))
    return jax.shard_map(local_step, mesh=mesh, in_specs=in_specs, out_specs=out_specs, check_vma=False)
```

```python
import functools

import jax
import jax.numpy as jnp
from jax import lax
from jax.experimental import pallas as pl
from jax.experimental.pallas import tpu as pltpu
from jax.sharding import PartitionSpec as P

F32 = jnp.float32
BF16 = jnp.bfloat16
LOG2E = 1.4426950408889634
NEG = -1e9 * LOG2E
HEAD = 32
MESH = pl.DeviceIdType.MESH


def dot(lhs, rhs, lc, rc):
    return lax.dot_general(lhs, rhs, (((lc,), (rc,)), ((), ())), preferred_element_type=F32)


def layer_norm(x):
    mean = jnp.mean(x, axis=-1, keepdims=True)
    cen = x - mean
    var = jnp.mean(cen * cen, axis=-1, keepdims=True)
    return (cen * lax.rsqrt(var + 1e-5)).astype(BF16)


def project(xs, w, t_ref, k_ref, first, kcol):
    width = w.shape[0] // 4
    xl = [layer_norm(x) for x in xs]
    for n, v in enumerate([dot(w[:width], v, 1, 1) for v in xl]):
        t_ref[first + n, 0:width] = v.astype(BF16)
    for n, v in enumerate([dot(w[2 * width:], v, 1, 1) for v in xl]):
        t_ref[first + n, width:3 * width] = v.astype(BF16)
    for n, v in enumerate([dot(v, w[width:2 * width], 1, 1) for v in xl]):
        if kcol is not None:
            v = v * kcol
        k_ref[first + n] = v.astype(BF16)


def diagonal(t, base, length):
    cols = []
    for r in range(4):
        parts = [t[base + HEAD * r:base + HEAD * r + HEAD]]
        if r > 0:
            parts.insert(0, jnp.zeros((HEAD * r, length), BF16))
        if r < 3:
            parts.append(jnp.zeros((HEAD * (3 - r), length), BF16))
        cols.append(jnp.concatenate(parts, axis=0))
    return jnp.concatenate(cols, axis=1)


def core(t_ref, k_ref, o_ref, rows, groups, bias, keeps):
    length = k_ref.shape[1]
    width = 128 * groups
    units = [(n, b, g) for n, b in enumerate(rows) for g in range(groups)]
    scores = []
    for n, b, g in units:
        t = t_ref[b, 128 * g:128 * g + 128, :]
        scores.append(dot(k_ref[b, :, 128 * g:128 * g + 128], diagonal(t, 0, length), 1, 0))
    yield
    probs = []
    dens = []
    for (n, b, g), s in zip(units, scores):
        s = s * (HEAD ** -0.5 * LOG2E)
        if bias is not None:
            s = s + bias[g]
        if keeps is not None:
            s = jnp.where(keeps[n] > 0, s, NEG)
        e = jnp.exp2(s - jnp.max(s, axis=0, keepdims=True))
        dens.append(jnp.sum(e, axis=0, keepdims=True))
        probs.append(e.astype(BF16))
    yield
    outs = [dot(t_ref[b, width + 128 * g:width + 128 * g + 128, :], p, 1, 0) for (n, b, g), p in zip(units, probs)]
    yield
    for (n, b, g), o, den in zip(units, outs, dens):
        inv = 1.0 / den
        gate = jax.nn.sigmoid(t_ref[b, 2 * width + 128 * g:2 * width + 128 * g + 128, :].astype(F32))
        parts = []
        for r in range(4):
            lanes = slice(length * r, length * r + length)
            parts.append(o[HEAD * r:HEAD * r + HEAD, lanes] * inv[:, lanes])
        o_ref[b, 128 * g:128 * g + 128, :] = (jnp.concatenate(parts, axis=0) * gate).astype(BF16)


def interleave(*gens):
    live = list(gens)
    while live:
        for gen in list(live):
            try:
                next(gen)
            except StopIteration:
                live.remove(gen)


def residual(x, update):
    return (x + update).astype(BF16)


def spread(row, lanes):
    return jnp.broadcast_to(row, (lanes, row.shape[1])).T


def widen(block, lanes):
    return jnp.concatenate([block] * (lanes // 128), axis=1)


def stage(stg, pair, first, second, ndev):
    rows = first.shape[0] // ndev
    off = pl.multiple_of(2 * rows * pair, 8)
    for d in range(ndev):
        both = jnp.concatenate([first[rows * d:rows * d + rows], second[rows * d:rows * d + rows]], axis=0)
        stg[d, pl.ds(off, 2 * rows), :] = both.astype(BF16)


def fill(work, ref):
    for t in range(work.shape[0]):
        work[t] = ref[..., 128 * t:128 * t + 128].astype(F32).reshape(work.shape[1:])


def take(work, start, count, stride):
    return jnp.concatenate([work.at[t][pl.ds(start, count, stride=stride), :] for t in range(work.shape[0])], axis=1)


def spread_bias(gath, gf, bias, transpose, mask_row):
    length, heads = gath.shape[0], gath.shape[1]
    gf[...] = gath[...].astype(F32)
    keep = None if mask_row is None else widen(spread(mask_row, 128), 4 * length)
    for g in range(heads // 4):
        parts = []
        for r in range(4):
            value = gf[:, 4 * g + r, :]
            parts.append(value.T if transpose else value)
        value = jnp.concatenate(parts, axis=1) * LOG2E
        if keep is not None:
            value = jnp.where(keep > 0, value, NEG)
        bias[g] = value


def bias_pieces(load, count, wb, store, after):
    def body(t, _):
        zl = [layer_norm(load(4 * t + n)) for n in range(4)]
        ps = [dot(wb, v, 1, 1) for v in zl]
        for n, v in enumerate(ps):
            store(4 * t + n, v.astype(BF16))
        after(t)
        return 0
    body(0, 0)
    lax.fori_loop(1, count // 4, body, 0)


class Comm:
    def __init__(self, nd, sems):
        self.nd = nd
        self.me = lax.axis_index('dap')
        self.partner = self.me + 1 - 2 * lax.rem(self.me, 2)
        self.ssem, self.rsem, self.fsem, self.gsem = sems

    def copy(self, src, dst, send, recv, dev):
        return pltpu.make_async_remote_copy(src_ref=src, dst_ref=dst, send_sem=send, recv_sem=recv,
                                            device_id={'dap': dev}, device_id_type=MESH)

    def near(self, k, unit):
        off = ((k + 1) // 2) * (2 * lax.rem(k, 2) - 1)
        return lax.rem(self.me + self.nd + unit * off, self.nd)

    def barrier_signal(self):
        bar = pltpu.get_barrier_semaphore()

        def body(k, _):
            pl.semaphore_signal(bar, inc=1, device_id={'dap': lax.rem(self.me + k, self.nd)}, device_id_type=MESH)
            return 0
        lax.fori_loop(1, self.nd, body, 0)

    def barrier_wait(self):
        pl.semaphore_wait(pltpu.get_barrier_semaphore(), self.nd - 1)

    def await_bytes(self, ref, sem):
        pltpu.make_async_copy(ref, ref, sem).wait()

    def at(self, chips, same=True):
        base = self.me if same else self.partner
        return lax.rem(base + self.nd + 2 * chips, self.nd)

    def slot(self, buf, chips, start=0, count=None):
        n = buf.shape[0] // self.nd
        return buf.at[pl.ds(self.at(chips) * n + start, n if count is None else count)]

    def gather_start(self, buf, i, c=0, nc=1):
        m = buf.shape[0] // self.nd // nc
        own = self.slot(buf, 0, c * m, m)

        def body(j, _):
            k = self.nd // 2 - j
            self.copy(own, own, self.ssem.at[i], self.gsem.at[i, k, 0], self.near(k, 2)).start()
            return 0
        lax.fori_loop(1, self.nd // 2, body, 0)
        self.copy(own, own, self.ssem.at[i], self.gsem.at[i, 0, 0], self.partner).start()

    def gather_finish(self, buf, i):
        n = buf.shape[0] // self.nd
        half = self.nd // 2

        def body(k, _):
            slot = buf.at[pl.ds(self.near(k, -2) * n, n)]
            self.await_bytes(slot, self.gsem.at[i, k, 0])
            self.copy(slot, slot, self.fsem.at[i], self.rsem.at[i], self.partner).start()
            return 0
        lax.fori_loop(1, half, body, 0)
        self.await_bytes(buf.at[pl.ds(0, n)], self.gsem.at[i, 0, 0])
        rest = buf.at[pl.ds(0, (half - 1) * n)]
        self.await_bytes(rest, self.rsem.at[i])
        self.await_bytes(rest, self.fsem.at[i])
        self.await_bytes(buf.at[pl.ds(0, half * n)], self.ssem.at[i])

    def relay(self, ref, i, recv, dev):
        self.copy(ref, ref, self.ssem.at[i], recv, dev).start()

    def relay_start(self, buf, i, c=0, nc=1):
        m = buf.shape[0] // self.nd // nc
        own = self.slot(buf, 0, c * m, m)
        self.relay(own, i, self.gsem.at[i, 0, c], self.at(1))
        self.relay(own, i, self.gsem.at[i, 4, c], self.at(-1))
        self.relay(own, i, self.rsem.at[i], self.partner)

    def relay_step(self, buf, i, p, c=0, nc=1):
        m = buf.shape[0] // self.nd // nc
        for part, sign in ((0, 1), (1, -1)):
            ref = self.slot(buf, -sign * p, c * m, m)
            self.await_bytes(ref, self.gsem.at[i, 4 * part + p - 1, c])
            on = self.slot(buf, -sign * p, c * m + part * (m // 2), m // 2) if p == self.nd // 4 - 1 else ref
            self.relay(on, i, self.gsem.at[i, 4 * part + p, c], self.at(sign))
            self.relay(ref, i, self.rsem.at[i], self.partner)

    def relay_finish(self, buf, i, nc=1):
        n = buf.shape[0] // self.nd
        m = n // nc
        half = self.nd // 2
        for c in range(nc):
            for part in range(2):
                ref = self.slot(buf, self.nd // 4, c * m + part * (m // 2), m // 2)
                self.await_bytes(ref, self.gsem.at[i, 4 * part + self.nd // 4 - 1, c])
        self.relay(self.slot(buf, self.nd // 4), i, self.rsem.at[i], self.partner)
        self.await_bytes(buf.at[pl.ds(0, half * n)], self.rsem.at[i])
        self.await_bytes(buf.at[pl.ds(0, (2 * half - 1) * n)], self.ssem.at[i])

    def swap_start(self, send, recv, i, t, rows):
        part = pl.ds(pl.multiple_of(rows * t, 8), rows)
        for k in range(self.nd - 1, 0, -1):
            off = (k + 1) // 2 if k % 2 else -(k // 2)
            d = lax.rem(self.me + self.nd + off, self.nd)
            self.copy(send.at[d, part], recv.at[self.me, part], self.ssem.at[i], self.rsem.at[i], d).start()
        pltpu.make_async_copy(send.at[self.me, part], recv.at[self.me, part], self.rsem.at[i]).start()

    def swap_finish(self, send, recv, i):
        self.await_bytes(recv, self.rsem.at[i])
        self.await_bytes(send.at[pl.ds(0, self.nd - 1)], self.ssem.at[i])


def kernel(names, late, nd, refs):
    r = dict(zip(names, refs))
    class N:
        pass
    v = N()
    v.__dict__.update(r)
    sl, nr, cm = v.m.shape
    rl, _, cz = v.z.shape
    ns = sl * nd
    wm, wz = v.row_w.shape[1] // 4, v.ts_w.shape[1] // 4
    gm, gz = wm // 128, wz // 128
    od = v.opm_i.shape[1] // 2
    def late_start():
        for n, name in enumerate(late):
            pltpu.make_async_copy(r['hbm_' + name], r[name], v.lsem.at[n]).start()

    def late_wait():
        for n, name in enumerate(late):
            pltpu.make_async_copy(r['hbm_' + name], r[name], v.lsem.at[n]).wait()

    comm = Comm(nd, (v.ssem, v.rsem, v.fsem, v.gsem))
    me = comm.me
    rows_m = sl * rl

    def store_piece(buf):
        def store(i, val):
            buf[me * rl + i] = val
        return store

    def loop(n, body):
        def step(t, _):
            body(t)
            return 0
        lax.fori_loop(0, n, step, 0)

    def row_project(load, b):
        loop(sl // 2, lambda t: project([load(2 * t), load(2 * t + 1)], v.row_w.at[b], v.rt, v.rk, 2 * t, None))

    def row_attend(load, b, finish):
        def attend(s):
            keep = widen(spread(v.mask_seq[pl.ds(s, 1), :], 128), 4 * nr)
            return core(v.rt, v.rk, v.ro, [s], gm, v.rbias, [keep])

        def back(t):
            ups = [dot(v.ro[2 * t + n], v.row_o[b], 0, 0) for n in range(2)]
            yield
            yield from finish(t, [residual(load(2 * t + n), ups[n]) for n in range(2)])

        def body(u):
            interleave(back(u), attend(2 * u + 2))
            interleave(attend(2 * u + 3))
        interleave(attend(0))
        interleave(attend(1))
        loop(sl // 2 - 1, body)
        interleave(back(sl // 2 - 1))

    def col_project(load, b, after=lambda t: None):
        def body(t):
            project([load(4 * t + n) for n in range(4)], v.col_w.at[b], v.ct, v.ck, 4 * t, None)
            after(t)
        loop(rl // 4, body)

    def col_attend(first, count, after=lambda u: None):
        def body(u):
            t = first + u
            rows = [2 * t, 2 * t + 1]
            keeps = [widen(spread(v.mask_col[pl.ds(i, 1), :], 128), 4 * ns) for i in rows]
            interleave(core(v.ct, v.ck, v.co, rows, gm, None, keeps))
            after(u)
        loop(count, body)

    def col_out(load, b, finish, loc, gat, after=lambda t: None):
        def out(t):
            rows = [4 * t + n for n in range(4)]
            ups = [dot(v.co[i], v.col_o[b], 0, 0) for i in rows]
            new = [residual(load(i), u) for i, u in zip(rows, ups)]
            newf = [x.astype(F32) for x in new]
            finish(t, new, newf)
            ln = [layer_norm(x) for x in newf]
            acs = [dot(v.opm_i[b], x, 1, 1) for x in ln]
            for i, x in zip(rows, acs):
                ac = (x * v.mask_col[pl.ds(i, 1), :]).astype(BF16)
                a, c = ac[:od], ac[od:]
                loc[i] = a if b == 0 else c
                gat[me * rl + i] = c if b == 0 else a
            after(t)
        loop(rl // 4, out)

    def opm(loc, gat, b, load, wb, piece, i_piece, between):
        v.gcol[...] = gat[...].astype(F32).reshape(v.gcol.shape)
        v.nrm[...] = dot(v.mask_col[...].astype(BF16), v.msa_mask[...].astype(F32).astype(BF16), 1, 0)

        def grow(t):
            left = loc[...].reshape(rl * od, ns)
            for n in range(4):
                g = 4 * t + n
                col = v.gcol[pl.ds(g, nr, stride=od), :].astype(BF16)
                x = dot(left, col, 1, 1).astype(BF16)
                off = pl.multiple_of(g * od, od)
                for i in range(rl):
                    v.xs[i, pl.ds(off, od), :] = x[od * i:od * i + od]
        loop(od // 4, grow)
        between()

        def fold(t):
            rows = [4 * t + n for n in range(4)]
            ups = [dot(v.opm_w[b], v.xs[i], 1, 0) for i in rows]
            ups = [u / (1e-3 + v.nrm[pl.ds(i, 1), :]) for i, u in zip(rows, ups)]
            ups = [u.T for u in ups]
            new = [residual(load(i), u) for i, u in zip(rows, ups)]
            for i, x in zip(rows, new):
                v.zc[i] = x
            ln = [layer_norm(x.astype(F32)) for x in new]
            ps = [dot(wb, x, 1, 1) for x in ln]
            for i, x in zip(rows, ps):
                piece[me * rl + i] = x.astype(BF16)
            comm.gather_start(piece, i_piece, t, rl // 4)
        loop(rl // 4, fold)

    def zload(i):
        return v.zc[i].astype(F32)

    def tri_project(w):
        loop(rl // 4, lambda t: project([zload(4 * t + n) for n in range(4)], w, v.tt, v.tk, 4 * t, v.kc[...]))

    def tri_attend(wo, finish):
        def attend(t):
            return core(v.tt, v.tk, v.to, [4 * t + n for n in range(4)], gz, v.tbias, None)

        def back(t):
            rows = [4 * t + n for n in range(4)]
            ups = [dot(v.to[i], wo, 0, 0) for i in rows]
            yield
            yield from finish(t, [residual(zload(i), u) for i, u in zip(rows, ups)])

        interleave(attend(0))
        loop(rl // 4 - 1, lambda u: interleave(back(u), attend(u + 1)))
        interleave(back(rl // 4 - 1))

    def pieces(t, new, wb, piece):
        ln = [layer_norm(x.astype(F32)) for x in new]
        yield
        ps = [dot(wb, x, 1, 1) for x in ln]
        for n, x in enumerate(ps):
            piece[me * rl + len(new) * t + n] = x.astype(BF16)

    def send(out, recv, i, rows, wb=None, piece=None):
        def finish(t, new):
            half = len(new) // 2
            for n in range(half):
                stage(out, half * t + n, new[2 * n].astype(F32), new[2 * n + 1].astype(F32), nd)
            count = len(new) * rows
            comm.swap_start(out, recv, i, t, count)
            if piece is not None:
                yield from pieces(t, new, wb, piece)
            else:
                yield
        return finish

    def keep(out, wb=None, piece=None):
        def finish(t, new):
            for n, x in enumerate(new):
                out[len(new) * t + n] = x
            if piece is not None:
                yield from pieces(t, new, wb, piece)
            else:
                yield
        return finish

    def turn(recv):
        fill(v.zwork, recv)
        for b in range(rl):
            v.zc[b] = take(v.zwork, b, nr, rl).astype(BF16)

    def mask_r():
        return v.res_mask[...].astype(F32)

    def prepare():
        v.mask_t[...] = v.msa_mask[...].astype(F32).T
        v.mask_seq[...] = v.msa_mask[pl.ds(pl.multiple_of(me * sl, sl), sl), :].astype(F32)
        for i in range(rl):
            v.mask_col[pl.ds(i, 1), :] = v.mask_t[pl.ds(me * rl + i, 1), :]
        v.kc[...] = spread(mask_r(), wz)
        size = od * od
        v.gcol[0:size] = v.opm_o[0].astype(F32)
        for q in range(od):
            v.gcol[size + od * q:size + od * q + od] = v.gcol[pl.ds(q, od, stride=od), :]
        for j in range(size // 128):
            v.opm_w[0, :, 128 * j:128 * j + 128] = v.gcol[size + 128 * j:size + 128 * j + 128].T.astype(BF16)
            v.opm_w[1, :, 128 * j:128 * j + 128] = v.opm_o[1, 128 * j:128 * j + 128, :].astype(F32).T.astype(BF16)

    comm.barrier_signal()
    late_start()
    nc = rl // 4

    def first_send(t):
        if isinstance(t, int) and t == 0:
            comm.barrier_wait()
        comm.gather_start(v.g0, 0, t, nc)
    bias_pieces(lambda i: v.z[i].astype(F32), rl, v.row_b[0], store_piece(v.g0), first_send)
    late_wait()
    mload = lambda s: v.m[s].astype(F32)
    row_project(mload, 0)
    prepare()
    comm.gather_finish(v.g0, 0)
    spread_bias(v.g0, v.gf, v.rbias, True, None)
    row_attend(mload, 0, send(v.s0, v.r0, 8, rl))
    comm.swap_finish(v.s0, v.r0, 8)

    fill(v.mwork, v.r0)
    cload = lambda i: take(v.mwork, i, ns, rl)
    col_project(cload, 0)

    def keep_four(t, new, newf):
        for n, x in enumerate(new):
            v.mc[4 * t + n] = x
    col_attend(0, rl // 2)
    col_out(cload, 0, keep_four, v.loc0, v.g1, lambda t: comm.relay_start(v.g1, 1, t, nc))

    c2load = lambda i: v.mc[i].astype(F32)

    def send_four(t, new, newf):
        for n in range(2):
            stage(v.s1, 2 * t + n, newf[2 * n], newf[2 * n + 1], nd)
    col_project(c2load, 1, lambda t: comm.relay_step(v.g1, 1, 1, t, nc))
    col_attend(0, rl // 4, lambda t: comm.relay_step(v.g1, 1, 2, t, nc))
    col_attend(rl // 4, rl // 4, lambda t: comm.relay_step(v.g1, 1, 3, t, nc))
    col_out(c2load, 1, send_four, v.loc1, v.g2)
    comm.relay_finish(v.g1, 1, nc)
    comm.relay_start(v.g2, 2)
    opm(v.loc0, v.g1, 0, lambda i: v.z[i].astype(F32), v.ts_b[0], v.g3, 3, lambda: comm.relay_step(v.g2, 2, 1))
    comm.relay_step(v.g2, 2, 2)
    tri_project(v.ts_w.at[0])
    comm.gather_finish(v.g3, 3)
    comm.relay_step(v.g2, 2, 3)
    spread_bias(v.g3, v.gf2, v.tbias, True, mask_r())
    tri_attend(v.ts_o[0], send(v.s2, v.r2, 9, rl, v.te_b[0], v.g4))
    comm.gather_start(v.g4, 4)
    comm.swap_finish(v.s2, v.r2, 9)
    turn(v.r2)
    tri_project(v.te_w.at[0])
    comm.gather_finish(v.g4, 4)
    comm.swap_start(v.s1, v.r1, 10, 0, rows_m)
    spread_bias(v.g4, v.gf2, v.tbias, False, mask_r())
    tri_attend(v.te_o[0], keep(v.zc, v.row_b[1], v.g5))


    comm.relay_finish(v.g2, 2)
    comm.relay_start(v.g5, 5)
    opm(v.loc1, v.g2, 1, zload, v.te_b[1], v.g6, 6, lambda: comm.relay_step(v.g5, 5, 1))
    comm.relay_step(v.g5, 5, 2)
    comm.swap_finish(v.s1, v.r1, 10)
    fill(v.mwork, v.r1)
    rload = lambda s: take(v.mwork, s, nr, sl)
    row_project(rload, 1)
    comm.relay_step(v.g5, 5, 3)
    tri_project(v.te_w.at[1])
    comm.gather_finish(v.g6, 6)
    spread_bias(v.g6, v.gf2, v.tbias, True, mask_r())
    tri_attend(v.te_o[1], send(v.s3, v.r3, 11, rl, v.ts_b[1], v.g7))
    comm.gather_start(v.g7, 7)
    comm.relay_finish(v.g5, 5)
    spread_bias(v.g5, v.gf, v.rbias, False, None)
    row_attend(rload, 1, keep(v.m_out))
    comm.swap_finish(v.s3, v.r3, 11)
    turn(v.r3)
    tri_project(v.ts_w.at[1])
    comm.gather_finish(v.g7, 7)
    spread_bias(v.g7, v.gf2, v.tbias, False, mask_r())
    tri_attend(v.ts_o[1], keep(v.z_out))


def solution(mesh):
    nd = mesh.shape['dap']

    def local_step(m, z, msa_mask, res_mask, w_row_bias, w_row_in, w_row_out, w_col_in, w_col_out, w_opm_in, w_opm_out, w_ts_bias, w_ts_in, w_ts_out, w_te_bias, w_te_in, w_te_out):
        sl, nr, cm = m.shape
        rl, _, cz = z.shape
        ns = sl * nd
        hm, ht = w_row_bias.shape[2], w_ts_bias.shape[2]
        wm, wz = hm * HEAD, ht * HEAD
        od = w_opm_in.shape[3]

        def rows_of(w):
            return jnp.moveaxis(w, 1, -1).reshape(2, -1, w.shape[1])

        ins = dict(m=m, z=z, msa_mask=msa_mask, res_mask=res_mask[None, :],
                   row_w=rows_of(w_row_in), row_o=w_row_out.reshape(2, wm, cm), row_b=rows_of(w_row_bias),
                   col_w=rows_of(w_col_in), col_o=w_col_out.reshape(2, wm, cm),
                   ts_w=rows_of(w_ts_in), ts_o=w_ts_out.reshape(2, wz, cz), ts_b=rows_of(w_ts_bias),
                   te_w=rows_of(w_te_in), te_o=w_te_out.reshape(2, wz, cz), te_b=rows_of(w_te_bias),
                   opm_i=rows_of(w_opm_in), opm_o=w_opm_out.reshape(2, od * od, cz))
        outs = dict(m_out=m, z_out=z)
        gm, gz = wm // 128, wz // 128
        xm, xz = (nd, sl * rl, cm), (nd, rl * rl, cz)
        grow, gtri, gopm = (nd * rl, hm, nr), (nd * rl, ht, nr), (nd * rl, od, ns)
        scratch = dict(
            s0=(xm, BF16), r0=(xm, BF16), s1=(xm, BF16), r1=(xm, BF16),
            s2=(xz, BF16), r2=(xz, BF16), s3=(xz, BF16), r3=(xz, BF16),
            g0=(grow, BF16), g5=(grow, BF16), g1=(gopm, BF16), g2=(gopm, BF16),
            g3=(gtri, BF16), g4=(gtri, BF16), g6=(gtri, BF16), g7=(gtri, BF16),
            gf=(grow, F32), gf2=(gtri, F32), rbias=((gm, nr, 4 * nr), F32), tbias=((gz, nr, 4 * nr), F32),
            mwork=((cm // 128, nd * sl * rl, 128), F32), zwork=((cz // 128, nr * rl, 128), F32),
            gcol=((nr * od, ns), F32), xs=((rl, od * od, nr), BF16), nrm=((rl, nr), F32), kc=((nr, wz), F32),
            rt=((sl, 3 * wm, nr), BF16), rk=((sl, nr, wm), BF16), ro=((sl, wm, nr), BF16),
            ct=((rl, 3 * wm, ns), BF16), ck=((rl, ns, wm), BF16), co=((rl, wm, ns), BF16),
            tt=((rl, 3 * wz, nr), BF16), tk=((rl, nr, wz), BF16), to=((rl, wz, nr), BF16),
            mask_t=((nr, ns), F32), mask_seq=((sl, nr), F32), mask_col=((rl, ns), F32), opm_w=((2, cz, od * od), BF16),
            mc=((rl, ns, cm), BF16), zc=((rl, nr, cz), BF16), loc0=((rl, od, ns), BF16), loc1=((rl, od, ns), BF16))
        sems = dict(ssem=(12,), rsem=(12,), fsem=(8,), gsem=(8, nd // 2, 3))
        late = [k for k in ins if k not in ('z', 'row_b')]
        for k in late:
            scratch[k] = (ins[k].shape, ins[k].dtype)
        sems['lsem'] = (len(late),)
        names = ['hbm_' + k if k in late else k for k in ins] + list(outs) + list(scratch) + list(sems)
        return pl.pallas_call(
            lambda *refs: kernel(names, late, nd, refs),
            out_shape=[jax.ShapeDtypeStruct(o.shape, o.dtype) for o in outs.values()],
            in_specs=[pl.BlockSpec(memory_space=pl.ANY if k in late else pltpu.VMEM) for k in ins],
            out_specs=[pl.BlockSpec(memory_space=pltpu.VMEM)] * len(outs),
            scratch_shapes=[pltpu.VMEM(*x) for x in scratch.values()] + [pltpu.SemaphoreType.DMA(x) for x in sems.values()],
            compiler_params=pltpu.CompilerParams(collective_id=0, has_side_effects=True, vmem_limit_bytes=67043328),
        )(*ins.values())

    in_specs = (P(('data', 'dap')), P(('data', 'dap')), P('data'), P('data')) + (P(),) * 13
    out_specs = (P(('data', 'dap')), P(('data', 'dap')))
    return jax.shard_map(local_step, mesh=mesh, in_specs=in_specs, out_specs=out_specs, check_vma=False)
```

```python
import functools

import jax
import jax.numpy as jnp
from jax import lax
from jax.experimental import pallas as pl
from jax.experimental.pallas import tpu as pltpu
from jax.sharding import PartitionSpec as P

F32 = jnp.float32
BF16 = jnp.bfloat16
LOG2E = 1.4426950408889634
NEG = -1e9 * LOG2E
HEAD = 32
MESH = pl.DeviceIdType.MESH


def dot(lhs, rhs, lc, rc):
    return lax.dot_general(lhs, rhs, (((lc,), (rc,)), ((), ())), preferred_element_type=F32)


def layer_norm(x):
    mean = jnp.mean(x, axis=-1, keepdims=True)
    cen = x - mean
    var = jnp.mean(cen * cen, axis=-1, keepdims=True)
    return (cen * lax.rsqrt(var + 1e-5)).astype(BF16)


def project(xs, w, t_ref, k_ref, first, kcol):
    width = w.shape[0] // 4
    xl = [layer_norm(x) for x in xs]
    for n, v in enumerate([dot(w[:width], v, 1, 1) for v in xl]):
        t_ref[first + n, 0:width] = v.astype(BF16)
    for n, v in enumerate([dot(w[2 * width:], v, 1, 1) for v in xl]):
        t_ref[first + n, width:3 * width] = v.astype(BF16)
    for n, v in enumerate([dot(v, w[width:2 * width], 1, 1) for v in xl]):
        if kcol is not None:
            v = v * kcol
        k_ref[first + n] = v.astype(BF16)


def diagonal(t, base, length):
    cols = []
    for r in range(4):
        parts = [t[base + HEAD * r:base + HEAD * r + HEAD]]
        if r > 0:
            parts.insert(0, jnp.zeros((HEAD * r, length), BF16))
        if r < 3:
            parts.append(jnp.zeros((HEAD * (3 - r), length), BF16))
        cols.append(jnp.concatenate(parts, axis=0))
    return jnp.concatenate(cols, axis=1)


def core(t_ref, k_ref, o_ref, rows, groups, bias, keeps):
    length = k_ref.shape[1]
    width = 128 * groups
    units = [(n, b, g) for n, b in enumerate(rows) for g in range(groups)]
    scores = []
    for n, b, g in units:
        t = t_ref[b, 128 * g:128 * g + 128, :]
        scores.append(dot(k_ref[b, :, 128 * g:128 * g + 128], diagonal(t, 0, length), 1, 0))
    yield
    probs = []
    dens = []
    for (n, b, g), s in zip(units, scores):
        s = s * (HEAD ** -0.5 * LOG2E)
        if bias is not None:
            s = s + bias[g]
        if keeps is not None:
            s = jnp.where(keeps[n] > 0, s, NEG)
        e = jnp.exp2(s - jnp.max(s, axis=0, keepdims=True))
        dens.append(jnp.sum(e, axis=0, keepdims=True))
        probs.append(e.astype(BF16))
    yield
    outs = [dot(t_ref[b, width + 128 * g:width + 128 * g + 128, :], p, 1, 0) for (n, b, g), p in zip(units, probs)]
    yield
    for (n, b, g), o, den in zip(units, outs, dens):
        inv = 1.0 / den
        gate = jax.nn.sigmoid(t_ref[b, 2 * width + 128 * g:2 * width + 128 * g + 128, :].astype(F32))
        parts = []
        for r in range(4):
            lanes = slice(length * r, length * r + length)
            parts.append(o[HEAD * r:HEAD * r + HEAD, lanes] * inv[:, lanes])
        o_ref[b, 128 * g:128 * g + 128, :] = (jnp.concatenate(parts, axis=0) * gate).astype(BF16)


def interleave(*gens):
    live = list(gens)
    while live:
        for gen in list(live):
            try:
                next(gen)
            except StopIteration:
                live.remove(gen)


def residual(x, update):
    return (x + update).astype(BF16)


def spread(row, lanes):
    return jnp.broadcast_to(row, (lanes, row.shape[1])).T


def widen(block, lanes):
    return jnp.concatenate([block] * (lanes // 128), axis=1)


def stage(stg, pair, first, second, ndev):
    rows = first.shape[0] // ndev
    off = pl.multiple_of(2 * rows * pair, 8)
    for d in range(ndev):
        both = jnp.concatenate([first[rows * d:rows * d + rows], second[rows * d:rows * d + rows]], axis=0)
        stg[d, pl.ds(off, 2 * rows), :] = both.astype(BF16)


def fill(work, ref):
    few = ref.shape[0] // 4
    rows = few * ref.shape[1]

    def body(j, _):
        for t in range(work.shape[0]):
            value = ref[pl.ds(few * j, few), :, 128 * t:128 * t + 128].astype(F32).reshape(rows, 128)
            work[t, pl.ds(pl.multiple_of(rows * j, 8), rows), :] = value
        return 0
    lax.fori_loop(0, 4, body, 0)


def take(work, start, count, stride):
    return jnp.concatenate([work.at[t][pl.ds(start, count, stride=stride), :] for t in range(work.shape[0])], axis=1)


def put_piece(buf, index, p):
    half = p.shape[0] // 2
    buf[index, 0] = p[:half, :128].astype(BF16)
    buf[index, 1] = p[half:, :128].astype(BF16)
    buf[index, 2] = jnp.concatenate([p[:half, 128:], p[half:, 128:]], axis=1).astype(BF16)


def spread_bias(gath, gf, bias, transpose, mask_row):
    length, half = gath.shape[0], gath.shape[2]
    gf[...] = gath[...].astype(F32)
    keep = None if mask_row is None else widen(spread(mask_row, 128), 4 * length)
    tails = [gf[:, 2, r, :] for r in range(half)]
    for g in range(2 * half // 4):
        parts = []
        for h in range(4 * g, 4 * g + 4):
            a, r = h // half, h % half
            value = jnp.concatenate([gf[:, a, r, :], tails[r][:, 64 * a:64 * a + 64]], axis=1)
            parts.append(value.T if transpose else value)
        value = jnp.concatenate(parts, axis=1) * LOG2E
        if keep is not None:
            value = jnp.where(keep > 0, value, NEG)
        bias[g] = value


def bias_pieces(load, count, wb, store, after):
    def body(t, _):
        zl = [layer_norm(load(4 * t + n)) for n in range(4)]
        ps = [dot(wb, v, 1, 1) for v in zl]
        for n, v in enumerate(ps):
            store(4 * t + n, v)
        after(t)
        return 0
    body(0, 0)
    lax.fori_loop(1, count // 4, body, 0)


class Comm:
    def __init__(self, nd, sems):
        self.nd = nd
        self.me = lax.axis_index('dap')
        self.partner = self.me + 1 - 2 * lax.rem(self.me, 2)
        self.ssem, self.rsem, self.fsem, self.gsem = sems

    def copy(self, src, dst, send, recv, dev):
        return pltpu.make_async_remote_copy(src_ref=src, dst_ref=dst, send_sem=send, recv_sem=recv,
                                            device_id={'dap': dev}, device_id_type=MESH)

    def near(self, k, unit):
        off = ((k + 1) // 2) * (2 * lax.rem(k, 2) - 1)
        return lax.rem(self.me + self.nd + unit * off, self.nd)

    def barrier_signal(self):
        bar = pltpu.get_barrier_semaphore()

        def body(k, _):
            pl.semaphore_signal(bar, inc=1, device_id={'dap': lax.rem(self.me + k, self.nd)}, device_id_type=MESH)
            return 0
        lax.fori_loop(1, self.nd, body, 0)

    def barrier_wait(self):
        pl.semaphore_wait(pltpu.get_barrier_semaphore(), self.nd - 1)

    def await_bytes(self, ref, sem):
        pltpu.make_async_copy(ref, ref, sem).wait()

    def at(self, chips, same=True):
        base = self.me if same else self.partner
        return lax.rem(base + self.nd + 2 * chips, self.nd)

    def slot(self, buf, chips, start=0, count=None):
        n = buf.shape[0] // self.nd
        return buf.at[pl.ds(self.at(chips) * n + start, n if count is None else count)]

    def gather_start(self, buf, i, c=0, nc=1):
        m = buf.shape[0] // self.nd // nc
        own = self.slot(buf, 0, c * m, m)

        def body(j, _):
            k = self.nd // 2 - j
            self.copy(own, own, self.ssem.at[i], self.gsem.at[i, k, 0], self.near(k, 2)).start()
            return 0
        lax.fori_loop(1, self.nd // 2, body, 0)
        self.copy(own, own, self.ssem.at[i], self.gsem.at[i, 0, 0], self.partner).start()

    def gather_finish(self, buf, i):
        n = buf.shape[0] // self.nd
        half = self.nd // 2

        def body(k, _):
            slot = buf.at[pl.ds(self.near(k, -2) * n, n)]
            self.await_bytes(slot, self.gsem.at[i, k, 0])
            self.copy(slot, slot, self.fsem.at[i], self.rsem.at[i], self.partner).start()
            return 0
        lax.fori_loop(1, half, body, 0)
        self.await_bytes(buf.at[pl.ds(0, n)], self.gsem.at[i, 0, 0])
        rest = buf.at[pl.ds(0, (half - 1) * n)]
        self.await_bytes(rest, self.rsem.at[i])
        self.await_bytes(rest, self.fsem.at[i])
        self.await_bytes(buf.at[pl.ds(0, half * n)], self.ssem.at[i])

    def relay(self, ref, i, recv, dev):
        self.copy(ref, ref, self.ssem.at[i], recv, dev).start()

    def relay_start(self, buf, i, c=0, nc=1):
        m = buf.shape[0] // self.nd // nc
        own = self.slot(buf, 0, c * m, m)
        self.relay(own, i, self.gsem.at[i, 0, c], self.at(1))
        self.relay(own, i, self.gsem.at[i, 4, c], self.at(-1))
        self.relay(own, i, self.rsem.at[i], self.partner)

    def relay_step(self, buf, i, p, c=0, nc=1):
        m = buf.shape[0] // self.nd // nc
        for part, sign in ((0, 1), (1, -1)):
            ref = self.slot(buf, -sign * p, c * m, m)
            self.await_bytes(ref, self.gsem.at[i, 4 * part + p - 1, c])
            on = self.slot(buf, -sign * p, c * m + part * (m // 2), m // 2) if p == self.nd // 4 - 1 else ref
            self.relay(on, i, self.gsem.at[i, 4 * part + p, c], self.at(sign))
            self.relay(ref, i, self.rsem.at[i], self.partner)

    def relay_finish(self, buf, i, nc=1):
        n = buf.shape[0] // self.nd
        m = n // nc
        half = self.nd // 2
        for c in range(nc):
            for part in range(2):
                ref = self.slot(buf, self.nd // 4, c * m + part * (m // 2), m // 2)
                self.await_bytes(ref, self.gsem.at[i, 4 * part + self.nd // 4 - 1, c])
        self.relay(self.slot(buf, self.nd // 4), i, self.rsem.at[i], self.partner)
        self.await_bytes(buf.at[pl.ds(0, half * n)], self.rsem.at[i])
        self.await_bytes(buf.at[pl.ds(0, (2 * half - 1) * n)], self.ssem.at[i])

    def swap_start(self, send, recv, i, t, rows):
        part = pl.ds(pl.multiple_of(rows * t, 8), rows)
        for k in range(self.nd - 1, 0, -1):
            off = (k + 1) // 2 if k % 2 else -(k // 2)
            d = lax.rem(self.me + self.nd + off, self.nd)
            self.copy(send.at[d, part], recv.at[self.me, part], self.ssem.at[i], self.rsem.at[i], d).start()
        pltpu.make_async_copy(send.at[self.me, part], recv.at[self.me, part], self.rsem.at[i]).start()

    def swap_finish(self, send, recv, i):
        self.await_bytes(recv, self.rsem.at[i])
        self.await_bytes(send.at[pl.ds(0, self.nd - 1)], self.ssem.at[i])


def kernel(names, late, nd, refs):
    r = dict(zip(names, refs))
    class N:
        pass
    v = N()
    v.__dict__.update(r)
    sl, nr, cm = v.m.shape
    rl, _, cz = v.z.shape
    ns = sl * nd
    wm, wz = v.row_w.shape[1] // 4, v.ts_w.shape[1] // 4
    gm, gz = wm // 128, wz // 128
    od = v.opm_i.shape[1] // 2
    def late_start():
        for n, name in enumerate(late):
            pltpu.make_async_copy(r['hbm_' + name], r[name], v.lsem.at[n]).start()

    def late_wait():
        for n, name in enumerate(late):
            pltpu.make_async_copy(r['hbm_' + name], r[name], v.lsem.at[n]).wait()

    comm = Comm(nd, (v.ssem, v.rsem, v.fsem, v.gsem))
    me = comm.me
    rows_m = sl * rl

    def store_piece(buf):
        def store(i, val):
            put_piece(buf, me * rl + i, val)
        return store

    def loop(n, body):
        def step(t, _):
            body(t)
            return 0
        lax.fori_loop(0, n, step, 0)

    def row_project(load, b):
        loop(sl // 2, lambda t: project([load(2 * t), load(2 * t + 1)], v.row_w.at[b], v.rt, v.rk, 2 * t, None))

    def row_attend(load, b, finish):
        def attend(s):
            keep = widen(spread(v.mask_seq[pl.ds(s, 1), :], 128), 4 * nr)
            return core(v.rt, v.rk, v.ro, [s], gm, v.rbias, [keep])

        def back(t):
            ups = [dot(v.ro[2 * t + n], v.row_o[b], 0, 0) for n in range(2)]
            yield
            yield from finish(t, [residual(load(2 * t + n), ups[n]) for n in range(2)])

        def body(u):
            interleave(back(u), attend(2 * u + 2))
            interleave(attend(2 * u + 3))
        interleave(attend(0))
        interleave(attend(1))
        loop(sl // 2 - 1, body)
        interleave(back(sl // 2 - 1))

    def col_project(load, b, after=lambda t: None):
        def body(t):
            project([load(4 * t + n) for n in range(4)], v.col_w.at[b], v.ct, v.ck, 4 * t, None)
            after(t)
        loop(rl // 4, body)

    def col_attend(first, count, after=lambda u: None):
        def body(u):
            t = first + u
            rows = [2 * t, 2 * t + 1]
            keeps = [widen(spread(v.mask_col[pl.ds(i, 1), :], 128), 4 * ns) for i in rows]
            interleave(core(v.ct, v.ck, v.co, rows, gm, None, keeps))
            after(u)
        loop(count, body)

    def col_out(load, b, finish, loc, gat, after=lambda t: None):
        def out(t):
            rows = [4 * t + n for n in range(4)]
            ups = [dot(v.co[i], v.col_o[b], 0, 0) for i in rows]
            new = [residual(load(i), u) for i, u in zip(rows, ups)]
            newf = [x.astype(F32) for x in new]
            finish(t, new, newf)
            ln = [layer_norm(x) for x in newf]
            acs = [dot(v.opm_i[b], x, 1, 1) for x in ln]
            for i, x in zip(rows, acs):
                ac = (x * v.mask_col[pl.ds(i, 1), :]).astype(BF16)
                a, c = ac[:od], ac[od:]
                loc[i] = a if b == 0 else c
                gat[me * rl + i] = c if b == 0 else a
            after(t)
        loop(rl // 4, out)

    def opm(loc, gat, b, load, wb, piece, i_piece, between):
        few = nr // 8

        def widen_gathered(j):
            value = gat[pl.ds(few * j, few)].astype(F32).reshape(few * od, ns)
            v.gcol[pl.ds(pl.multiple_of(few * od * j, 8), few * od), :] = value
        loop(8, widen_gathered)
        v.nrm[...] = dot(v.mask_col[...].astype(BF16), v.msa_mask[...].astype(F32).astype(BF16), 1, 0)

        def grow(t):
            left = loc[...].reshape(rl * od, ns)
            for n in range(4):
                g = 4 * t + n
                col = v.gcol[pl.ds(g, nr, stride=od), :].astype(BF16)
                x = dot(left, col, 1, 1).astype(BF16)
                off = pl.multiple_of(g * od, od)
                for i in range(rl):
                    v.xs[i, pl.ds(off, od), :] = x[od * i:od * i + od]
        loop(od // 4, grow)
        between()

        def fold(t):
            rows = [4 * t + n for n in range(4)]
            ups = [dot(v.opm_w[b], v.xs[i], 1, 0) for i in rows]
            ups = [u / (1e-3 + v.nrm[pl.ds(i, 1), :]) for i, u in zip(rows, ups)]
            ups = [u.T for u in ups]
            new = [residual(load(i), u) for i, u in zip(rows, ups)]
            for i, x in zip(rows, new):
                v.zc[i] = x
            ln = [layer_norm(x.astype(F32)) for x in new]
            ps = [dot(wb, x, 1, 1) for x in ln]
            for i, x in zip(rows, ps):
                put_piece(piece, me * rl + i, x)
            comm.gather_start(piece, i_piece, t, rl // 4)
        loop(rl // 4, fold)

    def zload(i):
        return v.zc[i].astype(F32)

    def tri_project(w):
        loop(rl // 4, lambda t: project([zload(4 * t + n) for n in range(4)], w, v.tt, v.tk, 4 * t, v.kc[...]))

    def tri_attend(wo, finish):
        def attend(t):
            return core(v.tt, v.tk, v.to, [4 * t + n for n in range(4)], gz, v.tbias, None)

        def back(t):
            rows = [4 * t + n for n in range(4)]
            ups = [dot(v.to[i], wo, 0, 0) for i in rows]
            yield
            yield from finish(t, [residual(zload(i), u) for i, u in zip(rows, ups)])

        interleave(attend(0))
        loop(rl // 4 - 1, lambda u: interleave(back(u), attend(u + 1)))
        interleave(back(rl // 4 - 1))

    def pieces(t, new, wb, piece):
        ln = [layer_norm(x.astype(F32)) for x in new]
        yield
        ps = [dot(wb, x, 1, 1) for x in ln]
        for n, x in enumerate(ps):
            put_piece(piece, me * rl + len(new) * t + n, x)

    def send(out, recv, i, rows, wb=None, piece=None):
        def finish(t, new):
            half = len(new) // 2
            for n in range(half):
                stage(out, half * t + n, new[2 * n].astype(F32), new[2 * n + 1].astype(F32), nd)
            count = len(new) * rows
            comm.swap_start(out, recv, i, t, count)
            if piece is not None:
                yield from pieces(t, new, wb, piece)
            else:
                yield
        return finish

    def keep(out, wb=None, piece=None):
        def finish(t, new):
            for n, x in enumerate(new):
                out[len(new) * t + n] = x
            if piece is not None:
                yield from pieces(t, new, wb, piece)
            else:
                yield
        return finish

    def turn(recv):
        fill(v.zwork, recv)
        for b in range(rl):
            v.zc[b] = take(v.zwork, b, nr, rl).astype(BF16)

    def mask_r():
        return v.res_mask[...].astype(F32)

    def prepare():
        v.mask_t[...] = v.msa_mask[...].astype(F32).T
        v.mask_seq[...] = v.msa_mask[pl.ds(pl.multiple_of(me * sl, sl), sl), :].astype(F32)
        for i in range(rl):
            v.mask_col[pl.ds(i, 1), :] = v.mask_t[pl.ds(me * rl + i, 1), :]
        v.kc[...] = spread(mask_r(), wz)
        size = od * od
        v.gcol[0:size] = v.opm_o[0].astype(F32)
        for q in range(od):
            v.gcol[size + od * q:size + od * q + od] = v.gcol[pl.ds(q, od, stride=od), :]
        for j in range(size // 128):
            v.opm_w[0, :, 128 * j:128 * j + 128] = v.gcol[size + 128 * j:size + 128 * j + 128].T.astype(BF16)
            v.opm_w[1, :, 128 * j:128 * j + 128] = v.opm_o[1, 128 * j:128 * j + 128, :].astype(F32).T.astype(BF16)

    comm.barrier_signal()
    late_start()
    nc = rl // 4

    def first_send(t):
        if isinstance(t, int) and t == 0:
            comm.barrier_wait()
        comm.gather_start(v.g0, 0, t, nc)
    bias_pieces(lambda i: v.z[i].astype(F32), rl, v.row_b[0], store_piece(v.g0), first_send)
    late_wait()
    mload = lambda s: v.m[s].astype(F32)
    row_project(mload, 0)
    prepare()
    comm.gather_finish(v.g0, 0)
    spread_bias(v.g0, v.gf, v.rbias, True, None)
    row_attend(mload, 0, send(v.s0, v.r0, 8, rl))
    comm.swap_finish(v.s0, v.r0, 8)

    fill(v.mwork, v.r0)
    cload = lambda i: take(v.mwork, i, ns, rl)
    col_project(cload, 0)

    def keep_four(t, new, newf):
        for n, x in enumerate(new):
            v.mc[4 * t + n] = x
    col_attend(0, rl // 2)
    col_out(cload, 0, keep_four, v.loc0, v.g1, lambda t: comm.relay_start(v.g1, 1, t, nc))

    c2load = lambda i: v.mc[i].astype(F32)

    def send_four(t, new, newf):
        for n in range(2):
            stage(v.s1, 2 * t + n, newf[2 * n], newf[2 * n + 1], nd)
    col_project(c2load, 1, lambda t: comm.relay_step(v.g1, 1, 1, t, nc))
    col_attend(0, rl // 4, lambda t: comm.relay_step(v.g1, 1, 2, t, nc))
    col_attend(rl // 4, rl // 4, lambda t: comm.relay_step(v.g1, 1, 3, t, nc))
    col_out(c2load, 1, send_four, v.loc1, v.g2)
    comm.relay_finish(v.g1, 1, nc)
    comm.relay_start(v.g2, 2)
    opm(v.loc0, v.g1, 0, lambda i: v.z[i].astype(F32), v.ts_b[0], v.g3, 3, lambda: comm.relay_step(v.g2, 2, 1))
    comm.relay_step(v.g2, 2, 2)
    tri_project(v.ts_w.at[0])
    comm.gather_finish(v.g3, 3)
    comm.relay_step(v.g2, 2, 3)
    spread_bias(v.g3, v.gf2, v.tbias, True, mask_r())
    tri_attend(v.ts_o[0], send(v.s2, v.r2, 9, rl, v.te_b[0], v.g4))
    comm.gather_start(v.g4, 4)
    comm.swap_finish(v.s2, v.r2, 9)
    turn(v.r2)
    tri_project(v.te_w.at[0])
    comm.gather_finish(v.g4, 4)
    comm.swap_start(v.s1, v.r1, 10, 0, rows_m)
    spread_bias(v.g4, v.gf2, v.tbias, False, mask_r())
    tri_attend(v.te_o[0], keep(v.zc, v.row_b[1], v.g5))


    comm.relay_finish(v.g2, 2)
    comm.relay_start(v.g5, 5)
    opm(v.loc1, v.g2, 1, zload, v.te_b[1], v.g6, 6, lambda: comm.relay_step(v.g5, 5, 1))
    comm.relay_step(v.g5, 5, 2)
    comm.swap_finish(v.s1, v.r1, 10)
    fill(v.mwork, v.r1)
    rload = lambda s: take(v.mwork, s, nr, sl)
    row_project(rload, 1)
    comm.relay_step(v.g5, 5, 3)
    tri_project(v.te_w.at[1])
    comm.gather_finish(v.g6, 6)
    spread_bias(v.g6, v.gf2, v.tbias, True, mask_r())
    tri_attend(v.te_o[1], send(v.s3, v.r3, 11, rl, v.ts_b[1], v.g7))
    comm.gather_start(v.g7, 7)
    comm.relay_finish(v.g5, 5)
    spread_bias(v.g5, v.gf, v.rbias, False, None)
    row_attend(rload, 1, keep(v.m_out))
    comm.swap_finish(v.s3, v.r3, 11)
    turn(v.r3)
    tri_project(v.ts_w.at[1])
    comm.gather_finish(v.g7, 7)
    spread_bias(v.g7, v.gf2, v.tbias, False, mask_r())
    tri_attend(v.ts_o[1], keep(v.z_out))


def solution(mesh):
    nd = mesh.shape['dap']

    def local_step(m, z, msa_mask, res_mask, w_row_bias, w_row_in, w_row_out, w_col_in, w_col_out, w_opm_in, w_opm_out, w_ts_bias, w_ts_in, w_ts_out, w_te_bias, w_te_in, w_te_out):
        sl, nr, cm = m.shape
        rl, _, cz = z.shape
        ns = sl * nd
        hm, ht = w_row_bias.shape[2], w_ts_bias.shape[2]
        wm, wz = hm * HEAD, ht * HEAD
        od = w_opm_in.shape[3]

        def rows_of(w):
            return jnp.moveaxis(w, 1, -1).reshape(2, -1, w.shape[1])

        ins = dict(m=m, z=z, msa_mask=msa_mask, res_mask=res_mask[None, :],
                   row_w=rows_of(w_row_in), row_o=w_row_out.reshape(2, wm, cm), row_b=rows_of(w_row_bias),
                   col_w=rows_of(w_col_in), col_o=w_col_out.reshape(2, wm, cm),
                   ts_w=rows_of(w_ts_in), ts_o=w_ts_out.reshape(2, wz, cz), ts_b=rows_of(w_ts_bias),
                   te_w=rows_of(w_te_in), te_o=w_te_out.reshape(2, wz, cz), te_b=rows_of(w_te_bias),
                   opm_i=rows_of(w_opm_in), opm_o=w_opm_out.reshape(2, od * od, cz))
        outs = dict(m_out=m, z_out=z)
        gm, gz = wm // 128, wz // 128
        xm, xz = (nd, sl * rl, cm), (nd, rl * rl, cz)
        grow, gtri, gopm = (nd * rl, 3, hm // 2, 128), (nd * rl, 3, ht // 2, 128), (nd * rl, od, ns)
        scratch = dict(
            s0=(xm, BF16), r0=(xm, BF16), s1=(xm, BF16), r1=(xm, BF16),
            s2=(xz, BF16), r2=(xz, BF16), s3=(xz, BF16), r3=(xz, BF16),
            g0=(grow, BF16), g5=(grow, BF16), g1=(gopm, BF16), g2=(gopm, BF16),
            g3=(gtri, BF16), g4=(gtri, BF16), g6=(gtri, BF16), g7=(gtri, BF16),
            gf=(grow, F32), gf2=(gtri, F32), rbias=((gm, nr, 4 * nr), F32), tbias=((gz, nr, 4 * nr), F32),
            mwork=((cm // 128, nd * sl * rl, 128), F32), zwork=((cz // 128, nr * rl, 128), F32),
            gcol=((nr * od, ns), F32), xs=((rl, od * od, nr), BF16), nrm=((rl, nr), F32), kc=((nr, wz), F32),
            rt=((sl, 3 * wm, nr), BF16), rk=((sl, nr, wm), BF16), ro=((sl, wm, nr), BF16),
            ct=((rl, 3 * wm, ns), BF16), ck=((rl, ns, wm), BF16), co=((rl, wm, ns), BF16),
            tt=((rl, 3 * wz, nr), BF16), tk=((rl, nr, wz), BF16), to=((rl, wz, nr), BF16),
            mask_t=((nr, ns), F32), mask_seq=((sl, nr), F32), mask_col=((rl, ns), F32), opm_w=((2, cz, od * od), BF16),
            mc=((rl, ns, cm), BF16), zc=((rl, nr, cz), BF16), loc0=((rl, od, ns), BF16), loc1=((rl, od, ns), BF16))
        sems = dict(ssem=(12,), rsem=(12,), fsem=(8,), gsem=(8, nd // 2, 3))
        late = [k for k in ins if k not in ('z', 'row_b')]
        for k in late:
            scratch[k] = (ins[k].shape, ins[k].dtype)
        sems['lsem'] = (len(late),)
        names = ['hbm_' + k if k in late else k for k in ins] + list(outs) + list(scratch) + list(sems)
        return pl.pallas_call(
            lambda *refs: kernel(names, late, nd, refs),
            out_shape=[jax.ShapeDtypeStruct(o.shape, o.dtype) for o in outs.values()],
            in_specs=[pl.BlockSpec(memory_space=pl.ANY if k in late else pltpu.VMEM) for k in ins],
            out_specs=[pl.BlockSpec(memory_space=pltpu.VMEM)] * len(outs),
            scratch_shapes=[pltpu.VMEM(*x) for x in scratch.values()] + [pltpu.SemaphoreType.DMA(x) for x in sems.values()],
            compiler_params=pltpu.CompilerParams(collective_id=0, has_side_effects=True, vmem_limit_bytes=67043328),
        )(*ins.values())

    in_specs = (P(('data', 'dap')), P(('data', 'dap')), P('data'), P('data')) + (P(),) * 13
    out_specs = (P(('data', 'dap')), P(('data', 'dap')))
    return jax.shard_map(local_step, mesh=mesh, in_specs=in_specs, out_specs=out_specs, check_vma=False)
```

```python
import functools

import jax
import jax.numpy as jnp
from jax import lax
from jax.experimental import pallas as pl
from jax.experimental.pallas import tpu as pltpu
from jax.sharding import PartitionSpec as P

F32 = jnp.float32
BF16 = jnp.bfloat16
LOG2E = 1.4426950408889634
NEG = -1e9 * LOG2E
HEAD = 32
MESH = pl.DeviceIdType.MESH


def dot(lhs, rhs, lc, rc):
    return lax.dot_general(lhs, rhs, (((lc,), (rc,)), ((), ())), preferred_element_type=F32)


def layer_norm(x):
    mean = jnp.mean(x, axis=-1, keepdims=True)
    cen = x - mean
    var = jnp.mean(cen * cen, axis=-1, keepdims=True)
    return (cen * lax.rsqrt(var + 1e-5)).astype(BF16)


def project(xs, w, t_ref, k_ref, first, kcol):
    width = w.shape[0] // 4
    xl = [layer_norm(x) for x in xs]
    for n, v in enumerate([dot(w[:width], v, 1, 1) for v in xl]):
        t_ref[first + n, 0:width] = v.astype(BF16)
    for n, v in enumerate([dot(w[2 * width:], v, 1, 1) for v in xl]):
        t_ref[first + n, width:3 * width] = v.astype(BF16)
    for n, v in enumerate([dot(v, w[width:2 * width], 1, 1) for v in xl]):
        if kcol is not None:
            v = v * kcol
        k_ref[first + n] = v.astype(BF16)


def diagonal(t, base, length):
    cols = []
    for r in range(4):
        parts = [t[base + HEAD * r:base + HEAD * r + HEAD]]
        if r > 0:
            parts.insert(0, jnp.zeros((HEAD * r, length), BF16))
        if r < 3:
            parts.append(jnp.zeros((HEAD * (3 - r), length), BF16))
        cols.append(jnp.concatenate(parts, axis=0))
    return jnp.concatenate(cols, axis=1)


def core(t_ref, k_ref, o_ref, rows, groups, bias, keeps):
    length = k_ref.shape[1]
    width = 128 * groups
    units = [(n, b, g) for n, b in enumerate(rows) for g in range(groups)]
    scores = []
    for n, b, g in units:
        t = t_ref[b, 128 * g:128 * g + 128, :]
        scores.append(dot(k_ref[b, :, 128 * g:128 * g + 128], diagonal(t, 0, length), 1, 0))
    yield
    probs = []
    dens = []
    for (n, b, g), s in zip(units, scores):
        s = s * (HEAD ** -0.5 * LOG2E)
        if bias is not None:
            s = s + bias[g]
        if keeps is not None:
            s = jnp.where(keeps[n] > 0, s, NEG)
        e = jnp.exp2(s - jnp.max(s, axis=0, keepdims=True))
        dens.append(jnp.sum(e, axis=0, keepdims=True))
        probs.append(e.astype(BF16))
    yield
    outs = [dot(t_ref[b, width + 128 * g:width + 128 * g + 128, :], p, 1, 0) for (n, b, g), p in zip(units, probs)]
    yield
    for (n, b, g), o, den in zip(units, outs, dens):
        inv = 1.0 / den
        gate = jax.nn.sigmoid(t_ref[b, 2 * width + 128 * g:2 * width + 128 * g + 128, :].astype(F32))
        parts = []
        for r in range(4):
            lanes = slice(length * r, length * r + length)
            parts.append(o[HEAD * r:HEAD * r + HEAD, lanes] * inv[:, lanes])
        o_ref[b, 128 * g:128 * g + 128, :] = (jnp.concatenate(parts, axis=0) * gate).astype(BF16)


def interleave(*gens):
    live = list(gens)
    while live:
        for gen in list(live):
            try:
                next(gen)
            except StopIteration:
                live.remove(gen)


def residual(x, update):
    return (x + update).astype(BF16)


def spread(row, lanes):
    return jnp.broadcast_to(row, (lanes, row.shape[1])).T


def widen(block, lanes):
    return jnp.concatenate([block] * (lanes // 128), axis=1)


def stage(stg, pair, first, second, ndev):
    rows = first.shape[0] // ndev
    off = pl.multiple_of(2 * rows * pair, 8)
    for d in range(ndev):
        both = jnp.concatenate([first[rows * d:rows * d + rows], second[rows * d:rows * d + rows]], axis=0)
        stg[d, pl.ds(off, 2 * rows), :] = both.astype(BF16)


def fill(work, ref):
    few = ref.shape[0] // 4
    rows = few * ref.shape[1]

    def body(j, _):
        for t in range(work.shape[0]):
            value = ref[pl.ds(few * j, few), :, 128 * t:128 * t + 128].astype(F32).reshape(rows, 128)
            work[t, pl.ds(pl.multiple_of(rows * j, 8), rows), :] = value
        return 0
    lax.fori_loop(0, 4, body, 0)


def take(work, start, count, stride):
    return jnp.concatenate([work.at[t][pl.ds(start, count, stride=stride), :] for t in range(work.shape[0])], axis=1)


def put_piece(buf, index, p):
    half = p.shape[0] // 2
    buf[index, 0] = p[:half, :128].astype(BF16)
    buf[index, 1] = p[half:, :128].astype(BF16)
    buf[index, 2] = jnp.concatenate([p[:half, 128:], p[half:, 128:]], axis=1).astype(BF16)


def spread_bias(gath, gf, bias, transpose, mask_row):
    length, half = gath.shape[0], gath.shape[2]
    gf[...] = gath[...].astype(F32)
    keep = None if mask_row is None else widen(spread(mask_row, 128), 4 * length)
    tails = [gf[:, 2, r, :] for r in range(half)]
    for g in range(2 * half // 4):
        parts = []
        for h in range(4 * g, 4 * g + 4):
            a, r = h // half, h % half
            value = jnp.concatenate([gf[:, a, r, :], tails[r][:, 64 * a:64 * a + 64]], axis=1)
            parts.append(value.T if transpose else value)
        value = jnp.concatenate(parts, axis=1) * LOG2E
        if keep is not None:
            value = jnp.where(keep > 0, value, NEG)
        bias[g] = value


def bias_pieces(load, count, wb, store, after):
    def body(t, _):
        zl = [layer_norm(load(4 * t + n)) for n in range(4)]
        ps = [dot(wb, v, 1, 1) for v in zl]
        for n, v in enumerate(ps):
            store(4 * t + n, v)
        after(t)
        return 0
    body(0, 0)
    lax.fori_loop(1, count // 4, body, 0)


class Comm:
    def __init__(self, nd, sems):
        self.nd = nd
        self.me = lax.axis_index('dap')
        self.partner = self.me + 1 - 2 * lax.rem(self.me, 2)
        self.ssem, self.rsem, self.fsem, self.gsem = sems

    def copy(self, src, dst, send, recv, dev):
        return pltpu.make_async_remote_copy(src_ref=src, dst_ref=dst, send_sem=send, recv_sem=recv,
                                            device_id={'dap': dev}, device_id_type=MESH)

    def near(self, k, unit):
        off = ((k + 1) // 2) * (2 * lax.rem(k, 2) - 1)
        return lax.rem(self.me + self.nd + unit * off, self.nd)

    def barrier_signal(self):
        bar = pltpu.get_barrier_semaphore()

        def body(k, _):
            pl.semaphore_signal(bar, inc=1, device_id={'dap': lax.rem(self.me + k, self.nd)}, device_id_type=MESH)
            return 0
        lax.fori_loop(1, self.nd, body, 0)

    def barrier_wait(self):
        pl.semaphore_wait(pltpu.get_barrier_semaphore(), self.nd - 1)

    def await_bytes(self, ref, sem):
        pltpu.make_async_copy(ref, ref, sem).wait()

    def at(self, chips, same=True):
        base = self.me if same else self.partner
        return lax.rem(base + self.nd + 2 * chips, self.nd)

    def slot(self, buf, chips, start=0, count=None):
        n = buf.shape[0] // self.nd
        return buf.at[pl.ds(self.at(chips) * n + start, n if count is None else count)]

    def gather_start(self, buf, i, c=0, nc=1):
        m = buf.shape[0] // self.nd // nc
        own = self.slot(buf, 0, c * m, m)

        def body(j, _):
            k = self.nd // 2 - j
            self.copy(own, own, self.ssem.at[i], self.gsem.at[i, k, 0], self.near(k, 2)).start()
            return 0
        lax.fori_loop(1, self.nd // 2, body, 0)
        self.copy(own, own, self.ssem.at[i], self.gsem.at[i, 0, 0], self.partner).start()

    def gather_finish(self, buf, i):
        n = buf.shape[0] // self.nd
        half = self.nd // 2

        def body(k, _):
            slot = buf.at[pl.ds(self.near(k, -2) * n, n)]
            self.await_bytes(slot, self.gsem.at[i, k, 0])
            self.copy(slot, slot, self.fsem.at[i], self.rsem.at[i], self.partner).start()
            return 0
        lax.fori_loop(1, half, body, 0)
        self.await_bytes(buf.at[pl.ds(0, n)], self.gsem.at[i, 0, 0])
        rest = buf.at[pl.ds(0, (half - 1) * n)]
        self.await_bytes(rest, self.rsem.at[i])
        self.await_bytes(rest, self.fsem.at[i])
        self.await_bytes(buf.at[pl.ds(0, half * n)], self.ssem.at[i])

    def relay(self, ref, i, recv, dev):
        self.copy(ref, ref, self.ssem.at[i], recv, dev).start()

    def relay_start(self, buf, i, c=0, nc=1):
        m = buf.shape[0] // self.nd // nc
        own = self.slot(buf, 0, c * m, m)
        self.relay(own, i, self.gsem.at[i, 0, c], self.at(1))
        self.relay(own, i, self.gsem.at[i, 4, c], self.at(-1))
        self.relay(own, i, self.rsem.at[i], self.partner)

    def relay_step(self, buf, i, p, c=0, nc=1):
        m = buf.shape[0] // self.nd // nc
        for part, sign in ((0, 1), (1, -1)):
            ref = self.slot(buf, -sign * p, c * m, m)
            self.await_bytes(ref, self.gsem.at[i, 4 * part + p - 1, c])
            on = self.slot(buf, -sign * p, c * m + part * (m // 2), m // 2) if p == self.nd // 4 - 1 else ref
            self.relay(on, i, self.gsem.at[i, 4 * part + p, c], self.at(sign))
            self.relay(ref, i, self.rsem.at[i], self.partner)

    def relay_finish(self, buf, i, nc=1):
        n = buf.shape[0] // self.nd
        m = n // nc
        half = self.nd // 2
        for c in range(nc):
            for part in range(2):
                ref = self.slot(buf, self.nd // 4, c * m + part * (m // 2), m // 2)
                self.await_bytes(ref, self.gsem.at[i, 4 * part + self.nd // 4 - 1, c])
        self.relay(self.slot(buf, self.nd // 4), i, self.rsem.at[i], self.partner)
        self.await_bytes(buf.at[pl.ds(0, half * n)], self.rsem.at[i])
        self.await_bytes(buf.at[pl.ds(0, (2 * half - 1) * n)], self.ssem.at[i])

    def swap_start(self, send, recv, i, t, rows):
        part = pl.ds(pl.multiple_of(rows * t, 8), rows)
        for k in range(self.nd - 1, 0, -1):
            off = (k + 1) // 2 if k % 2 else -(k // 2)
            d = lax.rem(self.me + self.nd + off, self.nd)
            self.copy(send.at[d, part], recv.at[self.me, part], self.ssem.at[i], self.rsem.at[i], d).start()
        pltpu.make_async_copy(send.at[self.me, part], recv.at[self.me, part], self.rsem.at[i]).start()

    def swap_finish(self, send, recv, i):
        self.await_bytes(recv, self.rsem.at[i])
        self.await_bytes(send.at[pl.ds(0, self.nd - 1)], self.ssem.at[i])


def kernel(names, late, nd, refs):
    r = dict(zip(names, refs))
    class N:
        pass
    v = N()
    v.__dict__.update(r)
    sl, nr, cm = v.m.shape
    rl, _, cz = v.z.shape
    ns = sl * nd
    wm, wz = v.row_w.shape[1] // 4, v.ts_w.shape[1] // 4
    gm, gz = wm // 128, wz // 128
    od = v.opm_i.shape[1] // 2
    def late_start():
        for n, name in enumerate(late):
            pltpu.make_async_copy(r['hbm_' + name], r[name], v.lsem.at[n]).start()

    def late_wait():
        for n, name in enumerate(late):
            pltpu.make_async_copy(r['hbm_' + name], r[name], v.lsem.at[n]).wait()

    comm = Comm(nd, (v.ssem, v.rsem, v.fsem, v.gsem))
    me = comm.me
    rows_m = sl * rl

    def store_piece(buf):
        def store(i, val):
            put_piece(buf, me * rl + i, val)
        return store

    def loop(n, body):
        def step(t, _):
            body(t)
            return 0
        lax.fori_loop(0, n, step, 0)

    def row_project(load, b):
        loop(sl // 2, lambda t: project([load(2 * t), load(2 * t + 1)], v.row_w.at[b], v.rt, v.rk, 2 * t, None))

    def row_attend(load, b, finish):
        def attend(s):
            keep = widen(spread(v.mask_seq[pl.ds(s, 1), :], 128), 4 * nr)
            return core(v.rt, v.rk, v.ro, [s], gm, v.rbias, [keep])

        def back(t):
            ups = [dot(v.ro[2 * t + n], v.row_o[b], 0, 0) for n in range(2)]
            yield
            yield from finish(t, [residual(load(2 * t + n), ups[n]) for n in range(2)])

        def body(u):
            interleave(back(u), attend(2 * u + 2))
            interleave(attend(2 * u + 3))
        loop(2, lambda s: interleave(attend(s)))
        loop(sl // 2 - 1, body)
        interleave(back(sl // 2 - 1))

    def col_project(load, b, after=lambda t: None):
        def body(t):
            project([load(4 * t + n) for n in range(4)], v.col_w.at[b], v.ct, v.ck, 4 * t, None)
            after(t)
        loop(rl // 4, body)

    def col_attend(first, count, after=lambda u: None):
        def body(u):
            t = first + u
            rows = [2 * t, 2 * t + 1]
            keeps = [widen(spread(v.mask_col[pl.ds(i, 1), :], 128), 4 * ns) for i in rows]
            interleave(core(v.ct, v.ck, v.co, rows, gm, None, keeps))
            after(u)
        loop(count, body)

    def col_out(load, b, finish, loc, gat, after=lambda t: None):
        def out(t):
            rows = [4 * t + n for n in range(4)]
            ups = [dot(v.co[i], v.col_o[b], 0, 0) for i in rows]
            new = [residual(load(i), u) for i, u in zip(rows, ups)]
            newf = [x.astype(F32) for x in new]
            finish(t, new, newf)
            ln = [layer_norm(x) for x in newf]
            acs = [dot(v.opm_i[b], x, 1, 1) for x in ln]
            for i, x in zip(rows, acs):
                ac = (x * v.mask_col[pl.ds(i, 1), :]).astype(BF16)
                a, c = ac[:od], ac[od:]
                loc[i] = a if b == 0 else c
                gat[me * rl + i] = c if b == 0 else a
            after(t)
        loop(rl // 4, out)

    def opm(loc, gat, b, load, wb, piece, i_piece, between):
        few = nr // 8

        def widen_gathered(j):
            value = gat[pl.ds(few * j, few)].astype(F32).reshape(few * od, ns)
            v.gcol[pl.ds(pl.multiple_of(few * od * j, 8), few * od), :] = value
        loop(8, widen_gathered)
        v.nrm[...] = dot(v.mask_col[...].astype(BF16), v.msa_mask[...].astype(F32).astype(BF16), 1, 0)

        def grow(t):
            left = loc[...].reshape(rl * od, ns)
            for n in range(4):
                g = 4 * t + n
                col = v.gcol[pl.ds(g, nr, stride=od), :].astype(BF16)
                x = dot(left, col, 1, 1).astype(BF16)
                off = pl.multiple_of(g * od, od)
                for i in range(rl):
                    v.xs[i, pl.ds(off, od), :] = x[od * i:od * i + od]
        loop(od // 4, grow)
        between()

        def fold(t):
            rows = [4 * t + n for n in range(4)]
            ups = [dot(v.opm_w[b], v.xs[i], 1, 0) for i in rows]
            ups = [u / (1e-3 + v.nrm[pl.ds(i, 1), :]) for i, u in zip(rows, ups)]
            ups = [u.T for u in ups]
            new = [residual(load(i), u) for i, u in zip(rows, ups)]
            for i, x in zip(rows, new):
                v.zc[i] = x
            ln = [layer_norm(x.astype(F32)) for x in new]
            ps = [dot(wb, x, 1, 1) for x in ln]
            for i, x in zip(rows, ps):
                put_piece(piece, me * rl + i, x)
            comm.gather_start(piece, i_piece, t, rl // 4)
        loop(rl // 4, fold)

    def zload(i):
        return v.zc[i].astype(F32)

    def tri_project(w):
        loop(rl // 4, lambda t: project([zload(4 * t + n) for n in range(4)], w, v.tt, v.tk, 4 * t, v.kc[...]))

    def tri_attend(wo, finish):
        def attend(t):
            return core(v.tt, v.tk, v.to, [4 * t + n for n in range(4)], gz, v.tbias, None)

        def back(t):
            rows = [4 * t + n for n in range(4)]
            ups = [dot(v.to[i], wo, 0, 0) for i in rows]
            yield
            yield from finish(t, [residual(zload(i), u) for i, u in zip(rows, ups)])

        interleave(attend(0))
        loop(rl // 4 - 1, lambda u: interleave(back(u), attend(u + 1)))
        interleave(back(rl // 4 - 1))

    def pieces(t, new, wb, piece):
        ln = [layer_norm(x.astype(F32)) for x in new]
        yield
        ps = [dot(wb, x, 1, 1) for x in ln]
        for n, x in enumerate(ps):
            put_piece(piece, me * rl + len(new) * t + n, x)

    def send(out, recv, i, rows, wb=None, piece=None):
        def finish(t, new):
            half = len(new) // 2
            for n in range(half):
                stage(out, half * t + n, new[2 * n].astype(F32), new[2 * n + 1].astype(F32), nd)
            count = len(new) * rows
            comm.swap_start(out, recv, i, t, count)
            if piece is not None:
                yield from pieces(t, new, wb, piece)
            else:
                yield
        return finish

    def keep(out, wb=None, piece=None):
        def finish(t, new):
            for n, x in enumerate(new):
                out[len(new) * t + n] = x
            if piece is not None:
                yield from pieces(t, new, wb, piece)
            else:
                yield
        return finish

    def turn(recv):
        fill(v.zwork, recv)
        for b in range(rl):
            v.zc[b] = take(v.zwork, b, nr, rl).astype(BF16)

    def mask_r():
        return v.res_mask[...].astype(F32)

    def prepare():
        v.mask_t[...] = v.msa_mask[...].astype(F32).T
        v.mask_seq[...] = v.msa_mask[pl.ds(pl.multiple_of(me * sl, sl), sl), :].astype(F32)
        for i in range(rl):
            v.mask_col[pl.ds(i, 1), :] = v.mask_t[pl.ds(me * rl + i, 1), :]
        v.kc[...] = spread(mask_r(), wz)
        size = od * od
        v.gcol[0:size] = v.opm_o[0].astype(F32)
        for q in range(od):
            v.gcol[size + od * q:size + od * q + od] = v.gcol[pl.ds(q, od, stride=od), :]
        for j in range(size // 128):
            v.opm_w[0, :, 128 * j:128 * j + 128] = v.gcol[size + 128 * j:size + 128 * j + 128].T.astype(BF16)
            v.opm_w[1, :, 128 * j:128 * j + 128] = v.opm_o[1, 128 * j:128 * j + 128, :].astype(F32).T.astype(BF16)

    comm.barrier_signal()
    late_start()
    nc = rl // 4

    def first_send(t):
        if isinstance(t, int) and t == 0:
            comm.barrier_wait()
        comm.gather_start(v.g0, 0, t, nc)
    bias_pieces(lambda i: v.z[i].astype(F32), rl, v.row_b[0], store_piece(v.g0), first_send)
    late_wait()
    mload = lambda s: v.m[s].astype(F32)
    row_project(mload, 0)
    prepare()
    comm.gather_finish(v.g0, 0)
    spread_bias(v.g0, v.gf, v.rbias, True, None)
    row_attend(mload, 0, send(v.s0, v.r0, 8, rl))
    comm.swap_finish(v.s0, v.r0, 8)

    fill(v.mwork, v.r0)
    cload = lambda i: take(v.mwork, i, ns, rl)
    col_project(cload, 0)

    def keep_four(t, new, newf):
        for n, x in enumerate(new):
            v.mc[4 * t + n] = x
    col_attend(0, rl // 2)
    col_out(cload, 0, keep_four, v.loc0, v.g1, lambda t: comm.relay_start(v.g1, 1, t, nc))

    c2load = lambda i: v.mc[i].astype(F32)

    def send_four(t, new, newf):
        for n in range(2):
            stage(v.s1, 2 * t + n, newf[2 * n], newf[2 * n + 1], nd)
    col_project(c2load, 1, lambda t: comm.relay_step(v.g1, 1, 1, t, nc))
    col_attend(0, rl // 4, lambda t: comm.relay_step(v.g1, 1, 2, t, nc))
    col_attend(rl // 4, rl // 4, lambda t: comm.relay_step(v.g1, 1, 3, t, nc))
    col_out(c2load, 1, send_four, v.loc1, v.g2)
    comm.relay_finish(v.g1, 1, nc)
    comm.relay_start(v.g2, 2)
    opm(v.loc0, v.g1, 0, lambda i: v.z[i].astype(F32), v.ts_b[0], v.g3, 3, lambda: comm.relay_step(v.g2, 2, 1))
    tri_project(v.ts_w.at[0])
    comm.gather_finish(v.g3, 3)
    comm.relay_step(v.g2, 2, 2)
    spread_bias(v.g3, v.gf2, v.tbias, True, mask_r())
    tri_attend(v.ts_o[0], send(v.s2, v.r2, 9, rl, v.te_b[0], v.g4))
    comm.gather_start(v.g4, 4)
    comm.relay_step(v.g2, 2, 3)
    comm.swap_finish(v.s2, v.r2, 9)
    turn(v.r2)
    tri_project(v.te_w.at[0])
    comm.gather_finish(v.g4, 4)
    comm.swap_start(v.s1, v.r1, 10, 0, rows_m)
    spread_bias(v.g4, v.gf2, v.tbias, False, mask_r())
    tri_attend(v.te_o[0], keep(v.zc, v.row_b[1], v.g5))


    comm.relay_finish(v.g2, 2)
    comm.relay_start(v.g5, 5)
    opm(v.loc1, v.g2, 1, zload, v.te_b[1], v.g6, 6, lambda: comm.relay_step(v.g5, 5, 1))
    comm.relay_step(v.g5, 5, 2)
    tri_project(v.te_w.at[1])
    comm.gather_finish(v.g6, 6)
    spread_bias(v.g6, v.gf2, v.tbias, True, mask_r())
    tri_attend(v.te_o[1], send(v.s3, v.r3, 11, rl, v.ts_b[1], v.g7))
    comm.gather_start(v.g7, 7)
    comm.swap_finish(v.s1, v.r1, 10)
    fill(v.mwork, v.r1)
    rload = lambda s: take(v.mwork, s, nr, sl)
    row_project(rload, 1)
    comm.relay_step(v.g5, 5, 3)
    comm.relay_finish(v.g5, 5)
    spread_bias(v.g5, v.gf, v.rbias, False, None)
    row_attend(rload, 1, keep(v.m_out))
    comm.swap_finish(v.s3, v.r3, 11)
    turn(v.r3)
    tri_project(v.ts_w.at[1])
    comm.gather_finish(v.g7, 7)
    spread_bias(v.g7, v.gf2, v.tbias, False, mask_r())
    tri_attend(v.ts_o[1], keep(v.z_out))


def solution(mesh):
    nd = mesh.shape['dap']

    def local_step(m, z, msa_mask, res_mask, w_row_bias, w_row_in, w_row_out, w_col_in, w_col_out, w_opm_in, w_opm_out, w_ts_bias, w_ts_in, w_ts_out, w_te_bias, w_te_in, w_te_out):
        sl, nr, cm = m.shape
        rl, _, cz = z.shape
        ns = sl * nd
        hm, ht = w_row_bias.shape[2], w_ts_bias.shape[2]
        wm, wz = hm * HEAD, ht * HEAD
        od = w_opm_in.shape[3]

        def rows_of(w):
            return jnp.moveaxis(w, 1, -1).reshape(2, -1, w.shape[1])

        ins = dict(m=m, z=z, msa_mask=msa_mask, res_mask=res_mask[None, :],
                   row_w=rows_of(w_row_in), row_o=w_row_out.reshape(2, wm, cm), row_b=rows_of(w_row_bias),
                   col_w=rows_of(w_col_in), col_o=w_col_out.reshape(2, wm, cm),
                   ts_w=rows_of(w_ts_in), ts_o=w_ts_out.reshape(2, wz, cz), ts_b=rows_of(w_ts_bias),
                   te_w=rows_of(w_te_in), te_o=w_te_out.reshape(2, wz, cz), te_b=rows_of(w_te_bias),
                   opm_i=rows_of(w_opm_in), opm_o=w_opm_out.reshape(2, od * od, cz))
        outs = dict(m_out=m, z_out=z)
        gm, gz = wm // 128, wz // 128
        xm, xz = (nd, sl * rl, cm), (nd, rl * rl, cz)
        grow, gtri, gopm = (nd * rl, 3, hm // 2, 128), (nd * rl, 3, ht // 2, 128), (nd * rl, od, ns)
        scratch = dict(
            s0=(xm, BF16), r0=(xm, BF16), s1=(xm, BF16), r1=(xm, BF16),
            s2=(xz, BF16), r2=(xz, BF16), s3=(xz, BF16), r3=(xz, BF16),
            g0=(grow, BF16), g5=(grow, BF16), g1=(gopm, BF16), g2=(gopm, BF16),
            g3=(gtri, BF16), g4=(gtri, BF16), g6=(gtri, BF16), g7=(gtri, BF16),
            gf=(grow, F32), gf2=(gtri, F32), rbias=((gm, nr, 4 * nr), F32), tbias=((gz, nr, 4 * nr), F32),
            mwork=((cm // 128, nd * sl * rl, 128), F32), zwork=((cz // 128, nr * rl, 128), F32),
            gcol=((nr * od, ns), F32), xs=((rl, od * od, nr), BF16), nrm=((rl, nr), F32), kc=((nr, wz), F32),
            rt=((sl, 3 * wm, nr), BF16), rk=((sl, nr, wm), BF16), ro=((sl, wm, nr), BF16),
            ct=((rl, 3 * wm, ns), BF16), ck=((rl, ns, wm), BF16), co=((rl, wm, ns), BF16),
            tt=((rl, 3 * wz, nr), BF16), tk=((rl, nr, wz), BF16), to=((rl, wz, nr), BF16),
            mask_t=((nr, ns), F32), mask_seq=((sl, nr), F32), mask_col=((rl, ns), F32), opm_w=((2, cz, od * od), BF16),
            mc=((rl, ns, cm), BF16), zc=((rl, nr, cz), BF16), loc0=((rl, od, ns), BF16), loc1=((rl, od, ns), BF16))
        sems = dict(ssem=(12,), rsem=(12,), fsem=(8,), gsem=(8, nd // 2, 3))
        late = [k for k in ins if k not in ('z', 'row_b')]
        for k in late:
            scratch[k] = (ins[k].shape, ins[k].dtype)
        sems['lsem'] = (len(late),)
        names = ['hbm_' + k if k in late else k for k in ins] + list(outs) + list(scratch) + list(sems)
        return pl.pallas_call(
            lambda *refs: kernel(names, late, nd, refs),
            out_shape=[jax.ShapeDtypeStruct(o.shape, o.dtype) for o in outs.values()],
            in_specs=[pl.BlockSpec(memory_space=pl.ANY if k in late else pltpu.VMEM) for k in ins],
            out_specs=[pl.BlockSpec(memory_space=pltpu.VMEM)] * len(outs),
            scratch_shapes=[pltpu.VMEM(*x) for x in scratch.values()] + [pltpu.SemaphoreType.DMA(x) for x in sems.values()],
            compiler_params=pltpu.CompilerParams(collective_id=0, has_side_effects=True, vmem_limit_bytes=67043328),
        )(*ins.values())

    in_specs = (P(('data', 'dap')), P(('data', 'dap')), P('data'), P('data')) + (P(),) * 13
    out_specs = (P(('data', 'dap')), P(('data', 'dap')))
    return jax.shard_map(local_step, mesh=mesh, in_specs=in_specs, out_specs=out_specs, check_vma=False)
```

```python
import functools

import jax
import jax.numpy as jnp
from jax import lax
from jax.experimental import pallas as pl
from jax.experimental.pallas import tpu as pltpu
from jax.sharding import PartitionSpec as P

F32 = jnp.float32
BF16 = jnp.bfloat16
LOG2E = 1.4426950408889634
NEG = -1e9 * LOG2E
HEAD = 32
MESH = pl.DeviceIdType.MESH


def dot(lhs, rhs, lc, rc):
    return lax.dot_general(lhs, rhs, (((lc,), (rc,)), ((), ())), preferred_element_type=F32)


def layer_norm(x):
    mean = jnp.mean(x, axis=-1, keepdims=True)
    cen = x - mean
    var = jnp.mean(cen * cen, axis=-1, keepdims=True)
    return (cen * lax.rsqrt(var + 1e-5)).astype(BF16)


def project(xs, w, t_ref, k_ref, first, kcol):
    width = w.shape[0] // 4
    xl = [layer_norm(x) for x in xs]
    for n, v in enumerate([dot(w[:width], v, 1, 1) for v in xl]):
        t_ref[first + n, 0:width] = v.astype(BF16)
    for n, v in enumerate([dot(w[2 * width:], v, 1, 1) for v in xl]):
        t_ref[first + n, width:3 * width] = v.astype(BF16)
    for n, v in enumerate([dot(v, w[width:2 * width], 1, 1) for v in xl]):
        if kcol is not None:
            v = v * kcol
        k_ref[first + n] = v.astype(BF16)


def diagonal(t, base, length):
    cols = []
    for r in range(4):
        parts = [t[base + HEAD * r:base + HEAD * r + HEAD]]
        if r > 0:
            parts.insert(0, jnp.zeros((HEAD * r, length), BF16))
        if r < 3:
            parts.append(jnp.zeros((HEAD * (3 - r), length), BF16))
        cols.append(jnp.concatenate(parts, axis=0))
    return jnp.concatenate(cols, axis=1)


def core(t_ref, k_ref, o_ref, rows, groups, bias, keeps):
    length = k_ref.shape[1]
    width = 128 * groups
    units = [(n, b, g) for n, b in enumerate(rows) for g in range(groups)]
    scores = []
    for n, b, g in units:
        t = t_ref[b, 128 * g:128 * g + 128, :]
        scores.append(dot(k_ref[b, :, 128 * g:128 * g + 128], diagonal(t, 0, length), 1, 0))
    yield
    probs = []
    dens = []
    for (n, b, g), s in zip(units, scores):
        s = s * (HEAD ** -0.5 * LOG2E)
        if bias is not None:
            s = s + bias[g]
        if keeps is not None:
            s = jnp.where(keeps[n] > 0, s, NEG)
        e = jnp.exp2(s - jnp.max(s, axis=0, keepdims=True))
        dens.append(jnp.sum(e, axis=0, keepdims=True))
        probs.append(e.astype(BF16))
    yield
    outs = [dot(t_ref[b, width + 128 * g:width + 128 * g + 128, :], p, 1, 0) for (n, b, g), p in zip(units, probs)]
    yield
    for (n, b, g), o, den in zip(units, outs, dens):
        inv = 1.0 / den
        gate = jax.nn.sigmoid(t_ref[b, 2 * width + 128 * g:2 * width + 128 * g + 128, :].astype(F32))
        parts = []
        for r in range(4):
            lanes = slice(length * r, length * r + length)
            parts.append(o[HEAD * r:HEAD * r + HEAD, lanes] * inv[:, lanes])
        o_ref[b, 128 * g:128 * g + 128, :] = (jnp.concatenate(parts, axis=0) * gate).astype(BF16)


def interleave(*gens):
    live = list(gens)
    while live:
        for gen in list(live):
            try:
                next(gen)
            except StopIteration:
                live.remove(gen)


def residual(x, update):
    return (x + update).astype(BF16)


def spread(row, lanes):
    return jnp.broadcast_to(row, (lanes, row.shape[1])).T


def widen(block, lanes):
    return jnp.concatenate([block] * (lanes // 128), axis=1)


def stage(stg, pair, first, second, ndev):
    rows = first.shape[0] // ndev
    off = pl.multiple_of(2 * rows * pair, 8)
    for d in range(ndev):
        both = jnp.concatenate([first[rows * d:rows * d + rows], second[rows * d:rows * d + rows]], axis=0)
        stg[d, pl.ds(off, 2 * rows), :] = both.astype(BF16)


def fill(work, ref):
    few = ref.shape[0] // 4
    rows = few * ref.shape[1]

    def body(j, _):
        for t in range(work.shape[0]):
            value = ref[pl.ds(few * j, few), :, 128 * t:128 * t + 128].astype(F32).reshape(rows, 128)
            work[t, pl.ds(pl.multiple_of(rows * j, 8), rows), :] = value
        return 0
    lax.fori_loop(0, 4, body, 0)


def take(work, start, count, stride):
    return jnp.concatenate([work.at[t][pl.ds(start, count, stride=stride), :] for t in range(work.shape[0])], axis=1)


def put_piece(buf, index, p):
    half = p.shape[0] // 2
    buf[index, 0] = p[:half, :128].astype(BF16)
    buf[index, 1] = p[half:, :128].astype(BF16)
    buf[index, 2] = jnp.concatenate([p[:half, 128:], p[half:, 128:]], axis=1).astype(BF16)


def spread_bias(gath, gf, bias, transpose, mask_row):
    length, half = gath.shape[0], gath.shape[2]
    gf[...] = gath[...].astype(F32)
    keep = None if mask_row is None else widen(spread(mask_row, 128), 4 * length)
    tails = [gf[:, 2, r, :] for r in range(half)]
    for g in range(2 * half // 4):
        parts = []
        for h in range(4 * g, 4 * g + 4):
            a, r = h // half, h % half
            value = jnp.concatenate([gf[:, a, r, :], tails[r][:, 64 * a:64 * a + 64]], axis=1)
            parts.append(value.T if transpose else value)
        value = jnp.concatenate(parts, axis=1) * LOG2E
        if keep is not None:
            value = jnp.where(keep > 0, value, NEG)
        bias[g] = value


def bias_pieces(load, count, wb, store, after):
    def body(t, _):
        zl = [layer_norm(load(4 * t + n)) for n in range(4)]
        ps = [dot(wb, v, 1, 1) for v in zl]
        for n, v in enumerate(ps):
            store(4 * t + n, v)
        after(t)
        return 0
    lax.fori_loop(0, count // 4, body, 0)


class Comm:
    def __init__(self, nd, sems):
        self.nd = nd
        self.me = lax.axis_index('dap')
        self.partner = self.me + 1 - 2 * lax.rem(self.me, 2)
        self.ssem, self.rsem, self.fsem, self.gsem = sems

    def copy(self, src, dst, send, recv, dev):
        return pltpu.make_async_remote_copy(src_ref=src, dst_ref=dst, send_sem=send, recv_sem=recv,
                                            device_id={'dap': dev}, device_id_type=MESH)

    def near(self, k, unit):
        off = ((k + 1) // 2) * (2 * lax.rem(k, 2) - 1)
        return lax.rem(self.me + self.nd + unit * off, self.nd)

    def barrier_signal(self):
        bar = pltpu.get_barrier_semaphore()

        def body(k, _):
            pl.semaphore_signal(bar, inc=1, device_id={'dap': lax.rem(self.me + k, self.nd)}, device_id_type=MESH)
            return 0
        lax.fori_loop(1, self.nd, body, 0)

    def barrier_wait(self):
        pl.semaphore_wait(pltpu.get_barrier_semaphore(), self.nd - 1)

    def await_bytes(self, ref, sem):
        pltpu.make_async_copy(ref, ref, sem).wait()

    def at(self, chips, same=True):
        base = self.me if same else self.partner
        return lax.rem(base + self.nd + 2 * chips, self.nd)

    def slot(self, buf, chips, start=0, count=None):
        n = buf.shape[0] // self.nd
        return buf.at[pl.ds(self.at(chips) * n + start, n if count is None else count)]

    def gather_start(self, buf, i, c=0, nc=1):
        m = buf.shape[0] // self.nd // nc
        own = self.slot(buf, 0, c * m, m)

        def body(j, _):
            k = self.nd // 2 - j
            self.copy(own, own, self.ssem.at[i], self.gsem.at[i, k, 0], self.near(k, 2)).start()
            return 0
        lax.fori_loop(1, self.nd // 2, body, 0)
        self.copy(own, own, self.ssem.at[i], self.gsem.at[i, 0, 0], self.partner).start()

    def gather_finish(self, buf, i):
        n = buf.shape[0] // self.nd
        half = self.nd // 2

        def body(k, _):
            slot = buf.at[pl.ds(self.near(k, -2) * n, n)]
            self.await_bytes(slot, self.gsem.at[i, k, 0])
            self.copy(slot, slot, self.fsem.at[i], self.rsem.at[i], self.partner).start()
            return 0
        lax.fori_loop(1, half, body, 0)
        self.await_bytes(buf.at[pl.ds(0, n)], self.gsem.at[i, 0, 0])
        rest = buf.at[pl.ds(0, (half - 1) * n)]
        self.await_bytes(rest, self.rsem.at[i])
        self.await_bytes(rest, self.fsem.at[i])
        self.await_bytes(buf.at[pl.ds(0, half * n)], self.ssem.at[i])

    def relay(self, ref, i, recv, dev):
        self.copy(ref, ref, self.ssem.at[i], recv, dev).start()

    def relay_start(self, buf, i, c=0, nc=1):
        m = buf.shape[0] // self.nd // nc
        own = self.slot(buf, 0, c * m, m)
        self.relay(own, i, self.gsem.at[i, 0, c], self.at(1))
        self.relay(own, i, self.gsem.at[i, 4, c], self.at(-1))
        self.relay(own, i, self.rsem.at[i], self.partner)

    def relay_step(self, buf, i, p, c=0, nc=1):
        m = buf.shape[0] // self.nd // nc
        for part, sign in ((0, 1), (1, -1)):
            ref = self.slot(buf, -sign * p, c * m, m)
            self.await_bytes(ref, self.gsem.at[i, 4 * part + p - 1, c])
            on = self.slot(buf, -sign * p, c * m + part * (m // 2), m // 2) if p == self.nd // 4 - 1 else ref
            self.relay(on, i, self.gsem.at[i, 4 * part + p, c], self.at(sign))
            self.relay(ref, i, self.rsem.at[i], self.partner)

    def relay_finish(self, buf, i, nc=1):
        n = buf.shape[0] // self.nd
        m = n // nc
        half = self.nd // 2
        for c in range(nc):
            for part in range(2):
                ref = self.slot(buf, self.nd // 4, c * m + part * (m // 2), m // 2)
                self.await_bytes(ref, self.gsem.at[i, 4 * part + self.nd // 4 - 1, c])
        self.relay(self.slot(buf, self.nd // 4), i, self.rsem.at[i], self.partner)
        self.await_bytes(buf.at[pl.ds(0, half * n)], self.rsem.at[i])
        self.await_bytes(buf.at[pl.ds(0, (2 * half - 1) * n)], self.ssem.at[i])

    def swap_start(self, send, recv, i, t, rows):
        part = pl.ds(pl.multiple_of(rows * t, 8), rows)
        def one(d):
            self.copy(send.at[d, part], recv.at[self.me, part], self.ssem.at[i], self.rsem.at[i], d).start()

        def body(j, _):
            one(self.near(self.nd - j, 1))
            return 0
        if isinstance(t, int):
            lax.fori_loop(1, self.nd, body, 0)
        else:
            for k in range(self.nd - 1, 0, -1):
                off = (k + 1) // 2 if k % 2 else -(k // 2)
                one(lax.rem(self.me + self.nd + off, self.nd))
        pltpu.make_async_copy(send.at[self.me, part], recv.at[self.me, part], self.rsem.at[i]).start()

    def swap_finish(self, send, recv, i):
        self.await_bytes(recv, self.rsem.at[i])
        self.await_bytes(send.at[pl.ds(0, self.nd - 1)], self.ssem.at[i])


def kernel(names, late, nd, refs):
    r = dict(zip(names, refs))
    class N:
        pass
    v = N()
    v.__dict__.update(r)
    sl, nr, cm = v.m.shape
    rl, _, cz = v.z.shape
    ns = sl * nd
    wm, wz = v.row_w.shape[1] // 4, v.ts_w.shape[1] // 4
    gm, gz = wm // 128, wz // 128
    od = v.opm_i.shape[1] // 2
    def late_start():
        for n, name in enumerate(late):
            pltpu.make_async_copy(r['hbm_' + name], r[name], v.lsem.at[n]).start()

    def late_wait():
        for n, name in enumerate(late):
            pltpu.make_async_copy(r['hbm_' + name], r[name], v.lsem.at[n]).wait()

    comm = Comm(nd, (v.ssem, v.rsem, v.fsem, v.gsem))
    me = comm.me
    rows_m = sl * rl

    def store_piece(buf):
        def store(i, val):
            put_piece(buf, me * rl + i, val)
        return store

    def loop(n, body):
        def step(t, _):
            body(t)
            return 0
        lax.fori_loop(0, n, step, 0)

    def row_project(load, b):
        loop(sl // 2, lambda t: project([load(2 * t), load(2 * t + 1)], v.row_w.at[b], v.rt, v.rk, 2 * t, None))

    def row_attend(load, b, finish):
        def attend(s):
            keep = widen(spread(v.mask_seq[pl.ds(s, 1), :], 128), 4 * nr)
            return core(v.rt, v.rk, v.ro, [s], gm, v.rbias, [keep])

        def back(t):
            ups = [dot(v.ro[2 * t + n], v.row_o[b], 0, 0) for n in range(2)]
            yield
            yield from finish(t, [residual(load(2 * t + n), ups[n]) for n in range(2)])

        def body(u):
            interleave(back(u), attend(2 * u + 2))
            interleave(attend(2 * u + 3))
        loop(2, lambda s: interleave(attend(s)))
        loop(sl // 2 - 1, body)
        interleave(back(sl // 2 - 1))

    def col_project(load, b, after=lambda t: None):
        def body(t):
            project([load(4 * t + n) for n in range(4)], v.col_w.at[b], v.ct, v.ck, 4 * t, None)
            after(t)
        loop(rl // 4, body)

    def col_attend(first, count, after=lambda u: None):
        def body(u):
            t = first + u
            rows = [2 * t, 2 * t + 1]
            keeps = [widen(spread(v.mask_col[pl.ds(i, 1), :], 128), 4 * ns) for i in rows]
            interleave(core(v.ct, v.ck, v.co, rows, gm, None, keeps))
            after(u)
        loop(count, body)

    def col_out(load, b, finish, loc, gat, after=lambda t: None):
        def out(t):
            rows = [4 * t + n for n in range(4)]
            ups = [dot(v.co[i], v.col_o[b], 0, 0) for i in rows]
            new = [residual(load(i), u) for i, u in zip(rows, ups)]
            newf = [x.astype(F32) for x in new]
            finish(t, new, newf)
            ln = [layer_norm(x) for x in newf]
            acs = [dot(v.opm_i[b], x, 1, 1) for x in ln]
            for i, x in zip(rows, acs):
                ac = (x * v.mask_col[pl.ds(i, 1), :]).astype(BF16)
                a, c = ac[:od], ac[od:]
                loc[i] = a if b == 0 else c
                gat[me * rl + i] = c if b == 0 else a
            after(t)
        loop(rl // 4, out)

    def opm(loc, gat, b, load, wb, piece, i_piece, between):
        few = nr // 8

        def widen_gathered(j):
            value = gat[pl.ds(few * j, few)].astype(F32).reshape(few * od, ns)
            v.gcol[pl.ds(pl.multiple_of(few * od * j, 8), few * od), :] = value
        loop(8, widen_gathered)
        v.nrm[...] = dot(v.mask_col[...].astype(BF16), v.msa_mask[...].astype(F32).astype(BF16), 1, 0)

        def grow(t):
            left = loc[...].reshape(rl * od, ns)
            for n in range(4):
                g = 4 * t + n
                col = v.gcol[pl.ds(g, nr, stride=od), :].astype(BF16)
                x = dot(left, col, 1, 1).astype(BF16)
                off = pl.multiple_of(g * od, od)
                for i in range(rl):
                    v.xs[i, pl.ds(off, od), :] = x[od * i:od * i + od]
        loop(od // 4, grow)
        between()

        def fold(t):
            rows = [4 * t + n for n in range(4)]
            ups = [dot(v.opm_w[b], v.xs[i], 1, 0) for i in rows]
            ups = [u / (1e-3 + v.nrm[pl.ds(i, 1), :]) for i, u in zip(rows, ups)]
            ups = [u.T for u in ups]
            new = [residual(load(i), u) for i, u in zip(rows, ups)]
            for i, x in zip(rows, new):
                v.zc[i] = x
            ln = [layer_norm(x.astype(F32)) for x in new]
            ps = [dot(wb, x, 1, 1) for x in ln]
            for i, x in zip(rows, ps):
                put_piece(piece, me * rl + i, x)
            comm.gather_start(piece, i_piece, t, rl // 4)
        loop(rl // 4, fold)

    def zload(i):
        return v.zc[i].astype(F32)

    def tri_project(w):
        loop(rl // 4, lambda t: project([zload(4 * t + n) for n in range(4)], w, v.tt, v.tk, 4 * t, v.kc[...]))

    def tri_attend(wo, finish):
        def attend(t):
            return core(v.tt, v.tk, v.to, [4 * t + n for n in range(4)], gz, v.tbias, None)

        def back(t):
            rows = [4 * t + n for n in range(4)]
            ups = [dot(v.to[i], wo, 0, 0) for i in rows]
            yield
            yield from finish(t, [residual(zload(i), u) for i, u in zip(rows, ups)])

        interleave(attend(0))
        loop(rl // 4 - 1, lambda u: interleave(back(u), attend(u + 1)))
        interleave(back(rl // 4 - 1))

    def pieces(t, new, wb, piece):
        ln = [layer_norm(x.astype(F32)) for x in new]
        yield
        ps = [dot(wb, x, 1, 1) for x in ln]
        for n, x in enumerate(ps):
            put_piece(piece, me * rl + len(new) * t + n, x)

    def send(out, recv, i, rows, wb=None, piece=None):
        def finish(t, new):
            half = len(new) // 2
            for n in range(half):
                stage(out, half * t + n, new[2 * n].astype(F32), new[2 * n + 1].astype(F32), nd)
            count = len(new) * rows
            comm.swap_start(out, recv, i, t, count)
            if piece is not None:
                yield from pieces(t, new, wb, piece)
            else:
                yield
        return finish

    def keep(out, wb=None, piece=None):
        def finish(t, new):
            for n, x in enumerate(new):
                out[len(new) * t + n] = x
            if piece is not None:
                yield from pieces(t, new, wb, piece)
            else:
                yield
        return finish

    def turn(recv):
        fill(v.zwork, recv)
        for b in range(rl):
            v.zc[b] = take(v.zwork, b, nr, rl).astype(BF16)

    def mask_r():
        return v.res_mask[...].astype(F32)

    def prepare():
        v.mask_t[...] = v.msa_mask[...].astype(F32).T
        v.mask_seq[...] = v.msa_mask[pl.ds(pl.multiple_of(me * sl, sl), sl), :].astype(F32)
        for i in range(rl):
            v.mask_col[pl.ds(i, 1), :] = v.mask_t[pl.ds(me * rl + i, 1), :]
        v.kc[...] = spread(mask_r(), wz)
        size = od * od
        v.gcol[0:size] = v.opm_o[0].astype(F32)
        for q in range(od):
            v.gcol[size + od * q:size + od * q + od] = v.gcol[pl.ds(q, od, stride=od), :]
        for j in range(size // 128):
            v.opm_w[0, :, 128 * j:128 * j + 128] = v.gcol[size + 128 * j:size + 128 * j + 128].T.astype(BF16)
            v.opm_w[1, :, 128 * j:128 * j + 128] = v.opm_o[1, 128 * j:128 * j + 128, :].astype(F32).T.astype(BF16)

    comm.barrier_signal()
    late_start()
    nc = rl // 4

    def first_send(t):
        @pl.when(t == 0)
        def _():
            comm.barrier_wait()
        comm.gather_start(v.g0, 0, t, nc)
    bias_pieces(lambda i: v.z[i].astype(F32), rl, v.row_b[0], store_piece(v.g0), first_send)
    late_wait()
    mload = lambda s: v.m[s].astype(F32)
    row_project(mload, 0)
    prepare()
    comm.gather_finish(v.g0, 0)
    spread_bias(v.g0, v.gf, v.rbias, True, None)
    row_attend(mload, 0, send(v.s0, v.r0, 8, rl))
    comm.swap_finish(v.s0, v.r0, 8)

    fill(v.mwork, v.r0)
    cload = lambda i: take(v.mwork, i, ns, rl)
    col_project(cload, 0)

    def keep_four(t, new, newf):
        for n, x in enumerate(new):
            v.mc[4 * t + n] = x
    col_attend(0, rl // 2)
    col_out(cload, 0, keep_four, v.loc0, v.g1, lambda t: comm.relay_start(v.g1, 1, t, nc))

    c2load = lambda i: v.mc[i].astype(F32)

    def send_four(t, new, newf):
        for n in range(2):
            stage(v.s1, 2 * t + n, newf[2 * n], newf[2 * n + 1], nd)
    col_project(c2load, 1, lambda t: comm.relay_step(v.g1, 1, 1, t, nc))
    col_attend(0, rl // 4, lambda t: comm.relay_step(v.g1, 1, 2, t, nc))
    col_attend(rl // 4, rl // 4, lambda t: comm.relay_step(v.g1, 1, 3, t, nc))
    col_out(c2load, 1, send_four, v.loc1, v.g2)
    comm.relay_finish(v.g1, 1, nc)
    comm.relay_start(v.g2, 2)
    opm(v.loc0, v.g1, 0, lambda i: v.z[i].astype(F32), v.ts_b[0], v.g3, 3, lambda: comm.relay_step(v.g2, 2, 1))
    comm.relay_step(v.g2, 2, 2)
    tri_project(v.ts_w.at[0])
    comm.gather_finish(v.g3, 3)
    comm.relay_step(v.g2, 2, 3)
    spread_bias(v.g3, v.gf2, v.tbias, True, mask_r())
    tri_attend(v.ts_o[0], send(v.s2, v.r2, 9, rl, v.te_b[0], v.g4))
    comm.gather_start(v.g4, 4)
    comm.swap_finish(v.s2, v.r2, 9)
    turn(v.r2)
    tri_project(v.te_w.at[0])
    comm.gather_finish(v.g4, 4)
    comm.swap_start(v.s1, v.r1, 10, 0, rows_m)
    spread_bias(v.g4, v.gf2, v.tbias, False, mask_r())
    tri_attend(v.te_o[0], keep(v.zc, v.row_b[1], v.g5))


    comm.relay_finish(v.g2, 2)
    comm.relay_start(v.g5, 5)
    opm(v.loc1, v.g2, 1, zload, v.te_b[1], v.g6, 6, lambda: comm.relay_step(v.g5, 5, 1))
    comm.relay_step(v.g5, 5, 2)
    comm.swap_finish(v.s1, v.r1, 10)
    fill(v.mwork, v.r1)
    rload = lambda s: take(v.mwork, s, nr, sl)
    row_project(rload, 1)
    comm.relay_step(v.g5, 5, 3)
    tri_project(v.te_w.at[1])
    comm.gather_finish(v.g6, 6)
    spread_bias(v.g6, v.gf2, v.tbias, True, mask_r())
    tri_attend(v.te_o[1], send(v.s3, v.r3, 11, rl, v.ts_b[1], v.g7))
    comm.gather_start(v.g7, 7)
    comm.relay_finish(v.g5, 5)
    spread_bias(v.g5, v.gf, v.rbias, False, None)
    row_attend(rload, 1, keep(v.m_out))
    comm.swap_finish(v.s3, v.r3, 11)
    turn(v.r3)
    tri_project(v.ts_w.at[1])
    comm.gather_finish(v.g7, 7)
    spread_bias(v.g7, v.gf2, v.tbias, False, mask_r())
    tri_attend(v.ts_o[1], keep(v.z_out))


def solution(mesh):
    nd = mesh.shape['dap']

    def local_step(m, z, msa_mask, res_mask, w_row_bias, w_row_in, w_row_out, w_col_in, w_col_out, w_opm_in, w_opm_out, w_ts_bias, w_ts_in, w_ts_out, w_te_bias, w_te_in, w_te_out):
        sl, nr, cm = m.shape
        rl, _, cz = z.shape
        ns = sl * nd
        hm, ht = w_row_bias.shape[2], w_ts_bias.shape[2]
        wm, wz = hm * HEAD, ht * HEAD
        od = w_opm_in.shape[3]

        def rows_of(w):
            return jnp.moveaxis(w, 1, -1).reshape(2, -1, w.shape[1])

        ins = dict(m=m, z=z, msa_mask=msa_mask, res_mask=res_mask[None, :],
                   row_w=rows_of(w_row_in), row_o=w_row_out.reshape(2, wm, cm), row_b=rows_of(w_row_bias),
                   col_w=rows_of(w_col_in), col_o=w_col_out.reshape(2, wm, cm),
                   ts_w=rows_of(w_ts_in), ts_o=w_ts_out.reshape(2, wz, cz), ts_b=rows_of(w_ts_bias),
                   te_w=rows_of(w_te_in), te_o=w_te_out.reshape(2, wz, cz), te_b=rows_of(w_te_bias),
                   opm_i=rows_of(w_opm_in), opm_o=w_opm_out.reshape(2, od * od, cz))
        outs = dict(m_out=m, z_out=z)
        gm, gz = wm // 128, wz // 128
        xm, xz = (nd, sl * rl, cm), (nd, rl * rl, cz)
        grow, gtri, gopm = (nd * rl, 3, hm // 2, 128), (nd * rl, 3, ht // 2, 128), (nd * rl, od, ns)
        scratch = dict(
            s0=(xm, BF16), r0=(xm, BF16), s1=(xm, BF16), r1=(xm, BF16),
            s2=(xz, BF16), r2=(xz, BF16), s3=(xz, BF16), r3=(xz, BF16),
            g0=(grow, BF16), g5=(grow, BF16), g1=(gopm, BF16), g2=(gopm, BF16),
            g3=(gtri, BF16), g4=(gtri, BF16), g6=(gtri, BF16), g7=(gtri, BF16),
            gf=(grow, F32), gf2=(gtri, F32), rbias=((gm, nr, 4 * nr), F32), tbias=((gz, nr, 4 * nr), F32),
            mwork=((cm // 128, nd * sl * rl, 128), F32), zwork=((cz // 128, nr * rl, 128), F32),
            gcol=((nr * od, ns), F32), xs=((rl, od * od, nr), BF16), nrm=((rl, nr), F32), kc=((nr, wz), F32),
            rt=((sl, 3 * wm, nr), BF16), rk=((sl, nr, wm), BF16), ro=((sl, wm, nr), BF16),
            ct=((rl, 3 * wm, ns), BF16), ck=((rl, ns, wm), BF16), co=((rl, wm, ns), BF16),
            tt=((rl, 3 * wz, nr), BF16), tk=((rl, nr, wz), BF16), to=((rl, wz, nr), BF16),
            mask_t=((nr, ns), F32), mask_seq=((sl, nr), F32), mask_col=((rl, ns), F32), opm_w=((2, cz, od * od), BF16),
            mc=((rl, ns, cm), BF16), zc=((rl, nr, cz), BF16), loc0=((rl, od, ns), BF16), loc1=((rl, od, ns), BF16))
        sems = dict(ssem=(12,), rsem=(12,), fsem=(8,), gsem=(8, nd // 2, 3))
        late = [k for k in ins if k not in ('z', 'row_b')]
        for k in late:
            scratch[k] = (ins[k].shape, ins[k].dtype)
        sems['lsem'] = (len(late),)
        names = ['hbm_' + k if k in late else k for k in ins] + list(outs) + list(scratch) + list(sems)
        return pl.pallas_call(
            lambda *refs: kernel(names, late, nd, refs),
            out_shape=[jax.ShapeDtypeStruct(o.shape, o.dtype) for o in outs.values()],
            in_specs=[pl.BlockSpec(memory_space=pl.ANY if k in late else pltpu.VMEM) for k in ins],
            out_specs=[pl.BlockSpec(memory_space=pltpu.VMEM)] * len(outs),
            scratch_shapes=[pltpu.VMEM(*x) for x in scratch.values()] + [pltpu.SemaphoreType.DMA(x) for x in sems.values()],
            compiler_params=pltpu.CompilerParams(collective_id=0, has_side_effects=True, vmem_limit_bytes=67043328),
        )(*ins.values())

    in_specs = (P(('data', 'dap')), P(('data', 'dap')), P('data'), P('data')) + (P(),) * 13
    out_specs = (P(('data', 'dap')), P(('data', 'dap')))
    return jax.shard_map(local_step, mesh=mesh, in_specs=in_specs, out_specs=out_specs, check_vma=False)
```
